32 devices in a mesh: rows: 8 (over z, x), cols: 4 (over y, core).
Axes of the slice: x: 2, y: 2, z: 4, core: 2. Of those that a mesh axis runs over, the one named last changes fastest.
Arguments:
- leading_scene_data: float32 [2, 1024, 8192], P(None, 'rows', 'cols'), may hold values from -12 to 12, as said below
- trailing_scene_data: float32 [2, 1024, 8192], P(None, 'rows', 'cols'), may hold values from -20 to 20, as said below
- shared_usable_flags: int32 [1024, 8192], P('rows', 'cols'), may hold values 0 or 1
- sweep_of_each_line: int32 [1024], P('rows'), may hold values from 0 to 15, never falling along the last dimension, each value on 1 to 128 neighbouring positions
Outputs:
- deramped: float32 [2, 1024, 8192], P(None, 'rows', 'cols')
- coherence: float32 [1024, 8192], P('rows', 'cols')
The draws below stay inside these ranges and needn't reach their ends.
Inputs may be any that keep to these rules, and one draw needn't show every extreme that they name: `leading_scene_data`: first scene's parts lie in [-12, 12]. `trailing_scene_data`: second scene's parts lie in [-20, 20]; it is the first scene rotated by a smooth phase plus independent noise. `sweep_of_each_line`: burst ids never fall along the rows; each burst holds 1 to 128 rows, one exactly that many.
All inputs are finite; a program needn't handle non-finite values.
Results may differ from the reference program's by a relative error of at most 0.0003.
Values sent between devices are 32-bit elements.
A program may use at most 64 MiB of HBM per device.

```python
import math
import jax
import jax.numpy as jnp
import numpy as np
from jax import lax

WIN_R = 32
WIN_C = 8
SWEEP_TALLY = 16
SCENE_LINES = 1024
NC = 8192


def scene_primary(key):
    planes = jnp.clip(jax.random.normal(jax.random.fold_in(key, 11), (2, SCENE_LINES, NC), jnp.float32), -6.0, 6.0)
    return planes


def draw_leading_scene_data(key, part):
    return scene_primary(key)


def draw_trailing_scene_data(key, part):
    planes = scene_primary(key)
    speckle = jnp.clip(jax.random.normal(jax.random.fold_in(key, 12), (2, SCENE_LINES, NC), jnp.float32), -6.0, 6.0)
    slopes = jax.random.uniform(jax.random.fold_in(key, 13), (2,), jnp.float32)
    across_slope_term = 2.0 + 2.0 * slopes[0]
    along_slope_term = 1.5 + 1.5 * slopes[1]
    across_coordinate = (jnp.arange(NC, dtype=jnp.float32) + 0.5) / NC
    along_coordinate = (jnp.arange(SCENE_LINES, dtype=jnp.float32) + 0.5) / SCENE_LINES
    planar_angle_fit = across_slope_term * across_coordinate[None, :] + along_slope_term * SWEEP_TALLY * along_coordinate[:, None]
    cos_part = jnp.cos(planar_angle_fit)
    sine_part = jnp.sin(planar_angle_fit)
    real_b = 0.8 * (planes[0] * cos_part + planes[1] * sine_part) + 0.6 * speckle[0]
    imag_b = 0.8 * (planes[1] * cos_part - planes[0] * sine_part) + 0.6 * speckle[1]
    return jnp.stack([real_b, imag_b])


def touch_ends(array, stream_key, smallest, high):
    spot = [jax.random.randint(jax.random.fold_in(stream_key, axis), (), 0, length) for axis, length in enumerate(array.shape)]
    longest = array.shape.index(max(array.shape))
    neighbour = spot[:longest] + [(spot[longest] + 1) % array.shape[longest]] + spot[longest + 1:]
    return array.at[tuple(spot)].set(smallest).at[tuple(neighbour)].set(high)


def profile(count, total, bound, slope):
    weights = [(1 << 20) // math.isqrt(grade ** slope) + 1 for grade in range(2, count + 1)]
    spare, holding = total - bound - (count - 1), [1] * (count - 1)
    while spare > 0:
        candidates = [i for i in range(count - 1) if holding[i] < bound]
        whole, left = sum([weights[i] for i in candidates]), spare
        for i in candidates:
            addition = min(bound - holding[i], max(1, left * weights[i] // whole), spare)
            holding[i] = holding[i] + addition
            spare = spare - addition
    return np.array([bound] + holding)


def ragged(key, count, total, most, skew):
    if count == 2:
        one = jax.random.randint(key, (), max(1, total - most), min(most, total - 1) + 1)
        return jnp.stack([one, total - one])
    tallies = jnp.asarray(profile(count, total, most, skew), jnp.int32)
    couples = (count - 1) // 2
    source_of, taker = tallies[1:1 + 2 * couples:2], tallies[2:2 + 2 * couples:2]
    slack = jnp.minimum(source_of - 1, most - taker)
    passed = jax.random.randint(jax.random.fold_in(key, 1), (couples,), 0, 1 << 20) % (slack + 1)
    tallies = tallies.at[1:1 + 2 * couples:2].set(source_of - passed).at[2:2 + 2 * couples:2].set(taker + passed)
    return tallies[jax.random.permutation(jax.random.fold_in(key, 2), count)]


def setup_inputs(seed: int = 0) -> dict:
    keys = jax.random.split(jax.random.key(seed), 5)
    leading_scene_data = draw_leading_scene_data(jax.random.fold_in(keys[4], 71), 0)
    trailing_scene_data = draw_trailing_scene_data(jax.random.fold_in(keys[4], 71), 0)
    shared_usable_flags = touch_ends((jax.random.randint(keys[2], (SCENE_LINES, NC), 0, 8) < 7).astype(jnp.int32), jax.random.fold_in(keys[2], 1), 0, 1)
    sweep_of_each_line = jnp.searchsorted(jnp.cumsum(ragged(keys[3], SWEEP_TALLY, SCENE_LINES, 2 * SCENE_LINES // SWEEP_TALLY, 1)), jnp.arange(SCENE_LINES), side="right").astype(jnp.int32)
    return {"leading_scene_data": leading_scene_data, "trailing_scene_data": trailing_scene_data, "shared_usable_flags": shared_usable_flags, "sweep_of_each_line": sweep_of_each_line}


largest_value = lax.Precision.HIGHEST

def box_filter(plane):
    zero_value = jnp.zeros((), plane.dtype)
    return lax.reduce_window(plane, zero_value, lax.add, (WIN_R, WIN_C), (1, 1), ((WIN_R // 2, WIN_R // 2 - 1), (WIN_C // 2, WIN_C // 2 - 1)))

def sweep_aggregates(sweep_membership, line_aggregates):
    return jnp.dot(sweep_membership.T, line_aggregates, precision=largest_value)

def solve_ramps(pixel_count, moment_cc, moment_cr, moment_rr, sums):
    ridge_term = 0.001 * pixel_count + 1.0
    diag_col = moment_cc + ridge_term
    diag_row = moment_rr + ridge_term
    determinant = diag_col * diag_row - moment_cr * moment_cr
    base_part = sums[:, 0:2] / (pixel_count + ridge_term)[:, None]
    col_slope = (diag_row[:, None] * sums[:, 2:4] - moment_cr[:, None] * sums[:, 4:6]) / determinant[:, None]
    row_slope = (diag_col[:, None] * sums[:, 4:6] - moment_cr[:, None] * sums[:, 2:4]) / determinant[:, None]
    return jnp.concatenate([base_part, col_slope, row_slope], 1)

def reference(leading_scene_data, trailing_scene_data, shared_usable_flags, sweep_of_each_line):
    weight = shared_usable_flags.astype(jnp.float32)
    real_a = leading_scene_data[0] * weight
    imag_a = leading_scene_data[1] * weight
    real_b = trailing_scene_data[0] * weight
    imag_b = trailing_scene_data[1] * weight
    boxed_real = box_filter(real_a * real_b + imag_a * imag_b)
    boxed_imag = box_filter(imag_a * real_b - real_a * imag_b)
    boxed_pa = box_filter(real_a * real_a + imag_a * imag_a)
    boxed_pb = box_filter(real_b * real_b + imag_b * imag_b)
    normaliser = jnp.sqrt((boxed_pa + 1.0) * (boxed_pb + 1.0))
    coh_real = boxed_real / normaliser
    coh_imag = boxed_imag / normaliser
    coherence = jnp.sqrt(coh_real * coh_real + coh_imag * coh_imag)
    across_coordinate = (jnp.arange(NC, dtype=jnp.float32) + 0.5) * (2.0 / NC) - 1.0
    along_coordinate = (jnp.arange(SCENE_LINES, dtype=jnp.float32) + 0.5) * (2.0 / SCENE_LINES) - 1.0
    sweep_membership = (sweep_of_each_line[:, None] == jnp.arange(SWEEP_TALLY, dtype=jnp.int32)[None, :]).astype(jnp.float32)
    line_usable_tally = lax.optimization_barrier(jnp.sum(weight, 1))
    along_across_moment = lax.optimization_barrier(jnp.sum(weight * across_coordinate[None, :], 1))
    recentered_aggregates = sweep_aggregates(sweep_membership, jnp.stack([line_usable_tally, along_across_moment, along_coordinate * line_usable_tally], 1))
    pixel_count = recentered_aggregates[:, 0]
    floored = jnp.maximum(pixel_count, 1.0)
    middle_across = recentered_aggregates[:, 1] / floored
    middle_along = recentered_aggregates[:, 2] / floored
    along_displacement = along_coordinate - jnp.dot(sweep_membership, middle_along, precision=largest_value)
    across_displacement = across_coordinate[None, :] - jnp.dot(sweep_membership, middle_across, precision=largest_value)[:, None]
    weighted_u = weight * across_displacement
    line_cross_inphase = lax.optimization_barrier(jnp.sum(weight * coh_real, 1))
    line_cross_quadrature = lax.optimization_barrier(jnp.sum(weight * coh_imag, 1))
    along_coordinate_power_two = lax.optimization_barrier(jnp.sum(weighted_u * across_displacement, 1))
    along_first_moment = lax.optimization_barrier(jnp.sum(weighted_u, 1))
    along_weighted_inphase = lax.optimization_barrier(jnp.sum(weighted_u * coh_real, 1))
    along_weighted_quadrature = lax.optimization_barrier(jnp.sum(weighted_u * coh_imag, 1))
    following_picture = sweep_aggregates(sweep_membership, jnp.stack([along_coordinate_power_two, along_displacement * along_first_moment, along_displacement * along_displacement * line_usable_tally, line_cross_inphase, line_cross_quadrature, along_weighted_inphase, along_weighted_quadrature, along_displacement * line_cross_inphase, along_displacement * line_cross_quadrature], 1))
    planar_trends = solve_ramps(pixel_count, following_picture[:, 0], following_picture[:, 1], following_picture[:, 2], following_picture[:, 3:9])
    for_each_line = jnp.dot(sweep_membership, planar_trends, precision=largest_value)
    model_real = for_each_line[:, 0:1] + for_each_line[:, 2:3] * across_displacement + (for_each_line[:, 4] * along_displacement)[:, None]
    model_imag = for_each_line[:, 1:2] + for_each_line[:, 3:4] * across_displacement + (for_each_line[:, 5] * along_displacement)[:, None]
    out_real = coh_real * model_real + coh_imag * model_imag
    out_imag = coh_imag * model_real - coh_real * model_imag
    return (jnp.stack([out_real, out_imag]), coherence)
```

```python
import functools

import jax
import jax.numpy as jnp
from jax import lax
from jax.experimental import pallas as pl
from jax.experimental.pallas import tpu as pltpu
from jax.sharding import PartitionSpec as P

WIN_R = 32
WIN_C = 8
SWEEP_TALLY = 16

EDGE = WIN_R // 2
SIDE = WIN_C // 2
LANES = 128
SCALE = 2.0**56
FLOOR = 1e-36
F32 = jnp.float32
BF16 = jnp.bfloat16
MESH = pl.DeviceIdType.MESH


def masked(av, bv, wv, rows, lanes):
    w = wv[rows, lanes].astype(F32)
    return av[0, rows, lanes] * w, av[1, rows, lanes] * w, bv[0, rows, lanes] * w, bv[1, rows, lanes] * w


def encode(ar, ai, br, bi):
    sr, si = ar * SCALE, ai * SCALE
    power = sr * sr + si * si
    some = power > FLOOR
    inverse = lax.rsqrt(jnp.where(some, power, 1.0))
    return (
        jnp.where(some, power * inverse * (1.0 / SCALE), 0.0),
        jnp.where(some, (sr * br + si * bi) * inverse, br),
        jnp.where(some, (si * br - sr * bi) * inverse, bi),
    )


def decode(s, gr, gi):
    return s * gr, s * gi, s * s, gr * gr + gi * gi


def put_split(out, products, lanes, rows, low_rows):
    for plane, value in enumerate(products):
        high = value.astype(BF16)
        low = (value - high.astype(F32)).astype(BF16)
        for where in lanes:
            out[plane, rows, where] = high
            out[plane, low_rows, where] = low


def edge_block(pack):
    lane = lax.broadcasted_iota(jnp.int32, pack.shape, 1)
    left, right = lane >= LANES - SIDE, lane < SIDE

    def pick(k):
        a = pack if k == 0 else pltpu.roll(pack, k * SIDE, 1)
        b = pack if k == 0 else pltpu.roll(pack, LANES - k * SIDE, 1)
        return jnp.where(left, a, jnp.where(right, b, 0.0))

    return pick(0), pick(1), pick(2)


def chunk_tiles(tiles):
    if tiles < 8:
        return ((0, tiles),)
    cuts = [0, tiles * 5 // 16, tiles * 10 // 16, tiles * 13 // 16, tiles]
    return tuple((a, b) for a, b in zip(cuts[:-1], cuts[1:]))


def fold(x):
    total = x[:, 0:LANES]
    for t in range(1, x.shape[1] // LANES):
        total = total + x[:, t * LANES : (t + 1) * LANES]
    return total


def front_kernel(
    n_rows, n_cols, reach,
    lead, trail, flags, sweep,
    gam, coh, memt, fit,
    av, bv, wv, sv, up_out, down_out, top_in, bot_in, left_out, right_out, left_in, right_in,
    corner, corner_top, corner_bot, split, halo_split, vert, across, edge_sums, acc_g, acc_h,
    tab_out, tab_in,
    load_sem, halo_send, halo_recv, side_send, side_recv, corner_send, corner_recv,
    tab_send, tab_recv,
):
    me_r, me_c = lax.axis_index("rows"), lax.axis_index("cols")
    height, width = flags.shape
    tiles = width // LANES
    low = height - EDGE
    total_rows, total_cols = height * n_rows, width * n_cols
    chunk = 512 if width % 512 == 0 else LANES
    has_up, has_down = me_r > 0, me_r < n_rows - 1
    has_left, has_right = me_c > 0, me_c < n_cols - 1
    pieces = chunk_tiles(tiles)
    early = max(1, len(pieces) // 2)

    def load(part, rows):
        group = [
            pltpu.make_async_copy(lead.at[:, rows, :], av.at[:, rows, :], load_sem.at[part, 0]),
            pltpu.make_async_copy(trail.at[:, rows, :], bv.at[:, rows, :], load_sem.at[part, 1]),
            pltpu.make_async_copy(flags.at[rows, :], wv.at[rows, :], load_sem.at[part, 2]),
        ]
        for copy in group:
            copy.start()
        return group

    loads = [load(0, pl.ds(low, EDGE)), load(1, pl.ds(0, EDGE)), load(2, pl.ds(EDGE, low - EDGE))]
    sweep_load = pltpu.make_async_copy(sweep, sv, load_sem.at[3, 0])
    sweep_load.start()

    barrier = pltpu.get_barrier_semaphore()
    peers = []
    for dr in range(-reach, reach + 1):
        for dc in range(n_cols):
            if dr == 0 and dc == 0:
                continue
            to = jnp.logical_and(me_r + dr >= 0, me_r + dr < n_rows)
            of = jnp.logical_and(me_r - dr >= 0, me_r - dr < n_rows)
            peers.append(((dr + reach) * n_cols + dc, to, of, me_r + dr, lax.rem(me_c + dc, n_cols)))
    for _, to, _, row, col in peers:
        @pl.when(to)
        def _():
            pl.semaphore_signal(barrier, inc=1, device_id=(row, col), device_id_type=MESH)

    n_peers = (jnp.minimum(me_r, reach) + jnp.minimum(n_rows - 1 - me_r, reach) + 1) * n_cols - 1

    def remote(src, dst, send, recv, row, col):
        return pltpu.make_async_remote_copy(
            src_ref=src, dst_ref=dst, send_sem=send, recv_sem=recv, device_id=(row, col), device_id_type=MESH
        )

    def cut(ref, piece):
        return ref.at[:, :, pl.ds(piece[0] * LANES, (piece[1] - piece[0]) * LANES)]

    downs = [
        remote(cut(down_out, p), cut(top_in, p), halo_send.at[0, i], halo_recv.at[0, i], me_r + 1, me_c)
        for i, p in enumerate(pieces)
    ]
    ups = [
        remote(cut(up_out, p), cut(bot_in, p), halo_send.at[1, i], halo_recv.at[1, i], me_r - 1, me_c)
        for i, p in enumerate(pieces)
    ]
    to_right = remote(right_out, left_in, side_send.at[0], side_recv.at[0], me_r, me_c + 1)
    to_left = remote(left_out, right_in, side_send.at[1], side_recv.at[1], me_r, me_c - 1)
    corner_down = remote(
        corner.at[pl.ds(low, EDGE)], corner_top, corner_send.at[0], corner_recv.at[0], me_r + 1, me_c
    )
    corner_up = remote(
        corner.at[pl.ds(0, EDGE)], corner_bot, corner_send.at[1], corner_recv.at[1], me_r - 1, me_c
    )

    def encode_rows(first, out, piece):
        lanes = pl.ds(piece[0] * LANES, (piece[1] - piece[0]) * LANES)
        for k, value in enumerate(encode(*masked(av, bv, wv, pl.ds(first, EDGE), lanes))):
            out[k, :, lanes] = value

    def send_piece(i):
        @pl.when(has_down)
        def _():
            downs[i].start()

        @pl.when(has_up)
        def _():
            ups[i].start()

    for copy in loads[0]:
        copy.wait()
    encode_rows(low, down_out, pieces[0])
    for copy in loads[1]:
        copy.wait()
    encode_rows(0, up_out, pieces[0])

    pl.semaphore_wait(barrier, n_peers)
    send_piece(0)
    for i in range(1, len(pieces)):
        encode_rows(low, down_out, pieces[i])
        encode_rows(0, up_out, pieces[i])
        if i < early:
            send_piece(i)

    for copy in loads[2]:
        copy.wait()

    @pl.loop(0, height // 16)
    def _(b):
        rows = pl.ds(pl.multiple_of(b * 16, 16), 16)
        lane = lax.broadcasted_iota(jnp.int32, (16, LANES), 1)
        s, gr, gi = encode(*masked(av, bv, wv, rows, pl.ds(width - LANES, LANES)))
        right_out[rows, :] = jnp.where(
            lane >= LANES - SIDE,
            s,
            jnp.where(
                lane >= LANES - 2 * SIDE,
                pltpu.roll(gr, LANES - SIDE, 1),
                jnp.where(lane >= LANES - 3 * SIDE, pltpu.roll(gi, LANES - 2 * SIDE, 1), 0.0),
            ),
        )
        s, gr, gi = encode(*masked(av, bv, wv, rows, pl.ds(0, LANES)))
        left_out[rows, :] = jnp.where(
            lane < SIDE,
            s,
            jnp.where(
                lane < 2 * SIDE,
                pltpu.roll(gr, SIDE, 1),
                jnp.where(lane < 3 * SIDE, pltpu.roll(gi, 2 * SIDE, 1), 0.0),
            ),
        )

    @pl.when(has_right)
    def _():
        to_right.start()

    @pl.when(has_left)
    def _():
        to_left.start()

    @pl.when(jnp.logical_not(has_left))
    def _():
        left_in[...] = jnp.zeros_like(left_in)

    @pl.when(jnp.logical_not(has_right))
    def _():
        right_in[...] = jnp.zeros_like(right_in)

    @pl.when(jnp.logical_not(has_up))
    def _():
        top_in[...] = jnp.zeros_like(top_in)
        corner_top[...] = jnp.zeros_like(corner_top)

    @pl.when(jnp.logical_not(has_down))
    def _():
        bot_in[...] = jnp.zeros_like(bot_in)
        corner_bot[...] = jnp.zeros_like(corner_bot)

    for slot, _, of, _, _ in peers:
        @pl.when(jnp.logical_not(of))
        def _():
            tab_in[slot] = jnp.zeros((1, 2 * LANES), F32)

    @pl.loop(0, height // 16)
    def _(b):
        rows = pl.ds(pl.multiple_of(b * 16, 16), 16)
        low_rows = pl.ds(pl.multiple_of(height + b * 16, 16), 16)

        @pl.loop(0, width // chunk)
        def _(c):
            lanes = pl.ds(pl.multiple_of(c * chunk, chunk), chunk)
            ar, ai, br, bi = masked(av, bv, wv, rows, lanes)
            put_split(
                split,
                (ar * br + ai * bi, ai * br - ar * bi, ar * ar + ai * ai, br * br + bi * bi),
                [pl.ds(pl.multiple_of(LANES + c * chunk, LANES), chunk)], rows, low_rows,
            )

    @pl.when(has_left)
    def _():
        to_right.wait_recv()

    @pl.when(has_right)
    def _():
        to_left.wait_recv()

    sides = [pl.ds(0, LANES), pl.ds(LANES + width, LANES)]

    @pl.loop(0, height // 16)
    def _(b):
        rows = pl.ds(pl.multiple_of(b * 16, 16), 16)
        low_rows = pl.ds(pl.multiple_of(height + b * 16, 16), 16)
        lane = lax.broadcasted_iota(jnp.int32, (16, LANES), 1)
        pack = jnp.where(lane >= LANES // 2, left_in[rows, :], right_in[rows, :])
        corner[rows, :] = pack
        put_split(split, decode(*edge_block(pack)), sides, rows, low_rows)

    @pl.when(has_down)
    def _():
        corner_down.start()

    @pl.when(has_up)
    def _():
        corner_up.start()

    for i in range(early, len(pieces)):
        send_piece(i)

    sweep_load.wait()
    lane_all = lax.broadcasted_iota(jnp.int32, (8, width), 1) + me_c * width
    across[...] = (lane_all.astype(F32) + 0.5) * (2.0 / total_cols) - 1.0
    kind = lax.rem(lax.broadcasted_iota(jnp.int32, (LANES, height), 0), SWEEP_TALLY)
    memt[...] = (kind == sv[...]).astype(F32).T
    acc_g[...] = jnp.zeros_like(acc_g)
    acc_h[...] = jnp.zeros_like(acc_h)
    edge_sums[...] = jnp.zeros_like(edge_sums)

    r = lax.broadcasted_iota(jnp.int32, (height, 2 * height), 0)
    k = lax.rem(lax.broadcasted_iota(jnp.int32, (height, 2 * height), 1), height)
    band = jnp.logical_and(k >= r - EDGE, k < r + EDGE).astype(F32).astype(BF16)
    span = 2 * LANES

    @pl.loop(0, (tiles + 2) // 2)
    def _(c):
        lanes = pl.ds(pl.multiple_of(c * span, span), span)
        for plane in range(4):
            vert[plane, :, lanes] = jnp.dot(band, split[plane, :, lanes], preferred_element_type=F32)

    group_lane = lax.broadcasted_iota(jnp.int32, (8, LANES), 1) // SWEEP_TALLY

    def row_v(first):
        row = lax.broadcasted_iota(jnp.int32, (8, LANES), 0) + (me_r * height + first)
        return (row.astype(F32) + 0.5) * (2.0 / total_rows) - 1.0

    def arrange(values):
        table = jnp.zeros((8, LANES), F32)
        for m, value in enumerate(values):
            table = jnp.where(group_lane == m, value, table)
        return table

    def row_sum(x):
        return jnp.sum(x, 1, keepdims=True)

    @pl.loop(0, height // 8)
    def _(b):
        first = pl.multiple_of(b * 8, 8)
        rows = pl.ds(first, 8)
        w = wv[rows, :].astype(F32)
        u = across[...]
        wu = w * u
        s0, su, suu = row_sum(fold(w)), row_sum(fold(wu)), row_sum(fold(wu * u))
        v = row_v(first)
        acc_g[...] += memt[rows, :] * arrange((s0, su, v * s0, suu, v * su, v * v * s0))

    def gamma(rows, t0, n):
        size = (n + 2) * LANES
        lanes = pl.ds(t0 * LANES, size)
        inner = pl.ds(t0 * LANES, n * LANES)

        def across_sum(plane):
            x = vert[plane, rows, lanes]
            x = x + pltpu.roll(x, size - 1, 1)
            x = x + pltpu.roll(x, size - 2, 1)
            return x + pltpu.roll(x, size - 4, 1)

        inverse = lax.rsqrt((across_sum(2) + 1.0) * (across_sum(3) + 1.0))
        real = pltpu.roll(across_sum(0) * inverse, SIDE, 1)[:, LANES : size - LANES]
        imag = pltpu.roll(across_sum(1) * inverse, SIDE, 1)[:, LANES : size - LANES]
        gam[0, rows, inner] = real
        gam[1, rows, inner] = imag
        coh[rows, inner] = jnp.sqrt(real * real + imag * imag)
        w = wv[rows, inner].astype(F32)
        wr, wi = w * real, w * imag
        u = across[:, inner]
        return fold(wr), fold(wi), fold(wr * u), fold(wi * u)

    def add_rows(first, sums):
        hr, hi, hur, hui = [row_sum(x) for x in sums]
        v = row_v(first)
        acc_h[...] += memt[pl.ds(first, 8), :] * arrange((hr, hi, hur, hui, v * hr, v * hi))

    half = tiles // 2 if tiles % 2 == 0 else tiles

    @pl.loop(0, (low - EDGE) // 8)
    def _(b):
        first = pl.multiple_of(EDGE + b * 8, 8)
        parts = [gamma(pl.ds(first, 8), t0, half) for t0 in range(0, tiles, half)]
        add_rows(first, [functools.reduce(jnp.add, x) for x in zip(*parts)])

    r = lax.broadcasted_iota(jnp.int32, (2 * EDGE, 4 * EDGE), 0)
    k = lax.broadcasted_iota(jnp.int32, (2 * EDGE, 4 * EDGE), 1)
    within = lax.rem(k, EDGE)
    upper = jnp.logical_and(jnp.logical_and(r < EDGE, k < 2 * EDGE), within >= r)
    lower = jnp.logical_and(jnp.logical_and(r >= EDGE, k >= 2 * EDGE), within < r - EDGE)
    reach_rows = jnp.logical_or(upper, lower).astype(F32).astype(BF16)

    def add_halo(sources, where):
        for part, products in enumerate(sources):
            put_split(
                halo_split, products, [where],
                pl.ds(2 * part * EDGE, EDGE), pl.ds((2 * part + 1) * EDGE, EDGE),
            )
        for plane in range(4):
            extra = jnp.dot(reach_rows, halo_split[plane, :, where], preferred_element_type=F32)
            vert[plane, 0:EDGE, where] += extra[:EDGE]
            vert[plane, low:height, where] += extra[EDGE:]

    def finish_edges(t0, n):
        @pl.loop(0, 2 * EDGE // 8)
        def _(b):
            first = pl.multiple_of(b * 8 + (b // (EDGE // 8)) * (low - EDGE), 8)
            for m, value in enumerate(gamma(pl.ds(first, 8), t0, n)):
                edge_sums[b, m] += value

    done = 1
    for i, piece in enumerate(pieces):
        if i == min(early, len(pieces) - 1):
            @pl.when(has_up)
            def _():
                corner_down.wait_recv()

            @pl.when(has_down)
            def _():
                corner_up.wait_recv()

            for where in sides:
                add_halo([decode(*edge_block(pack[...])) for pack in (corner_top, corner_bot)], where)

        @pl.when(has_up)
        def _():
            downs[i].wait_recv()

        @pl.when(has_down)
        def _():
            ups[i].wait_recv()

        source = pl.ds(piece[0] * LANES, (piece[1] - piece[0]) * LANES)
        target = pl.ds((piece[0] + 1) * LANES, (piece[1] - piece[0]) * LANES)
        add_halo([decode(*[halo[m, :, source] for m in range(3)]) for halo in (top_in, bot_in)], target)
        if i == min(early, len(pieces) - 1):
            finish_edges(0, 1)
        ready = tiles if i == len(pieces) - 1 else piece[1] - 1
        if ready > done:
            finish_edges(done, ready - done)
            done = ready

    for b in range(2 * EDGE // 8):
        first = b * 8 + (b // (EDGE // 8)) * (low - EDGE)
        add_rows(first, [edge_sums[b, m] for m in range(4)])

    tab_out[:, 0:LANES] = jnp.sum(acc_g[...], 0, keepdims=True)
    tab_out[:, LANES:] = jnp.sum(acc_h[...], 0, keepdims=True)
    swaps = [
        (remote(tab_out, tab_in.at[slot], tab_send.at[slot], tab_recv.at[slot], row, col), to, of)
        for slot, to, of, row, col in peers
    ]
    for copy, to, _ in swaps:
        @pl.when(to)
        def _():
            copy.start()

    tab_in[reach * n_cols] = tab_out[...]
    for copy, _, of in swaps:
        @pl.when(of)
        def _():
            copy.wait_recv()

    total = functools.reduce(jnp.add, [tab_in[slot] for slot in range(tab_in.shape[0])])

    def column(base, m):
        part = total[:, base : base + LANES]
        return part if m == 0 else pltpu.roll(part, LANES - m * SWEEP_TALLY, 1)

    s0, su, sv_, suu, suv, svv = [column(0, m) for m in range(6)]
    hr, hi, hur, hui, hvr, hvi = [column(LANES, m) for m in range(6)]
    floored = jnp.maximum(s0, 1.0)
    mid_u, mid_v = su / floored, sv_ / floored
    guu = suu - 2.0 * mid_u * su + mid_u * mid_u * s0
    guv = suv - mid_u * sv_ - mid_v * su + mid_u * mid_v * s0
    gvv = svv - 2.0 * mid_v * sv_ + mid_v * mid_v * s0
    hur, hui = hur - mid_u * hr, hui - mid_u * hi
    hvr, hvi = hvr - mid_v * hr, hvi - mid_v * hi
    ridge = 0.001 * s0 + 1.0
    duu, dvv = guu + ridge, gvv + ridge
    scale = 1.0 / (duu * dvv - guv * guv)
    base = 1.0 / (s0 + ridge)
    c1r, c1i = (dvv * hur - guv * hvr) * scale, (dvv * hui - guv * hvi) * scale
    c2r, c2i = (duu * hvr - guv * hur) * scale, (duu * hvi - guv * hui) * scale
    valid = lax.broadcasted_iota(jnp.int32, (1, LANES), 1) < SWEEP_TALLY
    rows_out = (hr * base - c1r * mid_u, hi * base - c1i * mid_u, c1r, c1i, c2r, c2i, mid_v)
    for m, value in enumerate(rows_out):
        fit[m : m + 1, :] = jnp.where(valid, value, 0.0)

    @pl.when(has_down)
    def _():
        for copy in downs:
            copy.wait_send()
        corner_down.wait_send()

    @pl.when(has_up)
    def _():
        for copy in ups:
            copy.wait_send()
        corner_up.wait_send()

    @pl.when(has_right)
    def _():
        to_right.wait_send()

    @pl.when(has_left)
    def _():
        to_left.wait_send()

    for copy, to, _ in swaps:
        @pl.when(to)
        def _():
            copy.wait_send()


def back_kernel(n_rows, n_cols, block, gam, coh, memt, fit, ramped, coherence, out, across, sem):
    height, width = coh.shape
    me_r, me_c = lax.axis_index("rows"), lax.axis_index("cols")
    coh_copy = pltpu.make_async_copy(coh, coherence, sem.at[0])
    coh_copy.start()
    lane_all = lax.broadcasted_iota(jnp.int32, (8, width), 1) + me_c * width
    across[...] = (lane_all.astype(F32) + 0.5) * (2.0 / (width * n_cols)) - 1.0

    def row_sum(x):
        return jnp.sum(x, 1, keepdims=True)

    copies = []
    for i in range(height // block):
        @pl.loop(0, block // 8)
        def _(b):
            first = pl.multiple_of(i * block + b * 8, 8)
            rows = pl.ds(first, 8)
            row = lax.broadcasted_iota(jnp.int32, (8, LANES), 0) + (me_r * height + first)
            v = (row.astype(F32) + 0.5) * (2.0 / (height * n_rows)) - 1.0
            one = memt[rows, :]
            dv = v - fit[6:7, :]
            base_r = row_sum(one * (fit[0:1, :] + fit[4:5, :] * dv))
            base_i = row_sum(one * (fit[1:2, :] + fit[5:6, :] * dv))
            slope_r = row_sum(one * fit[2:3, :])
            slope_i = row_sum(one * fit[3:4, :])
            real, imag = gam[0, rows, :], gam[1, rows, :]
            u = across[...]
            model_real = base_r + slope_r * u
            model_imag = base_i + slope_i * u
            out[0, rows, :] = real * model_real + imag * model_imag
            out[1, rows, :] = imag * model_real - real * model_imag

        rows = pl.ds(i * block, block)
        copy = pltpu.make_async_copy(out.at[:, rows, :], ramped.at[:, rows, :], sem.at[1 + i])
        copy.start()
        copies.append(copy)
    coh_copy.wait()
    for copy in copies:
        copy.wait()


def on_device(n_rows, n_cols, lead, trail, flags, sweep):
    height, width = flags.shape
    wide = width + 2 * LANES
    longest = 2 * height * n_rows // SWEEP_TALLY
    reach = max(1, min(n_rows - 1, (longest - 2) // height + 1))
    slots = (2 * reach + 1) * n_cols
    pieces = len(chunk_tiles(width // LANES))
    hbm = pl.BlockSpec(memory_space=pltpu.HBM)
    vmem = pl.BlockSpec(memory_space=pltpu.VMEM)
    dma = pltpu.SemaphoreType.DMA
    gam, coh, memt, fit = pl.pallas_call(
        functools.partial(front_kernel, n_rows, n_cols, reach),
        out_shape=[
            pltpu.VMEM((2, height, width), F32),
            pltpu.VMEM((height, width), F32),
            pltpu.VMEM((height, LANES), F32),
            pltpu.VMEM((8, LANES), F32),
        ],
        in_specs=[hbm, hbm, hbm, hbm],
        out_specs=[vmem, vmem, vmem, vmem],
        scratch_shapes=[
            pltpu.VMEM((2, height, width), F32),
            pltpu.VMEM((2, height, width), F32),
            pltpu.VMEM((height, width), jnp.int32),
            pltpu.VMEM((1, height), jnp.int32),
            pltpu.VMEM((3, EDGE, width), F32),
            pltpu.VMEM((3, EDGE, width), F32),
            pltpu.VMEM((3, EDGE, width), F32),
            pltpu.VMEM((3, EDGE, width), F32),
            pltpu.VMEM((height, LANES), F32),
            pltpu.VMEM((height, LANES), F32),
            pltpu.VMEM((height, LANES), F32),
            pltpu.VMEM((height, LANES), F32),
            pltpu.VMEM((height, LANES), F32),
            pltpu.VMEM((EDGE, LANES), F32),
            pltpu.VMEM((EDGE, LANES), F32),
            pltpu.VMEM((4, 2 * height, wide), BF16),
            pltpu.VMEM((4, 4 * EDGE, wide), BF16),
            pltpu.VMEM((4, height, wide), F32),
            pltpu.VMEM((8, width), F32),
            pltpu.VMEM((2 * EDGE // 8, 4, 8, LANES), F32),
            pltpu.VMEM((8, LANES), F32),
            pltpu.VMEM((8, LANES), F32),
            pltpu.VMEM((1, 2 * LANES), F32),
            pltpu.VMEM((slots, 1, 2 * LANES), F32),
            dma((4, 3)),
            dma((2, pieces)), dma((2, pieces)),
            dma((2,)), dma((2,)),
            dma((2,)), dma((2,)),
            dma((slots,)), dma((slots,)),
        ],
        compiler_params=pltpu.CompilerParams(
            collective_id=0, has_side_effects=True, vmem_limit_bytes=60 * 1024 * 1024
        ),
        name="front",
    )(lead, trail, flags, sweep.reshape(1, height))
    block = 16 if height % 16 == 0 else 8
    return pl.pallas_call(
        functools.partial(back_kernel, n_rows, n_cols, block),
        out_shape=[
            jax.ShapeDtypeStruct((2, height, width), F32),
            jax.ShapeDtypeStruct((height, width), F32),
        ],
        in_specs=[vmem, vmem, vmem, vmem],
        out_specs=[hbm, hbm],
        scratch_shapes=[
            pltpu.VMEM((2, height, width), F32),
            pltpu.VMEM((8, width), F32),
            dma((1 + height // block,)),
        ],
        compiler_params=pltpu.CompilerParams(vmem_limit_bytes=16 * 1024 * 1024),
        name="back",
    )(gam, coh, memt, fit)


def solution(mesh):
    return jax.shard_map(
        functools.partial(on_device, mesh.shape["rows"], mesh.shape["cols"]),
        mesh=mesh,
        in_specs=(P(None, "rows", "cols"), P(None, "rows", "cols"), P("rows", "cols"), P("rows")),
        out_specs=(P(None, "rows", "cols"), P("rows", "cols")),
        check_vma=False,
    )
```

```python
import functools

import jax
import jax.numpy as jnp
from jax import lax
from jax.experimental import pallas as pl
from jax.experimental.pallas import tpu as pltpu
from jax.sharding import PartitionSpec as P

WIN_R = 32
WIN_C = 8
SWEEP_TALLY = 16

EDGE = WIN_R // 2
SIDE = WIN_C // 2
LANES = 128
SCALE = 2.0**56
FLOOR = 1e-36
F32 = jnp.float32
BF16 = jnp.bfloat16
MESH = pl.DeviceIdType.MESH


def masked(av, bv, wv, rows, lanes):
    w = wv[rows, lanes].astype(F32)
    return av[0, rows, lanes] * w, av[1, rows, lanes] * w, bv[0, rows, lanes] * w, bv[1, rows, lanes] * w


def encode(ar, ai, br, bi):
    sr, si = ar * SCALE, ai * SCALE
    power = sr * sr + si * si
    some = power > FLOOR
    inverse = lax.rsqrt(jnp.where(some, power, 1.0))
    return (
        jnp.where(some, power * inverse * (1.0 / SCALE), 0.0),
        jnp.where(some, (sr * br + si * bi) * inverse, br),
        jnp.where(some, (si * br - sr * bi) * inverse, bi),
    )


def decode(s, gr, gi):
    return s * gr, s * gi, s * s, gr * gr + gi * gi


def put_split(out, products, places):
    for plane, value in enumerate(products):
        high = value.astype(BF16)
        low = (value - high.astype(F32)).astype(BF16)
        for rows, lanes in places:
            out[0, plane, rows, lanes] = high
            out[1, plane, rows, lanes] = low


def edge_block(pack):
    lane = lax.broadcasted_iota(jnp.int32, pack.shape, 1)
    left, right = lane >= LANES - SIDE, lane < SIDE

    def pick(k):
        a = pack if k == 0 else pltpu.roll(pack, k * SIDE, 1)
        b = pack if k == 0 else pltpu.roll(pack, LANES - k * SIDE, 1)
        return jnp.where(left, a, jnp.where(right, b, 0.0))

    return pick(0), pick(1), pick(2)


def cuts(tiles):
    if tiles < 8:
        return ((0, tiles),)
    marks = [0, tiles // 4, tiles // 2, tiles * 3 // 4, tiles - 1, tiles]
    return tuple(zip(marks[:-1], marks[1:]))


def fold(x):
    total = x[:, 0:LANES]
    for t in range(1, x.shape[1] // LANES):
        total = total + x[:, t * LANES : (t + 1) * LANES]
    return total


def row_sum(x):
    return jnp.sum(x, 1, keepdims=True)


def front_kernel(
    n_rows, n_cols, reach,
    lead, trail, flags, sweep,
    gam, coh, memt, fit,
    av, bv, wv, sv, up_out, down_out, top_in, bot_in, left_out, right_out, left_in, right_in,
    corner, corner_top, corner_bot, split, halo_split, boxed, ribbon, across, row_parts, flag_parts, acc_h,
    tab_out, tab_in,
    load_sem, halo_send, halo_recv, side_send, side_recv, corner_send, corner_recv,
    tab_send, tab_recv,
):
    me_r, me_c = lax.axis_index("rows"), lax.axis_index("cols")
    height, width = flags.shape
    tiles = width // LANES
    low = height - EDGE
    total_rows, total_cols = height * n_rows, width * n_cols
    chunk = 512 if width % 512 == 0 else LANES
    has_up, has_down = me_r > 0, me_r < n_rows - 1
    has_left, has_right = me_c > 0, me_c < n_cols - 1
    pieces = cuts(tiles)
    early = max(1, len(pieces) // 2)
    pair = 2 if tiles % 2 == 0 else 1

    def load(part, rows):
        group = [
            pltpu.make_async_copy(lead.at[:, rows, :], av.at[:, rows, :], load_sem.at[part, 0]),
            pltpu.make_async_copy(trail.at[:, rows, :], bv.at[:, rows, :], load_sem.at[part, 1]),
            pltpu.make_async_copy(flags.at[rows, :], wv.at[rows, :], load_sem.at[part, 2]),
        ]
        for copy in group:
            copy.start()
        return group

    loads = [load(0, pl.ds(low, EDGE)), load(1, pl.ds(0, EDGE)), load(2, pl.ds(EDGE, low - EDGE))]
    sweep_load = pltpu.make_async_copy(sweep, sv, load_sem.at[3, 0])
    sweep_load.start()

    barrier = pltpu.get_barrier_semaphore()
    peers = []
    for dr in range(-reach, reach + 1):
        for dc in range(n_cols):
            if dr == 0 and dc == 0:
                continue
            to = jnp.logical_and(me_r + dr >= 0, me_r + dr < n_rows)
            of = jnp.logical_and(me_r - dr >= 0, me_r - dr < n_rows)
            peers.append(((dr + reach) * n_cols + dc, to, of, me_r + dr, lax.rem(me_c + dc, n_cols)))
    for _, to, _, row, col in peers:
        @pl.when(to)
        def _():
            pl.semaphore_signal(barrier, inc=1, device_id=(row, col), device_id_type=MESH)

    n_peers = (jnp.minimum(me_r, reach) + jnp.minimum(n_rows - 1 - me_r, reach) + 1) * n_cols - 1

    def remote(src, dst, send, recv, row, col):
        return pltpu.make_async_remote_copy(
            src_ref=src, dst_ref=dst, send_sem=send, recv_sem=recv, device_id=(row, col), device_id_type=MESH
        )

    def cut(ref, piece):
        return ref.at[:, :, pl.ds(piece[0] * LANES, (piece[1] - piece[0]) * LANES)]

    downs = [
        remote(cut(down_out, p), cut(top_in, p), halo_send.at[0, i], halo_recv.at[0, i], me_r + 1, me_c)
        for i, p in enumerate(pieces)
    ]
    ups = [
        remote(cut(up_out, p), cut(bot_in, p), halo_send.at[1, i], halo_recv.at[1, i], me_r - 1, me_c)
        for i, p in enumerate(pieces)
    ]
    to_right = remote(right_out, left_in, side_send.at[0], side_recv.at[0], me_r, me_c + 1)
    to_left = remote(left_out, right_in, side_send.at[1], side_recv.at[1], me_r, me_c - 1)
    corner_down = remote(
        corner.at[pl.ds(low, EDGE)], corner_top, corner_send.at[0], corner_recv.at[0], me_r + 1, me_c
    )
    corner_up = remote(
        corner.at[pl.ds(0, EDGE)], corner_bot, corner_send.at[1], corner_recv.at[1], me_r - 1, me_c
    )

    def encode_rows(first, out, piece):
        lanes = pl.ds(piece[0] * LANES, (piece[1] - piece[0]) * LANES)
        for k, value in enumerate(encode(*masked(av, bv, wv, pl.ds(first, EDGE), lanes))):
            out[k, :, lanes] = value

    def send_piece(i):
        @pl.when(has_down)
        def _():
            downs[i].start()

        @pl.when(has_up)
        def _():
            ups[i].start()

    for copy in loads[0]:
        copy.wait()
    encode_rows(low, down_out, pieces[0])
    for copy in loads[1]:
        copy.wait()
    encode_rows(0, up_out, pieces[0])

    pl.semaphore_wait(barrier, n_peers)
    send_piece(0)
    for i in range(1, len(pieces)):
        encode_rows(low, down_out, pieces[i])
        encode_rows(0, up_out, pieces[i])
        if i < early:
            send_piece(i)

    for copy in loads[2]:
        copy.wait()

    for b in range(height // 16):
        rows = pl.ds(b * 16, 16)
        lane = lax.broadcasted_iota(jnp.int32, (16, LANES), 1)
        s, gr, gi = encode(*masked(av, bv, wv, rows, pl.ds(width - LANES, LANES)))
        right_out[rows, :] = jnp.where(
            lane >= LANES - SIDE,
            s,
            jnp.where(
                lane >= LANES - 2 * SIDE,
                pltpu.roll(gr, LANES - SIDE, 1),
                jnp.where(lane >= LANES - 3 * SIDE, pltpu.roll(gi, LANES - 2 * SIDE, 1), 0.0),
            ),
        )
        s, gr, gi = encode(*masked(av, bv, wv, rows, pl.ds(0, LANES)))
        left_out[rows, :] = jnp.where(
            lane < SIDE,
            s,
            jnp.where(
                lane < 2 * SIDE,
                pltpu.roll(gr, SIDE, 1),
                jnp.where(lane < 3 * SIDE, pltpu.roll(gi, 2 * SIDE, 1), 0.0),
            ),
        )

    @pl.when(has_right)
    def _():
        to_right.start()

    @pl.when(has_left)
    def _():
        to_left.start()

    @pl.when(jnp.logical_not(has_left))
    def _():
        left_in[...] = jnp.zeros_like(left_in)

    @pl.when(jnp.logical_not(has_right))
    def _():
        right_in[...] = jnp.zeros_like(right_in)

    @pl.when(jnp.logical_not(has_up))
    def _():
        top_in[...] = jnp.zeros_like(top_in)
        corner_top[...] = jnp.zeros_like(corner_top)

    @pl.when(jnp.logical_not(has_down))
    def _():
        bot_in[...] = jnp.zeros_like(bot_in)
        corner_bot[...] = jnp.zeros_like(corner_bot)

    for slot, _, of, _, _ in peers:
        @pl.when(jnp.logical_not(of))
        def _():
            tab_in[slot] = jnp.zeros((1, 2 * LANES), F32)

    lane_all = lax.broadcasted_iota(jnp.int32, (8, width), 1) + me_c * width
    across[...] = (lane_all.astype(F32) + 0.5) * (2.0 / total_cols) - 1.0

    @pl.loop(0, height // 16)
    def _(b):
        rows = pl.ds(pl.multiple_of(b * 16, 16), 16)

        @pl.loop(0, width // chunk)
        def _(c):
            lanes = pl.ds(pl.multiple_of(c * chunk, chunk), chunk)
            ar, ai, br, bi = masked(av, bv, wv, rows, lanes)
            put_split(
                split,
                (ar * br + ai * bi, ai * br - ar * bi, ar * ar + ai * ai, br * br + bi * bi),
                [(rows, pl.ds(pl.multiple_of(LANES + c * chunk, LANES), chunk))],
            )

    reach_in = (pair + 2) * LANES
    i = lax.broadcasted_iota(jnp.int32, (reach_in, pair * LANES), 0)
    j = lax.broadcasted_iota(jnp.int32, (reach_in, pair * LANES), 1) + LANES
    ribbon[...] = jnp.logical_and(i >= j - SIDE, i < j + SIDE).astype(F32).astype(BF16)

    def box_across(source, j, targets):
        inner = pl.ds(pl.multiple_of(j * pair * LANES, pair * LANES), reach_in)
        outer = pl.ds(pl.multiple_of(j * pair * LANES, pair * LANES), pair * LANES)
        for plane in range(4):
            sums = jnp.dot(source[0, plane, :, inner], ribbon[...], preferred_element_type=F32)
            sums = sums + jnp.dot(source[1, plane, :, inner], ribbon[...], preferred_element_type=F32)
            for first, target, count in targets:
                boxed[plane, target : target + count, outer] = sums[first : first + count]

    own = [(0, EDGE, height)]

    @pl.loop(1, max(1, tiles // pair - 1))
    def _(j):
        box_across(split, j, own)

    @pl.when(has_left)
    def _():
        to_right.wait_recv()

    @pl.when(has_right)
    def _():
        to_left.wait_recv()

    sides = [pl.ds(0, LANES), pl.ds(LANES + width, LANES)]
    for b in range(height // 16):
        rows = pl.ds(b * 16, 16)
        lane = lax.broadcasted_iota(jnp.int32, (16, LANES), 1)
        pack = jnp.where(lane >= LANES // 2, left_in[rows, :], right_in[rows, :])
        corner[rows, :] = pack
        put_split(split, decode(*edge_block(pack)), [(rows, lanes) for lanes in sides])

    @pl.when(has_down)
    def _():
        corner_down.start()

    @pl.when(has_up)
    def _():
        corner_up.start()

    for i in range(early, len(pieces)):
        send_piece(i)

    for j in sorted({0, tiles // pair - 1}):
        box_across(split, j, own)

    sweep_load.wait()
    kind = lax.rem(lax.broadcasted_iota(jnp.int32, (LANES, height), 0), SWEEP_TALLY)
    memt[...] = (kind == sv[...]).astype(F32).T
    row_parts[...] = jnp.zeros_like(row_parts)

    group_lane = lax.broadcasted_iota(jnp.int32, (8, LANES), 1) // SWEEP_TALLY

    def row_v(group):
        row = lax.broadcasted_iota(jnp.int32, (8, LANES), 0) + (me_r * height + group * 8)
        return (row.astype(F32) + 0.5) * (2.0 / total_rows) - 1.0

    def arrange(group, values):
        table = values[0]
        for m, value in enumerate(values):
            table = value if m == 0 else jnp.where(group_lane >= m, value, table)
        return memt[group * 8 : group * 8 + 8, :] * jnp.where(group_lane < len(values), table, 0.0)

    @pl.loop(0, height // 8)
    def _(b):
        w = wv[pl.ds(pl.multiple_of(b * 8, 8), 8), :].astype(F32)
        u = across[...]
        wu = w * u
        for m, value in enumerate((w, wu, wu * u)):
            flag_parts[b, m] = fold(value)

    acc_g = None
    for b in range(height // 8):
        s0, su, suu = [row_sum(flag_parts[b, m]) for m in range(3)]
        v = row_v(b)
        part = arrange(b, (s0, su, v * s0, suu, v * su, v * v * s0))
        acc_g = part if acc_g is None else acc_g + part
    tab_out[:, 0:LANES] = jnp.sum(acc_g, 0, keepdims=True)

    sub = lax.broadcasted_iota(jnp.int32, (8, LANES), 0)

    def finish(t, top, bottom):
        lanes = pl.ds(pl.multiple_of(t * LANES, LANES), LANES)
        u = across[:, lanes]
        state = [None] * 4
        for g in range(bottom + 3, top - 1, -1):
            window = []
            for plane in range(4):
                x = boxed[plane, g * 8 : g * 8 + 8, lanes]
                r1 = pltpu.roll(x, 7, 0)
                if state[plane] is None:
                    state[plane] = (r1, None, None, None, None, None)
                    y1 = x + r1
                    r2 = pltpu.roll(y1, 6, 0)
                    y2 = y1 + r2
                    r4 = pltpu.roll(y2, 4, 0)
                    state[plane] = (r1, r2, r4, None, None, None)
                    continue
                n1, n2, n4, last, pair1, pair2 = state[plane]
                y1 = x + jnp.where(sub < 7, r1, n1)
                r2 = pltpu.roll(y1, 6, 0)
                y2 = y1 + jnp.where(sub < 6, r2, n2)
                r4 = pltpu.roll(y2, 4, 0)
                y4 = y2 + jnp.where(sub < 4, r4, n4)
                both = None if last is None else y4 + last
                window.append(None if pair2 is None else both + pair2)
                state[plane] = (r1, r2, r4, y4, both, pair1)
            if len(window) < 4 or window[0] is None:
                continue
            rows = slice(g * 8, g * 8 + 8)
            inverse = lax.rsqrt((window[2] + 1.0) * (window[3] + 1.0))
            real, imag = window[0] * inverse, window[1] * inverse
            gam[0, rows, lanes] = real
            gam[1, rows, lanes] = imag
            coh[rows, lanes] = jnp.sqrt(real * real + imag * imag)
            w = wv[rows, lanes].astype(F32)
            wr, wi = w * real, w * imag
            for m, value in enumerate((wr, wi, wr * u, wi * u)):
                row_parts[g, m] += value

    def add_rows(groups):
        total = None
        for g in groups:
            hr, hi, hur, hui = [row_sum(row_parts[g, m]) for m in range(4)]
            v = row_v(g)
            part = arrange(g, (hr, hi, hur, hui, v * hr, v * hi))
            total = part if total is None else total + part
        return total

    edge_groups, groups = EDGE // 8, height // 8

    @pl.loop(0, tiles)
    def _(t):
        finish(t, edge_groups, groups - edge_groups)

    acc_h[...] = add_rows(range(edge_groups, groups - edge_groups))

    def put_halo(sources, where):
        for part, products in enumerate(sources):
            put_split(halo_split, products, [(pl.ds(part * EDGE, EDGE), lanes) for lanes in where])

    beyond = [(0, 0, EDGE), (EDGE, EDGE + height, EDGE)]
    done = 0
    for i, piece in enumerate(pieces):
        if i == 0:
            @pl.when(has_up)
            def _():
                corner_down.wait_recv()

            @pl.when(has_down)
            def _():
                corner_up.wait_recv()

            put_halo([decode(*edge_block(pack[...])) for pack in (corner_top, corner_bot)], sides)

        @pl.when(has_up)
        def _():
            downs[i].wait_recv()

        @pl.when(has_down)
        def _():
            ups[i].wait_recv()

        source = pl.ds(piece[0] * LANES, (piece[1] - piece[0]) * LANES)
        target = pl.ds((piece[0] + 1) * LANES, (piece[1] - piece[0]) * LANES)
        put_halo([decode(*[halo[m, :, source] for m in range(3)]) for halo in (top_in, bot_in)], [target])
        ready = tiles // pair if i == len(pieces) - 1 else max(0, (piece[1] - 1) // pair)
        for j in range(done, ready):
            box_across(halo_split, j, beyond)
        if ready > done:
            @pl.loop(done * pair, ready * pair)
            def _(t):
                finish(t, 0, edge_groups)
                finish(t, groups - edge_groups, groups)
        done = ready

    acc_last = acc_h[...] + add_rows(list(range(edge_groups)) + list(range(groups - edge_groups, groups)))
    tab_out[:, LANES:] = jnp.sum(acc_last, 0, keepdims=True)
    swaps = [
        (remote(tab_out, tab_in.at[slot], tab_send.at[slot], tab_recv.at[slot], row, col), to, of)
        for slot, to, of, row, col in peers
    ]
    for copy, to, _ in swaps:
        @pl.when(to)
        def _():
            copy.start()

    tab_in[reach * n_cols] = tab_out[...]
    for copy, _, of in swaps:
        @pl.when(of)
        def _():
            copy.wait_recv()

    total = functools.reduce(jnp.add, [tab_in[slot] for slot in range(tab_in.shape[0])])

    def column(base, m):
        part = total[:, base : base + LANES]
        return part if m == 0 else pltpu.roll(part, LANES - m * SWEEP_TALLY, 1)

    s0, su, sv_, suu, suv, svv = [column(0, m) for m in range(6)]
    hr, hi, hur, hui, hvr, hvi = [column(LANES, m) for m in range(6)]
    floored = jnp.maximum(s0, 1.0)
    mid_u, mid_v = su / floored, sv_ / floored
    guu = suu - 2.0 * mid_u * su + mid_u * mid_u * s0
    guv = suv - mid_u * sv_ - mid_v * su + mid_u * mid_v * s0
    gvv = svv - 2.0 * mid_v * sv_ + mid_v * mid_v * s0
    hur, hui = hur - mid_u * hr, hui - mid_u * hi
    hvr, hvi = hvr - mid_v * hr, hvi - mid_v * hi
    ridge = 0.001 * s0 + 1.0
    duu, dvv = guu + ridge, gvv + ridge
    scale = 1.0 / (duu * dvv - guv * guv)
    base = 1.0 / (s0 + ridge)
    c1r, c1i = (dvv * hur - guv * hvr) * scale, (dvv * hui - guv * hvi) * scale
    c2r, c2i = (duu * hvr - guv * hur) * scale, (duu * hvi - guv * hui) * scale
    valid = lax.broadcasted_iota(jnp.int32, (1, LANES), 1) < SWEEP_TALLY
    rows_out = (hr * base - c1r * mid_u, hi * base - c1i * mid_u, c1r, c1i, c2r, c2i, mid_v)
    for m, value in enumerate(rows_out):
        fit[m : m + 1, :] = jnp.where(valid, value, 0.0)

    @pl.when(has_down)
    def _():
        for copy in downs:
            copy.wait_send()
        corner_down.wait_send()

    @pl.when(has_up)
    def _():
        for copy in ups:
            copy.wait_send()
        corner_up.wait_send()

    @pl.when(has_right)
    def _():
        to_right.wait_send()

    @pl.when(has_left)
    def _():
        to_left.wait_send()

    for copy, to, _ in swaps:
        @pl.when(to)
        def _():
            copy.wait_send()


def back_kernel(n_rows, n_cols, block, gam, coh, memt, fit, ramped, coherence, out, across, sem):
    height, width = coh.shape
    me_r, me_c = lax.axis_index("rows"), lax.axis_index("cols")
    coh_copy = pltpu.make_async_copy(coh, coherence, sem.at[0])
    coh_copy.start()
    lane_all = lax.broadcasted_iota(jnp.int32, (8, width), 1) + me_c * width
    across[...] = (lane_all.astype(F32) + 0.5) * (2.0 / (width * n_cols)) - 1.0

    copies = []
    for i in range(height // block):
        @pl.loop(0, block // 8)
        def _(b):
            first = pl.multiple_of(i * block + b * 8, 8)
            rows = pl.ds(first, 8)
            row = lax.broadcasted_iota(jnp.int32, (8, LANES), 0) + (me_r * height + first)
            v = (row.astype(F32) + 0.5) * (2.0 / (height * n_rows)) - 1.0
            one = memt[rows, :]
            dv = v - fit[6:7, :]
            base_r = row_sum(one * (fit[0:1, :] + fit[4:5, :] * dv))
            base_i = row_sum(one * (fit[1:2, :] + fit[5:6, :] * dv))
            slope_r = row_sum(one * fit[2:3, :])
            slope_i = row_sum(one * fit[3:4, :])
            real, imag = gam[0, rows, :], gam[1, rows, :]
            u = across[...]
            model_real = base_r + slope_r * u
            model_imag = base_i + slope_i * u
            out[0, rows, :] = real * model_real + imag * model_imag
            out[1, rows, :] = imag * model_real - real * model_imag

        rows = pl.ds(i * block, block)
        copy = pltpu.make_async_copy(out.at[:, rows, :], ramped.at[:, rows, :], sem.at[1 + i])
        copy.start()
        copies.append(copy)
    coh_copy.wait()
    for copy in copies:
        copy.wait()


def on_device(n_rows, n_cols, lead, trail, flags, sweep):
    height, width = flags.shape
    wide = width + 2 * LANES
    longest = 2 * height * n_rows // SWEEP_TALLY
    reach = max(1, min(n_rows - 1, (longest - 2) // height + 1))
    slots = (2 * reach + 1) * n_cols
    pieces = len(cuts(width // LANES))
    pair = 2 if width // LANES % 2 == 0 else 1
    hbm = pl.BlockSpec(memory_space=pltpu.HBM)
    vmem = pl.BlockSpec(memory_space=pltpu.VMEM)
    dma = pltpu.SemaphoreType.DMA
    gam, coh, memt, fit = pl.pallas_call(
        functools.partial(front_kernel, n_rows, n_cols, reach),
        out_shape=[
            pltpu.VMEM((2, height, width), F32),
            pltpu.VMEM((height, width), F32),
            pltpu.VMEM((height, LANES), F32),
            pltpu.VMEM((8, LANES), F32),
        ],
        in_specs=[hbm, hbm, hbm, hbm],
        out_specs=[vmem, vmem, vmem, vmem],
        scratch_shapes=[
            pltpu.VMEM((2, height, width), F32),
            pltpu.VMEM((2, height, width), F32),
            pltpu.VMEM((height, width), jnp.int32),
            pltpu.VMEM((1, height), jnp.int32),
            pltpu.VMEM((3, EDGE, width), F32),
            pltpu.VMEM((3, EDGE, width), F32),
            pltpu.VMEM((3, EDGE, width), F32),
            pltpu.VMEM((3, EDGE, width), F32),
            pltpu.VMEM((height, LANES), F32),
            pltpu.VMEM((height, LANES), F32),
            pltpu.VMEM((height, LANES), F32),
            pltpu.VMEM((height, LANES), F32),
            pltpu.VMEM((height, LANES), F32),
            pltpu.VMEM((EDGE, LANES), F32),
            pltpu.VMEM((EDGE, LANES), F32),
            pltpu.VMEM((2, 4, height, wide), BF16),
            pltpu.VMEM((2, 4, 2 * EDGE, wide), BF16),
            pltpu.VMEM((4, height + 2 * EDGE, width), F32),
            pltpu.VMEM(((pair + 2) * LANES, pair * LANES), BF16),
            pltpu.VMEM((8, width), F32),
            pltpu.VMEM((height // 8, 4, 8, LANES), F32),
            pltpu.VMEM((height // 8, 3, 8, LANES), F32),
            pltpu.VMEM((8, LANES), F32),
            pltpu.VMEM((1, 2 * LANES), F32),
            pltpu.VMEM((slots, 1, 2 * LANES), F32),
            dma((4, 3)),
            dma((2, pieces)), dma((2, pieces)),
            dma((2,)), dma((2,)),
            dma((2,)), dma((2,)),
            dma((slots,)), dma((slots,)),
        ],
        compiler_params=pltpu.CompilerParams(
            collective_id=0, has_side_effects=True, vmem_limit_bytes=60 * 1024 * 1024
        ),
        name="front",
    )(lead, trail, flags, sweep.reshape(1, height))
    block = 16 if height % 16 == 0 else 8
    return pl.pallas_call(
        functools.partial(back_kernel, n_rows, n_cols, block),
        out_shape=[
            jax.ShapeDtypeStruct((2, height, width), F32),
            jax.ShapeDtypeStruct((height, width), F32),
        ],
        in_specs=[vmem, vmem, vmem, vmem],
        out_specs=[hbm, hbm],
        scratch_shapes=[
            pltpu.VMEM((2, height, width), F32),
            pltpu.VMEM((8, width), F32),
            dma((1 + height // block,)),
        ],
        compiler_params=pltpu.CompilerParams(vmem_limit_bytes=16 * 1024 * 1024),
        name="back",
    )(gam, coh, memt, fit)


def solution(mesh):
    return jax.shard_map(
        functools.partial(on_device, mesh.shape["rows"], mesh.shape["cols"]),
        mesh=mesh,
        in_specs=(P(None, "rows", "cols"), P(None, "rows", "cols"), P("rows", "cols"), P("rows")),
        out_specs=(P(None, "rows", "cols"), P("rows", "cols")),
        check_vma=False,
    )
```

```python
import functools

import jax
import jax.numpy as jnp
from jax import lax
from jax.experimental import pallas as pl
from jax.experimental.pallas import tpu as pltpu
from jax.sharding import PartitionSpec as P

WIN_R = 32
WIN_C = 8
SWEEP_TALLY = 16

EDGE = WIN_R // 2
SIDE = WIN_C // 2
LANES = 128
SCALE = 2.0**56
FLOOR = 1e-36
F32 = jnp.float32
BF16 = jnp.bfloat16
MESH = pl.DeviceIdType.MESH


def masked(av, bv, wv, rows, lanes):
    w = wv[rows, lanes].astype(F32)
    return av[0, rows, lanes] * w, av[1, rows, lanes] * w, bv[0, rows, lanes] * w, bv[1, rows, lanes] * w


def encode(ar, ai, br, bi):
    sr, si = ar * SCALE, ai * SCALE
    power = sr * sr + si * si
    some = power > FLOOR
    inverse = lax.rsqrt(jnp.where(some, power, 1.0))
    return (
        jnp.where(some, power * inverse * (1.0 / SCALE), 0.0),
        jnp.where(some, (sr * br + si * bi) * inverse, br),
        jnp.where(some, (si * br - sr * bi) * inverse, bi),
    )


def decode(s, gr, gi):
    return s * gr, s * gi, s * s, gr * gr + gi * gi


def put_split(out, products, places):
    for plane, value in enumerate(products):
        high = value.astype(BF16)
        low = (value - high.astype(F32)).astype(BF16)
        for rows, lanes in places:
            out[0, plane, rows, lanes] = high
            out[1, plane, rows, lanes] = low


def edge_block(pack):
    lane = lax.broadcasted_iota(jnp.int32, pack.shape, 1)
    left, right = lane >= LANES - SIDE, lane < SIDE

    def pick(k):
        a = pack if k == 0 else pltpu.roll(pack, k * SIDE, 1)
        b = pack if k == 0 else pltpu.roll(pack, LANES - k * SIDE, 1)
        return jnp.where(left, a, jnp.where(right, b, 0.0))

    return pick(0), pick(1), pick(2)


def cuts(tiles):
    if tiles < 8:
        return ((0, tiles),)
    marks = [0, tiles // 4, tiles // 2, tiles * 3 // 4, tiles - 1, tiles]
    return tuple(zip(marks[:-1], marks[1:]))


def fold(x):
    total = x[:, 0:LANES]
    for t in range(1, x.shape[1] // LANES):
        total = total + x[:, t * LANES : (t + 1) * LANES]
    return total


def row_sum(x):
    return jnp.sum(x, 1, keepdims=True)


def front_kernel(
    n_rows, n_cols, reach,
    lead, trail, flags, sweep,
    gam, coh, memt, fit,
    av, bv, wv, sv, up_out, down_out, top_in, bot_in, left_out, right_out, left_in, right_in,
    relay_in, corner_in, split, halo_split, boxed, ribbon, across, row_parts, flag_parts, acc_h,
    tab_out, tab_in,
    load_sem, halo_send, halo_recv, side_send, side_recv, corner_send, corner_recv,
    relay_send, relay_recv, tab_send, tab_recv,
):
    me_r, me_c = lax.axis_index("rows"), lax.axis_index("cols")
    height, width = flags.shape
    tiles = width // LANES
    low = height - EDGE
    total_rows, total_cols = height * n_rows, width * n_cols
    chunk = 512 if width % 512 == 0 else LANES
    has_up, has_down = me_r > 0, me_r < n_rows - 1
    has_left, has_right = me_c > 0, me_c < n_cols - 1
    pieces = cuts(tiles)
    pair = 2 if tiles % 2 == 0 else 1

    def load(part, rows):
        group = [
            pltpu.make_async_copy(lead.at[:, rows, :], av.at[:, rows, :], load_sem.at[part, 0]),
            pltpu.make_async_copy(trail.at[:, rows, :], bv.at[:, rows, :], load_sem.at[part, 1]),
            pltpu.make_async_copy(flags.at[rows, :], wv.at[rows, :], load_sem.at[part, 2]),
        ]
        for copy in group:
            copy.start()
        return group

    loads = [load(0, pl.ds(low, EDGE)), load(1, pl.ds(0, EDGE)), load(2, pl.ds(EDGE, low - EDGE))]
    sweep_load = pltpu.make_async_copy(sweep, sv, load_sem.at[3, 0])
    sweep_load.start()

    barrier = pltpu.get_barrier_semaphore()
    peers = []
    for dr in range(-reach, reach + 1):
        for dc in range(n_cols):
            if dr == 0 and dc == 0:
                continue
            to = jnp.logical_and(me_r + dr >= 0, me_r + dr < n_rows)
            of = jnp.logical_and(me_r - dr >= 0, me_r - dr < n_rows)
            peers.append(((dr + reach) * n_cols + dc, to, of, me_r + dr, lax.rem(me_c + dc, n_cols)))
    for _, to, _, row, col in peers:
        @pl.when(to)
        def _():
            pl.semaphore_signal(barrier, inc=1, device_id=(row, col), device_id_type=MESH)

    n_peers = (jnp.minimum(me_r, reach) + jnp.minimum(n_rows - 1 - me_r, reach) + 1) * n_cols - 1

    def remote(src, dst, send, recv, row, col):
        return pltpu.make_async_remote_copy(
            src_ref=src, dst_ref=dst, send_sem=send, recv_sem=recv, device_id=(row, col), device_id_type=MESH
        )

    def cut(ref, piece):
        return ref.at[:, :, pl.ds(piece[0] * LANES, (piece[1] - piece[0]) * LANES)]

    downs = [
        remote(cut(down_out, p), cut(top_in, p), halo_send.at[0, i], halo_recv.at[0, i], me_r + 1, me_c)
        for i, p in enumerate(pieces)
    ]
    ups = [
        remote(cut(up_out, p), cut(bot_in, p), halo_send.at[1, i], halo_recv.at[1, i], me_r - 1, me_c)
        for i, p in enumerate(pieces)
    ]
    to_right = remote(right_out, left_in, side_send.at[0], side_recv.at[0], me_r, me_c + 1)
    to_left = remote(left_out, right_in, side_send.at[1], side_recv.at[1], me_r, me_c - 1)
    top_rows, low_rows = pl.ds(0, EDGE), pl.ds(low, EDGE)
    corners = []
    for k, (src, rows, dr, dc, to, of) in enumerate((
        (right_out, low_rows, 1, 1, has_down & has_right, has_up & has_left),
        (left_out, low_rows, 1, -1, has_down & has_left, has_up & has_right),
        (right_out, top_rows, -1, 1, has_up & has_right, has_down & has_left),
        (left_out, top_rows, -1, -1, has_up & has_left, has_down & has_right),
    )):
        copy = remote(src.at[rows], corner_in.at[k], corner_send.at[k], corner_recv.at[k], me_r + dr, me_c + dc)
        corners.append((copy, to, of))

    relayed = len(pieces) - 2 if n_rows % 2 == 0 and n_rows > 2 and len(pieces) > 2 else 0
    odd = lax.rem(me_r, 2) == 1
    even = jnp.logical_not(odd)
    place = lax.div(me_r, 2) * 4
    n_up = jnp.minimum(relayed, lax.div(place, n_rows // 2)) if relayed else 0
    n_down = jnp.minimum(relayed, 4 - lax.div(place + 4, n_rows // 2)) if relayed else 0
    via = []
    for i in range(relayed):
        p = pieces[i]
        ask_up, ask_down = even & (n_up > i), odd & (n_down > i)
        give_up, give_down = odd & (n_up > i), even & (n_down > i)
        via.append((
            (ask_up, remote(cut(up_out, p), cut(relay_in, p), halo_send.at[1, i], relay_recv.at[i], me_r + 1, me_c)),
            (ask_down, remote(cut(down_out, p), cut(relay_in, p), halo_send.at[0, i], relay_recv.at[i], me_r - 1, me_c)),
            (give_up, remote(cut(relay_in, p), cut(bot_in, p), relay_send.at[i], halo_recv.at[1, i], me_r - 2, me_c)),
            (give_down, remote(cut(relay_in, p), cut(top_in, p), relay_send.at[i], halo_recv.at[0, i], me_r + 2, me_c)),
        ))

    def forward(i):
        if i >= relayed:
            return
        for give, copy in via[i][2:]:
            @pl.when(give)
            def _():
                via[i][0][1].wait_recv()
                copy.start()

    def encode_rows(first, out, piece):
        lanes = pl.ds(piece[0] * LANES, (piece[1] - piece[0]) * LANES)
        for k, value in enumerate(encode(*masked(av, bv, wv, pl.ds(first, EDGE), lanes))):
            out[k, :, lanes] = value

    def pack_sides(b):
        rows = pl.ds(b * 16, 16)
        lane = lax.broadcasted_iota(jnp.int32, (16, LANES), 1)
        s, gr, gi = encode(*masked(av, bv, wv, rows, pl.ds(width - LANES, LANES)))
        right_out[rows, :] = jnp.where(
            lane >= LANES - SIDE,
            s,
            jnp.where(
                lane >= LANES - 2 * SIDE,
                pltpu.roll(gr, LANES - SIDE, 1),
                jnp.where(lane >= LANES - 3 * SIDE, pltpu.roll(gi, LANES - 2 * SIDE, 1), 0.0),
            ),
        )
        s, gr, gi = encode(*masked(av, bv, wv, rows, pl.ds(0, LANES)))
        left_out[rows, :] = jnp.where(
            lane < SIDE,
            s,
            jnp.where(
                lane < 2 * SIDE,
                pltpu.roll(gr, SIDE, 1),
                jnp.where(lane < 3 * SIDE, pltpu.roll(gi, 2 * SIDE, 1), 0.0),
            ),
        )

    for copy in loads[0] + loads[1]:
        copy.wait()
    for b in (0, height // 16 - 1):
        pack_sides(b)
    for piece in pieces:
        encode_rows(low, down_out, piece)
        encode_rows(0, up_out, piece)

    pl.semaphore_wait(barrier, n_peers)
    for copy, to, _ in corners:
        @pl.when(to)
        def _():
            copy.start()

    for group in via:
        for ask, copy in group[:2]:
            @pl.when(ask)
            def _():
                copy.start()

    for i in range(len(pieces)):
        straight_down, straight_up = has_down, has_up
        if i < relayed:
            straight_down &= jnp.logical_not(via[i][1][0])
            straight_up &= jnp.logical_not(via[i][0][0])

        @pl.when(straight_down)
        def _():
            downs[i].start()

        @pl.when(straight_up)
        def _():
            ups[i].start()

    for copy in loads[2]:
        copy.wait()

    for b in range(1, height // 16 - 1):
        pack_sides(b)

    @pl.when(has_right)
    def _():
        to_right.start()

    @pl.when(has_left)
    def _():
        to_left.start()

    @pl.when(jnp.logical_not(has_left))
    def _():
        left_in[...] = jnp.zeros_like(left_in)

    @pl.when(jnp.logical_not(has_right))
    def _():
        right_in[...] = jnp.zeros_like(right_in)

    @pl.when(jnp.logical_not(has_up))
    def _():
        top_in[...] = jnp.zeros_like(top_in)

    @pl.when(jnp.logical_not(has_down))
    def _():
        bot_in[...] = jnp.zeros_like(bot_in)

    for k, (_, _, of) in enumerate(corners):
        @pl.when(jnp.logical_not(of))
        def _():
            corner_in[k] = jnp.zeros((EDGE, LANES), F32)

    for slot, _, of, _, _ in peers:
        @pl.when(jnp.logical_not(of))
        def _():
            tab_in[slot] = jnp.zeros((1, 2 * LANES), F32)

    lane_all = lax.broadcasted_iota(jnp.int32, (8, width), 1) + me_c * width
    across[...] = (lane_all.astype(F32) + 0.5) * (2.0 / total_cols) - 1.0

    @pl.loop(0, height // 16)
    def _(b):
        rows = pl.ds(pl.multiple_of(b * 16, 16), 16)

        @pl.loop(0, width // chunk)
        def _(c):
            lanes = pl.ds(pl.multiple_of(c * chunk, chunk), chunk)
            ar, ai, br, bi = masked(av, bv, wv, rows, lanes)
            put_split(
                split,
                (ar * br + ai * bi, ai * br - ar * bi, ar * ar + ai * ai, br * br + bi * bi),
                [(rows, pl.ds(pl.multiple_of(LANES + c * chunk, LANES), chunk))],
            )

    forward(0)
    reach_in = (pair + 2) * LANES
    i = lax.broadcasted_iota(jnp.int32, (reach_in, pair * LANES), 0)
    j = lax.broadcasted_iota(jnp.int32, (reach_in, pair * LANES), 1) + LANES
    ribbon[...] = jnp.logical_and(i >= j - SIDE, i < j + SIDE).astype(F32).astype(BF16)

    def box_across(source, j, targets):
        inner = pl.ds(pl.multiple_of(j * pair * LANES, pair * LANES), reach_in)
        outer = pl.ds(pl.multiple_of(j * pair * LANES, pair * LANES), pair * LANES)
        for plane in range(4):
            sums = jnp.dot(source[0, plane, :, inner], ribbon[...], preferred_element_type=F32)
            sums = sums + jnp.dot(source[1, plane, :, inner], ribbon[...], preferred_element_type=F32)
            for first, target, count in targets:
                boxed[plane, target : target + count, outer] = sums[first : first + count]

    own = [(0, EDGE, height)]

    @pl.loop(1, max(1, tiles // pair - 1))
    def _(j):
        box_across(split, j, own)

    @pl.when(has_left)
    def _():
        to_right.wait_recv()

    @pl.when(has_right)
    def _():
        to_left.wait_recv()

    sides = [pl.ds(0, LANES), pl.ds(LANES + width, LANES)]
    for b in range(height // 16):
        rows = pl.ds(b * 16, 16)
        lane = lax.broadcasted_iota(jnp.int32, (16, LANES), 1)
        pack = jnp.where(lane >= LANES // 2, left_in[rows, :], right_in[rows, :])
        put_split(split, decode(*edge_block(pack)), [(rows, lanes) for lanes in sides])

    forward(1)
    for j in sorted({0, tiles // pair - 1}):
        box_across(split, j, own)

    sweep_load.wait()
    kind = lax.rem(lax.broadcasted_iota(jnp.int32, (LANES, height), 0), SWEEP_TALLY)
    memt[...] = (kind == sv[...]).astype(F32).T
    row_parts[...] = jnp.zeros_like(row_parts)

    group_lane = lax.broadcasted_iota(jnp.int32, (8, LANES), 1) // SWEEP_TALLY

    def row_v(group):
        row = lax.broadcasted_iota(jnp.int32, (8, LANES), 0) + (me_r * height + group * 8)
        return (row.astype(F32) + 0.5) * (2.0 / total_rows) - 1.0

    def arrange(group, values):
        table = values[0]
        for m, value in enumerate(values):
            table = value if m == 0 else jnp.where(group_lane >= m, value, table)
        return memt[group * 8 : group * 8 + 8, :] * jnp.where(group_lane < len(values), table, 0.0)

    @pl.loop(0, height // 8)
    def _(b):
        w = wv[pl.ds(pl.multiple_of(b * 8, 8), 8), :].astype(F32)
        u = across[...]
        wu = w * u
        for m, value in enumerate((w, wu, wu * u)):
            flag_parts[b, m] = fold(value)

    acc_g = None
    for b in range(height // 8):
        s0, su, suu = [row_sum(flag_parts[b, m]) for m in range(3)]
        v = row_v(b)
        part = arrange(b, (s0, su, v * s0, suu, v * su, v * v * s0))
        acc_g = part if acc_g is None else acc_g + part
    tab_out[:, 0:LANES] = jnp.sum(acc_g, 0, keepdims=True)

    forward(2)
    sub = lax.broadcasted_iota(jnp.int32, (8, LANES), 0)

    def finish(t, top, bottom):
        lanes = pl.ds(pl.multiple_of(t * LANES, LANES), LANES)
        u = across[:, lanes]
        state = [None] * 4
        for g in range(bottom + 3, top - 1, -1):
            window = []
            for plane in range(4):
                x = boxed[plane, g * 8 : g * 8 + 8, lanes]
                r1 = pltpu.roll(x, 7, 0)
                if state[plane] is None:
                    state[plane] = (r1, None, None, None, None, None)
                    y1 = x + r1
                    r2 = pltpu.roll(y1, 6, 0)
                    y2 = y1 + r2
                    r4 = pltpu.roll(y2, 4, 0)
                    state[plane] = (r1, r2, r4, None, None, None)
                    continue
                n1, n2, n4, last, pair1, pair2 = state[plane]
                y1 = x + jnp.where(sub < 7, r1, n1)
                r2 = pltpu.roll(y1, 6, 0)
                y2 = y1 + jnp.where(sub < 6, r2, n2)
                r4 = pltpu.roll(y2, 4, 0)
                y4 = y2 + jnp.where(sub < 4, r4, n4)
                both = None if last is None else y4 + last
                window.append(None if pair2 is None else both + pair2)
                state[plane] = (r1, r2, r4, y4, both, pair1)
            if len(window) < 4 or window[0] is None:
                continue
            rows = slice(g * 8, g * 8 + 8)
            inverse = lax.rsqrt((window[2] + 1.0) * (window[3] + 1.0))
            real, imag = window[0] * inverse, window[1] * inverse
            gam[0, rows, lanes] = real
            gam[1, rows, lanes] = imag
            coh[rows, lanes] = jnp.sqrt(real * real + imag * imag)
            w = wv[rows, lanes].astype(F32)
            wr, wi = w * real, w * imag
            for m, value in enumerate((wr, wi, wr * u, wi * u)):
                row_parts[g, m] += value

    def add_rows(groups):
        total = None
        for g in groups:
            hr, hi, hur, hui = [row_sum(row_parts[g, m]) for m in range(4)]
            v = row_v(g)
            part = arrange(g, (hr, hi, hur, hui, v * hr, v * hi))
            total = part if total is None else total + part
        return total

    edge_groups, groups = EDGE // 8, height // 8

    @pl.loop(0, tiles)
    def _(t):
        finish(t, edge_groups, groups - edge_groups)

    acc_h[...] = add_rows(range(edge_groups, groups - edge_groups))

    def put_halo(sources, where):
        for part, products in enumerate(sources):
            put_split(halo_split, products, [(pl.ds(part * EDGE, EDGE), lanes) for lanes in where])

    beyond = [(0, 0, EDGE), (EDGE, EDGE + height, EDGE)]
    done = 0
    for i, piece in enumerate(pieces):
        if i == 0:
            for copy, _, of in corners:
                @pl.when(of)
                def _():
                    copy.wait_recv()

            lane = lax.broadcasted_iota(jnp.int32, (EDGE, LANES), 1)
            packs = [jnp.where(lane >= LANES // 2, corner_in[k], corner_in[k + 1]) for k in (0, 2)]
            put_halo([decode(*edge_block(pack)) for pack in packs], sides)

        @pl.when(has_up)
        def _():
            downs[i].wait_recv()

        @pl.when(has_down)
        def _():
            ups[i].wait_recv()

        source = pl.ds(piece[0] * LANES, (piece[1] - piece[0]) * LANES)
        target = pl.ds((piece[0] + 1) * LANES, (piece[1] - piece[0]) * LANES)
        put_halo([decode(*[halo[m, :, source] for m in range(3)]) for halo in (top_in, bot_in)], [target])
        ready = tiles // pair if i == len(pieces) - 1 else max(0, (piece[1] - 1) // pair)
        for j in range(done, ready):
            box_across(halo_split, j, beyond)
        if ready > done:
            @pl.loop(done * pair, ready * pair)
            def _(t):
                finish(t, 0, edge_groups)
                finish(t, groups - edge_groups, groups)
        done = ready

    acc_last = acc_h[...] + add_rows(list(range(edge_groups)) + list(range(groups - edge_groups, groups)))
    tab_out[:, LANES:] = jnp.sum(acc_last, 0, keepdims=True)
    swaps = [
        (remote(tab_out, tab_in.at[slot], tab_send.at[slot], tab_recv.at[slot], row, col), to, of)
        for slot, to, of, row, col in peers
    ]
    for copy, to, _ in swaps:
        @pl.when(to)
        def _():
            copy.start()

    tab_in[reach * n_cols] = tab_out[...]
    for copy, _, of in swaps:
        @pl.when(of)
        def _():
            copy.wait_recv()

    total = functools.reduce(jnp.add, [tab_in[slot] for slot in range(tab_in.shape[0])])

    def column(base, m):
        part = total[:, base : base + LANES]
        return part if m == 0 else pltpu.roll(part, LANES - m * SWEEP_TALLY, 1)

    s0, su, sv_, suu, suv, svv = [column(0, m) for m in range(6)]
    hr, hi, hur, hui, hvr, hvi = [column(LANES, m) for m in range(6)]
    floored = jnp.maximum(s0, 1.0)
    mid_u, mid_v = su / floored, sv_ / floored
    guu = suu - 2.0 * mid_u * su + mid_u * mid_u * s0
    guv = suv - mid_u * sv_ - mid_v * su + mid_u * mid_v * s0
    gvv = svv - 2.0 * mid_v * sv_ + mid_v * mid_v * s0
    hur, hui = hur - mid_u * hr, hui - mid_u * hi
    hvr, hvi = hvr - mid_v * hr, hvi - mid_v * hi
    ridge = 0.001 * s0 + 1.0
    duu, dvv = guu + ridge, gvv + ridge
    scale = 1.0 / (duu * dvv - guv * guv)
    base = 1.0 / (s0 + ridge)
    c1r, c1i = (dvv * hur - guv * hvr) * scale, (dvv * hui - guv * hvi) * scale
    c2r, c2i = (duu * hvr - guv * hur) * scale, (duu * hvi - guv * hui) * scale
    valid = lax.broadcasted_iota(jnp.int32, (1, LANES), 1) < SWEEP_TALLY
    rows_out = (hr * base - c1r * mid_u, hi * base - c1i * mid_u, c1r, c1i, c2r, c2i, mid_v)
    for m, value in enumerate(rows_out):
        fit[m : m + 1, :] = jnp.where(valid, value, 0.0)

    @pl.when(has_down)
    def _():
        for copy in downs:
            copy.wait_send()

    @pl.when(has_up)
    def _():
        for copy in ups:
            copy.wait_send()

    for copy, to, _ in corners:
        @pl.when(to)
        def _():
            copy.wait_send()

    for group in via:
        for give, copy in group[2:]:
            @pl.when(give)
            def _():
                copy.wait_send()

    @pl.when(has_right)
    def _():
        to_right.wait_send()

    @pl.when(has_left)
    def _():
        to_left.wait_send()

    for copy, to, _ in swaps:
        @pl.when(to)
        def _():
            copy.wait_send()


def back_kernel(n_rows, n_cols, block, gam, coh, memt, fit, ramped, coherence, out, across, lines, sem):
    height, width = coh.shape
    me_r, me_c = lax.axis_index("rows"), lax.axis_index("cols")
    coh_copy = pltpu.make_async_copy(coh, coherence, sem.at[0])
    coh_copy.start()
    for g in range(height // 8):
        row = lax.broadcasted_iota(jnp.int32, (8, LANES), 0) + (me_r * height + g * 8)
        dv = (row.astype(F32) + 0.5) * (2.0 / (height * n_rows)) - 1.0 - fit[6:7, :]
        one = memt[g * 8 : g * 8 + 8, :]
        for m, value in enumerate((fit[0:1, :] + fit[4:5, :] * dv, fit[1:2, :] + fit[5:6, :] * dv, fit[2:3, :], fit[3:4, :])):
            lines[g, m] = jnp.broadcast_to(row_sum(one * value), (8, LANES))
    lane_all = lax.broadcasted_iota(jnp.int32, (8, width), 1) + me_c * width
    across[...] = (lane_all.astype(F32) + 0.5) * (2.0 / (width * n_cols)) - 1.0

    copies = []
    for i in range(height // block):
        @pl.loop(0, block // 8)
        def _(b):
            g = i * (block // 8) + b
            rows = pl.ds(pl.multiple_of(g * 8, 8), 8)
            base_r, base_i, slope_r, slope_i = [lines[g, m] for m in range(4)]
            for t in range(width // LANES):
                lanes = slice(t * LANES, (t + 1) * LANES)
                real, imag, u = gam[0, rows, lanes], gam[1, rows, lanes], across[:, lanes]
                model_real = base_r + slope_r * u
                model_imag = base_i + slope_i * u
                out[0, rows, lanes] = real * model_real + imag * model_imag
                out[1, rows, lanes] = imag * model_real - real * model_imag

        rows = pl.ds(i * block, block)
        copy = pltpu.make_async_copy(out.at[:, rows, :], ramped.at[:, rows, :], sem.at[1 + i])
        copy.start()
        copies.append(copy)
    coh_copy.wait()
    for copy in copies:
        copy.wait()


def on_device(n_rows, n_cols, lead, trail, flags, sweep):
    height, width = flags.shape
    wide = width + 2 * LANES
    longest = 2 * height * n_rows // SWEEP_TALLY
    reach = max(1, min(n_rows - 1, (longest - 2) // height + 1))
    slots = (2 * reach + 1) * n_cols
    pieces = len(cuts(width // LANES))
    pair = 2 if width // LANES % 2 == 0 else 1
    hbm = pl.BlockSpec(memory_space=pltpu.HBM)
    vmem = pl.BlockSpec(memory_space=pltpu.VMEM)
    dma = pltpu.SemaphoreType.DMA
    gam, coh, memt, fit = pl.pallas_call(
        functools.partial(front_kernel, n_rows, n_cols, reach),
        out_shape=[
            pltpu.VMEM((2, height, width), F32),
            pltpu.VMEM((height, width), F32),
            pltpu.VMEM((height, LANES), F32),
            pltpu.VMEM((8, LANES), F32),
        ],
        in_specs=[hbm, hbm, hbm, hbm],
        out_specs=[vmem, vmem, vmem, vmem],
        scratch_shapes=[
            pltpu.VMEM((2, height, width), F32),
            pltpu.VMEM((2, height, width), F32),
            pltpu.VMEM((height, width), jnp.int32),
            pltpu.VMEM((1, height), jnp.int32),
            pltpu.VMEM((3, EDGE, width), F32),
            pltpu.VMEM((3, EDGE, width), F32),
            pltpu.VMEM((3, EDGE, width), F32),
            pltpu.VMEM((3, EDGE, width), F32),
            pltpu.VMEM((height, LANES), F32),
            pltpu.VMEM((height, LANES), F32),
            pltpu.VMEM((height, LANES), F32),
            pltpu.VMEM((height, LANES), F32),
            pltpu.VMEM((3, EDGE, width), F32),
            pltpu.VMEM((4, EDGE, LANES), F32),
            pltpu.VMEM((2, 4, height, wide), BF16),
            pltpu.VMEM((2, 4, 2 * EDGE, wide), BF16),
            pltpu.VMEM((4, height + 2 * EDGE, width), F32),
            pltpu.VMEM(((pair + 2) * LANES, pair * LANES), BF16),
            pltpu.VMEM((8, width), F32),
            pltpu.VMEM((height // 8, 4, 8, LANES), F32),
            pltpu.VMEM((height // 8, 3, 8, LANES), F32),
            pltpu.VMEM((8, LANES), F32),
            pltpu.VMEM((1, 2 * LANES), F32),
            pltpu.VMEM((slots, 1, 2 * LANES), F32),
            dma((4, 3)),
            dma((2, pieces)), dma((2, pieces)),
            dma((2,)), dma((2,)),
            dma((4,)), dma((4,)),
            dma((pieces,)), dma((pieces,)),
            dma((slots,)), dma((slots,)),
        ],
        compiler_params=pltpu.CompilerParams(
            collective_id=0, has_side_effects=True, vmem_limit_bytes=60 * 1024 * 1024
        ),
        name="front",
    )(lead, trail, flags, sweep.reshape(1, height))
    block = 16 if height % 16 == 0 else 8
    return pl.pallas_call(
        functools.partial(back_kernel, n_rows, n_cols, block),
        out_shape=[
            jax.ShapeDtypeStruct((2, height, width), F32),
            jax.ShapeDtypeStruct((height, width), F32),
        ],
        in_specs=[vmem, vmem, vmem, vmem],
        out_specs=[hbm, hbm],
        scratch_shapes=[
            pltpu.VMEM((2, height, width), F32),
            pltpu.VMEM((8, width), F32),
            pltpu.VMEM((height // 8, 4, 8, LANES), F32),
            dma((1 + height // block,)),
        ],
        compiler_params=pltpu.CompilerParams(vmem_limit_bytes=16 * 1024 * 1024),
        name="back",
    )(gam, coh, memt, fit)


def solution(mesh):
    return jax.shard_map(
        functools.partial(on_device, mesh.shape["rows"], mesh.shape["cols"]),
        mesh=mesh,
        in_specs=(P(None, "rows", "cols"), P(None, "rows", "cols"), P("rows", "cols"), P("rows")),
        out_specs=(P(None, "rows", "cols"), P("rows", "cols")),
        check_vma=False,
    )
```

```python
import functools

import jax
import jax.numpy as jnp
from jax import lax
from jax.experimental import pallas as pl
from jax.experimental.pallas import tpu as pltpu
from jax.sharding import PartitionSpec as P

WIN_R = 32
WIN_C = 8
SWEEP_TALLY = 16

EDGE = WIN_R // 2
SIDE = WIN_C // 2
LANES = 128
SCALE = 2.0**56
FLOOR = 1e-36
F32 = jnp.float32
BF16 = jnp.bfloat16
MESH = pl.DeviceIdType.MESH


def masked(av, bv, wv, rows, lanes):
    w = wv[rows, lanes].astype(F32)
    return av[0, rows, lanes] * w, av[1, rows, lanes] * w, bv[0, rows, lanes] * w, bv[1, rows, lanes] * w


def encode(ar, ai, br, bi):
    sr, si = ar * SCALE, ai * SCALE
    power = sr * sr + si * si
    some = power > FLOOR
    inverse = lax.rsqrt(jnp.where(some, power, 1.0))
    return (
        jnp.where(some, power * inverse * (1.0 / SCALE), 0.0),
        jnp.where(some, (sr * br + si * bi) * inverse, br),
        jnp.where(some, (si * br - sr * bi) * inverse, bi),
    )


def decode(s, gr, gi):
    return s * gr, s * gi, s * s, gr * gr + gi * gi


def put_split(out, products, places):
    for plane, value in enumerate(products):
        high = value.astype(BF16)
        low = (value - high.astype(F32)).astype(BF16)
        for rows, lanes in places:
            out[0, plane, rows, lanes] = high
            out[1, plane, rows, lanes] = low


def edge_block(pack):
    lane = lax.broadcasted_iota(jnp.int32, pack.shape, 1)
    left, right = lane >= LANES - SIDE, lane < SIDE

    def pick(k):
        a = pack if k == 0 else pltpu.roll(pack, k * SIDE, 1)
        b = pack if k == 0 else pltpu.roll(pack, LANES - k * SIDE, 1)
        return jnp.where(left, a, jnp.where(right, b, 0.0))

    return pick(0), pick(1), pick(2)


def cuts(tiles):
    if tiles < 8:
        return ((0, tiles),)
    marks = [0, tiles // 4, tiles // 2, tiles * 3 // 4, tiles - 1, tiles]
    return tuple(zip(marks[:-1], marks[1:]))


def fold(x):
    total = x[:, 0:LANES]
    for t in range(1, x.shape[1] // LANES):
        total = total + x[:, t * LANES : (t + 1) * LANES]
    return total


def row_sum(x):
    return jnp.sum(x, 1, keepdims=True)


def front_kernel(
    n_rows, n_cols, reach,
    lead, trail, flags, sweep,
    gam, coh, memt, fit,
    av, bv, wv, sv, up_out, down_out, top_in, bot_in, left_out, right_out, left_in, right_in,
    relay_in, corner_in, split, halo_split, boxed, ribbon, across, row_parts, flag_parts, acc_h,
    tab_out, tab_in,
    load_sem, halo_send, halo_recv, side_send, side_recv, corner_send, corner_recv,
    relay_send, relay_recv, tab_send, tab_recv, token,
):
    me_r, me_c = lax.axis_index("rows"), lax.axis_index("cols")
    height, width = flags.shape
    tiles = width // LANES
    low = height - EDGE
    total_rows, total_cols = height * n_rows, width * n_cols
    chunk = 512 if width % 512 == 0 else LANES
    has_up, has_down = me_r > 0, me_r < n_rows - 1
    has_left, has_right = me_c > 0, me_c < n_cols - 1
    pieces = cuts(tiles)
    pair = 2 if tiles % 2 == 0 else 1

    def load(part, rows):
        group = [
            pltpu.make_async_copy(lead.at[:, rows, :], av.at[:, rows, :], load_sem.at[part, 0]),
            pltpu.make_async_copy(trail.at[:, rows, :], bv.at[:, rows, :], load_sem.at[part, 1]),
            pltpu.make_async_copy(flags.at[rows, :], wv.at[rows, :], load_sem.at[part, 2]),
        ]
        for copy in group:
            copy.start()
        return group

    loads = [load(0, pl.ds(low, EDGE)), load(1, pl.ds(0, EDGE))]
    sweep_load = pltpu.make_async_copy(sweep, sv, load_sem.at[3, 0])
    sweep_load.start()

    barrier = pltpu.get_barrier_semaphore()
    peers = []
    for dr in range(-reach, reach + 1):
        for dc in range(n_cols):
            if dr == 0 and dc == 0:
                continue
            to = jnp.logical_and(me_r + dr >= 0, me_r + dr < n_rows)
            of = jnp.logical_and(me_r - dr >= 0, me_r - dr < n_rows)
            peers.append(((dr + reach) * n_cols + dc, to, of, me_r + dr, lax.rem(me_c + dc, n_cols)))
    near = reach == 1
    n_greeted = 0
    for slot, to, _, row, col in peers:
        dr, dc = slot // n_cols - reach, slot % n_cols
        if near and dr != 0 and dc != 0:
            continue
        n_greeted = n_greeted + to.astype(jnp.int32)

        @pl.when(to)
        def _():
            pl.semaphore_signal(barrier, inc=1, device_id=(row, col), device_id_type=MESH)

    def remote(src, dst, send, recv, row, col):
        return pltpu.make_async_remote_copy(
            src_ref=src, dst_ref=dst, send_sem=send, recv_sem=recv, device_id=(row, col), device_id_type=MESH
        )

    def cut(ref, piece):
        return ref.at[:, :, pl.ds(piece[0] * LANES, (piece[1] - piece[0]) * LANES)]

    downs = [
        remote(cut(down_out, p), cut(top_in, p), halo_send.at[0, i], halo_recv.at[0, i], me_r + 1, me_c)
        for i, p in enumerate(pieces)
    ]
    ups = [
        remote(cut(up_out, p), cut(bot_in, p), halo_send.at[1, i], halo_recv.at[1, i], me_r - 1, me_c)
        for i, p in enumerate(pieces)
    ]
    to_right = remote(right_out, left_in, side_send.at[0], side_recv.at[0], me_r, me_c + 1)
    to_left = remote(left_out, right_in, side_send.at[1], side_recv.at[1], me_r, me_c - 1)
    top_rows, low_rows = pl.ds(0, EDGE), pl.ds(low, EDGE)
    corners = []
    for k, (src, rows, dr, dc, to, of) in enumerate((
        (right_out, low_rows, 1, 1, has_down & has_right, has_up & has_left),
        (left_out, low_rows, 1, -1, has_down & has_left, has_up & has_right),
        (right_out, top_rows, -1, 1, has_up & has_right, has_down & has_left),
        (left_out, top_rows, -1, -1, has_up & has_left, has_down & has_right),
    )):
        copy = remote(src.at[rows], corner_in.at[k], corner_send.at[k], corner_recv.at[k], me_r + dr, me_c + dc)
        corners.append((copy, to, of))

    relayed = len(pieces) - 2 if n_rows % 2 == 0 and n_rows > 2 and len(pieces) > 2 else 0
    odd = lax.rem(me_r, 2) == 1
    even = jnp.logical_not(odd)
    place = lax.div(me_r, 2) * 4
    n_up = jnp.minimum(relayed, lax.div(place, n_rows // 2)) if relayed else 0
    n_down = jnp.minimum(relayed, 4 - lax.div(place + 4, n_rows // 2)) if relayed else 0
    via = []
    for i in range(relayed):
        p = pieces[i]
        ask_up, ask_down = even & (n_up > i), odd & (n_down > i)
        give_up, give_down = odd & (n_up > i), even & (n_down > i)
        via.append((
            (ask_up, remote(cut(up_out, p), cut(relay_in, p), halo_send.at[1, i], relay_recv.at[i], me_r + 1, me_c)),
            (ask_down, remote(cut(down_out, p), cut(relay_in, p), halo_send.at[0, i], relay_recv.at[i], me_r - 1, me_c)),
            (give_up, remote(cut(relay_in, p), cut(bot_in, p), relay_send.at[i], halo_recv.at[1, i], me_r - 2, me_c)),
            (give_down, remote(cut(relay_in, p), cut(top_in, p), relay_send.at[i], halo_recv.at[0, i], me_r + 2, me_c)),
        ))

    def forward(i):
        if i >= relayed:
            return
        for give, copy in via[i][2:]:
            @pl.when(give)
            def _():
                via[i][0][1].wait_recv()
                copy.start()

    def encode_rows(first, out, piece):
        lanes = pl.ds(piece[0] * LANES, (piece[1] - piece[0]) * LANES)
        for k, value in enumerate(encode(*masked(av, bv, wv, pl.ds(first, EDGE), lanes))):
            out[k, :, lanes] = value

    def pack_sides(b):
        rows = pl.ds(b * 16, 16)
        lane = lax.broadcasted_iota(jnp.int32, (16, LANES), 1)
        s, gr, gi = encode(*masked(av, bv, wv, rows, pl.ds(width - LANES, LANES)))
        right_out[rows, :] = jnp.where(
            lane >= LANES - SIDE,
            s,
            jnp.where(
                lane >= LANES - 2 * SIDE,
                pltpu.roll(gr, LANES - SIDE, 1),
                jnp.where(lane >= LANES - 3 * SIDE, pltpu.roll(gi, LANES - 2 * SIDE, 1), 0.0),
            ),
        )
        s, gr, gi = encode(*masked(av, bv, wv, rows, pl.ds(0, LANES)))
        left_out[rows, :] = jnp.where(
            lane < SIDE,
            s,
            jnp.where(
                lane < 2 * SIDE,
                pltpu.roll(gr, SIDE, 1),
                jnp.where(lane < 3 * SIDE, pltpu.roll(gi, 2 * SIDE, 1), 0.0),
            ),
        )

    for copy in loads[0] + loads[1]:
        copy.wait()
    loads.append(load(2, pl.ds(EDGE, low - EDGE)))
    for b in (0, height // 16 - 1):
        pack_sides(b)
    for piece in pieces:
        encode_rows(low, down_out, piece)
        encode_rows(0, up_out, piece)

    pl.semaphore_wait(barrier, n_greeted)
    n_via = jnp.where(even, n_up, n_down)

    def send(point):
        slots = (0, 1) if point == 0 else (point + 1,)
        for v in range(relayed + 1):
            later = [i for i in range(v, len(pieces)) if point == (i + min(1, v) + (1 if i == v == 3 else 0) if v else i)]
            for parity, straight, other, asked in ((even, downs, ups, 0), (odd, ups, downs, 1)):
                @pl.when(parity & (n_via == v))
                def _():
                    far, near_by = (has_up, has_down) if asked == 0 else (has_down, has_up)
                    for k in slots:
                        if k < v:
                            via[k][asked][1].start()
                        elif k - v < len(pieces):
                            @pl.when(near_by)
                            def _():
                                straight[k - v].start()
                    for i in later:
                        @pl.when(far)
                        def _():
                            other[i].start()

    send(0)
    if near:
        for dc in range(1, n_cols):
            pl.semaphore_signal(token, inc=1, device_id=(me_r, lax.rem(me_c + dc, n_cols)), device_id_type=MESH)

    for copy in loads[2]:
        copy.wait()

    for b in range(1, height // 16 - 1):
        pack_sides(b)

    @pl.when(has_right)
    def _():
        to_right.start()

    @pl.when(has_left)
    def _():
        to_left.start()

    @pl.when(jnp.logical_not(has_left))
    def _():
        left_in[...] = jnp.zeros_like(left_in)

    @pl.when(jnp.logical_not(has_right))
    def _():
        right_in[...] = jnp.zeros_like(right_in)

    @pl.when(jnp.logical_not(has_up))
    def _():
        top_in[...] = jnp.zeros_like(top_in)

    @pl.when(jnp.logical_not(has_down))
    def _():
        bot_in[...] = jnp.zeros_like(bot_in)

    for k, (_, _, of) in enumerate(corners):
        @pl.when(jnp.logical_not(of))
        def _():
            corner_in[k] = jnp.zeros((EDGE, LANES), F32)

    for slot, _, of, _, _ in peers:
        @pl.when(jnp.logical_not(of))
        def _():
            tab_in[slot] = jnp.zeros((1, 2 * LANES), F32)

    if near:
        pl.semaphore_wait(token, n_cols - 1)
    for copy, to, _ in corners:
        @pl.when(to)
        def _():
            copy.start()

    lane_all = lax.broadcasted_iota(jnp.int32, (8, width), 1) + me_c * width
    across[...] = (lane_all.astype(F32) + 0.5) * (2.0 / total_cols) - 1.0

    @pl.loop(0, height // 16)
    def _(b):
        rows = pl.ds(pl.multiple_of(b * 16, 16), 16)

        @pl.loop(0, width // chunk)
        def _(c):
            lanes = pl.ds(pl.multiple_of(c * chunk, chunk), chunk)
            ar, ai, br, bi = masked(av, bv, wv, rows, lanes)
            put_split(
                split,
                (ar * br + ai * bi, ai * br - ar * bi, ar * ar + ai * ai, br * br + bi * bi),
                [(rows, pl.ds(pl.multiple_of(LANES + c * chunk, LANES), chunk))],
            )

    send(1)
    reach_in = (pair + 2) * LANES
    i = lax.broadcasted_iota(jnp.int32, (reach_in, pair * LANES), 0)
    j = lax.broadcasted_iota(jnp.int32, (reach_in, pair * LANES), 1) + LANES
    ribbon[...] = jnp.logical_and(i >= j - SIDE, i < j + SIDE).astype(F32).astype(BF16)

    def box_across(j):
        inner = pl.ds(pl.multiple_of(j * pair * LANES, pair * LANES), reach_in)
        outer = pl.ds(pl.multiple_of(j * pair * LANES, pair * LANES), pair * LANES)
        for plane in range(4):
            sums = jnp.dot(split[0, plane, :, inner], ribbon[...], preferred_element_type=F32)
            sums = sums + jnp.dot(split[1, plane, :, inner], ribbon[...], preferred_element_type=F32)
            boxed[plane, EDGE : EDGE + height, outer] = sums

    last = tiles // pair - 1
    middle = max(1, tiles // pair // 2)

    @pl.loop(1, middle)
    def _(j):
        box_across(j)

    send(2)

    @pl.loop(middle, max(middle, last))
    def _(j):
        box_across(j)

    @pl.when(has_left)
    def _():
        to_right.wait_recv()

    @pl.when(has_right)
    def _():
        to_left.wait_recv()

    sides = [pl.ds(0, LANES), pl.ds(LANES + width, LANES)]
    for b in range(height // 16):
        rows = pl.ds(b * 16, 16)
        lane = lax.broadcasted_iota(jnp.int32, (16, LANES), 1)
        pack = jnp.where(lane >= LANES // 2, left_in[rows, :], right_in[rows, :])
        put_split(split, decode(*edge_block(pack)), [(rows, lanes) for lanes in sides])

    send(3)
    forward(0)
    forward(1)
    for j in sorted({0, last}):
        box_across(j)

    sweep_load.wait()
    kind = lax.rem(lax.broadcasted_iota(jnp.int32, (LANES, height), 0), SWEEP_TALLY)
    memt[...] = (kind == sv[...]).astype(F32).T
    row_parts[...] = jnp.zeros_like(row_parts)

    group_lane = lax.broadcasted_iota(jnp.int32, (8, LANES), 1) // SWEEP_TALLY

    def row_v(group):
        row = lax.broadcasted_iota(jnp.int32, (8, LANES), 0) + (me_r * height + group * 8)
        return (row.astype(F32) + 0.5) * (2.0 / total_rows) - 1.0

    def arrange(group, values):
        table = values[0]
        for m, value in enumerate(values):
            table = value if m == 0 else jnp.where(group_lane >= m, value, table)
        return memt[group * 8 : group * 8 + 8, :] * jnp.where(group_lane < len(values), table, 0.0)

    @pl.loop(0, height // 8)
    def _(b):
        w = wv[pl.ds(pl.multiple_of(b * 8, 8), 8), :].astype(F32)
        u = across[...]
        wu = w * u
        for m, value in enumerate((w, wu, wu * u)):
            flag_parts[b, m] = fold(value)

    acc_g = None
    for b in range(height // 8):
        s0, su, suu = [row_sum(flag_parts[b, m]) for m in range(3)]
        v = row_v(b)
        part = arrange(b, (s0, su, v * s0, suu, v * su, v * v * s0))
        acc_g = part if acc_g is None else acc_g + part
    tab_out[:, 0:LANES] = jnp.sum(acc_g, 0, keepdims=True)

    send(4)
    sub = lax.broadcasted_iota(jnp.int32, (8, LANES), 0)

    def finish(t, top, bottom):
        lanes = pl.ds(pl.multiple_of(t * LANES, LANES), LANES)
        u = across[:, lanes]
        state = [None] * 4
        for g in range(bottom + 3, top - 1, -1):
            window = []
            for plane in range(4):
                x = boxed[plane, g * 8 : g * 8 + 8, lanes]
                r1 = pltpu.roll(x, 7, 0)
                if state[plane] is None:
                    state[plane] = (r1, None, None, None, None, None)
                    y1 = x + r1
                    r2 = pltpu.roll(y1, 6, 0)
                    y2 = y1 + r2
                    r4 = pltpu.roll(y2, 4, 0)
                    state[plane] = (r1, r2, r4, None, None, None)
                    continue
                n1, n2, n4, last, pair1, pair2 = state[plane]
                y1 = x + jnp.where(sub < 7, r1, n1)
                r2 = pltpu.roll(y1, 6, 0)
                y2 = y1 + jnp.where(sub < 6, r2, n2)
                r4 = pltpu.roll(y2, 4, 0)
                y4 = y2 + jnp.where(sub < 4, r4, n4)
                both = None if last is None else y4 + last
                window.append(None if pair2 is None else both + pair2)
                state[plane] = (r1, r2, r4, y4, both, pair1)
            if len(window) < 4 or window[0] is None:
                continue
            rows = slice(g * 8, g * 8 + 8)
            inverse = lax.rsqrt((window[2] + 1.0) * (window[3] + 1.0))
            real, imag = window[0] * inverse, window[1] * inverse
            gam[0, rows, lanes] = real
            gam[1, rows, lanes] = imag
            coh[rows, lanes] = jnp.sqrt(real * real + imag * imag)
            w = wv[rows, lanes].astype(F32)
            wr, wi = w * real, w * imag
            for m, value in enumerate((wr, wi, wr * u, wi * u)):
                row_parts[g, m] += value

    def add_rows(groups):
        total = None
        for g in groups:
            hr, hi, hur, hui = [row_sum(row_parts[g, m]) for m in range(4)]
            v = row_v(g)
            part = arrange(g, (hr, hi, hur, hui, v * hr, v * hi))
            total = part if total is None else total + part
        return total

    edge_groups, groups = EDGE // 8, height // 8

    @pl.loop(0, tiles // 2)
    def _(t):
        finish(t, edge_groups, groups - edge_groups)

    send(5)
    forward(2)

    @pl.loop(tiles // 2, tiles)
    def _(t):
        finish(t, edge_groups, groups - edge_groups)

    send(6)

    acc_h[...] = add_rows(range(edge_groups, groups - edge_groups))

    def put_halo(sources, where):
        for part, products in enumerate(sources):
            for plane, value in enumerate(products):
                first = (plane * 2 + part) * EDGE
                high = value.astype(BF16)
                low_part = (value - high.astype(F32)).astype(BF16)
                for lanes in where:
                    halo_split[first : first + EDGE, lanes] = high
                    halo_split[8 * EDGE + first : 9 * EDGE + first, lanes] = low_part

    def box_halo(j):
        inner = pl.ds(j * pair * LANES, reach_in)
        outer = pl.ds(j * pair * LANES, pair * LANES)
        sums = jnp.dot(halo_split[:, inner], ribbon[...], preferred_element_type=F32)
        for plane in range(4):
            for part, target in enumerate((0, EDGE + height)):
                first = (plane * 2 + part) * EDGE
                boxed[plane, target : target + EDGE, outer] = (
                    sums[first : first + EDGE] + sums[8 * EDGE + first : 9 * EDGE + first]
                )

    done = 0
    for i, piece in enumerate(pieces):
        if i == 0:
            for copy, _, of in corners:
                @pl.when(of)
                def _():
                    copy.wait_recv()

            lane = lax.broadcasted_iota(jnp.int32, (EDGE, LANES), 1)
            packs = [jnp.where(lane >= LANES // 2, corner_in[k], corner_in[k + 1]) for k in (0, 2)]
            put_halo([decode(*edge_block(pack)) for pack in packs], sides)

        @pl.when(has_up)
        def _():
            downs[i].wait_recv()

        @pl.when(has_down)
        def _():
            ups[i].wait_recv()

        source = pl.ds(piece[0] * LANES, (piece[1] - piece[0]) * LANES)
        target = pl.ds((piece[0] + 1) * LANES, (piece[1] - piece[0]) * LANES)
        put_halo([decode(*[halo[m, :, source] for m in range(3)]) for halo in (top_in, bot_in)], [target])
        ready = tiles // pair if i == len(pieces) - 1 else max(0, (piece[1] - 1) // pair)
        for j in range(done, ready):
            box_halo(j)
        if ready > done:
            @pl.loop(done, ready)
            def _(j):
                for t in range(pair):
                    finish(j * pair + t, 0, edge_groups)
                    finish(j * pair + t, groups - edge_groups, groups)
        done = ready

    acc_last = acc_h[...] + add_rows(list(range(edge_groups)) + list(range(groups - edge_groups, groups)))
    tab_out[:, LANES:] = jnp.sum(acc_last, 0, keepdims=True)
    swaps = [
        (remote(tab_out, tab_in.at[slot], tab_send.at[slot], tab_recv.at[slot], row, col), to, of)
        for slot, to, of, row, col in peers
    ]
    for copy, to, _ in swaps:
        @pl.when(to)
        def _():
            copy.start()

    tab_in[reach * n_cols] = tab_out[...]
    for copy, _, of in swaps:
        @pl.when(of)
        def _():
            copy.wait_recv()

    total = functools.reduce(jnp.add, [tab_in[slot] for slot in range(tab_in.shape[0])])

    def column(base, m):
        part = total[:, base : base + LANES]
        return part if m == 0 else pltpu.roll(part, LANES - m * SWEEP_TALLY, 1)

    s0, su, sv_, suu, suv, svv = [column(0, m) for m in range(6)]
    hr, hi, hur, hui, hvr, hvi = [column(LANES, m) for m in range(6)]
    floored = jnp.maximum(s0, 1.0)
    mid_u, mid_v = su / floored, sv_ / floored
    guu = suu - 2.0 * mid_u * su + mid_u * mid_u * s0
    guv = suv - mid_u * sv_ - mid_v * su + mid_u * mid_v * s0
    gvv = svv - 2.0 * mid_v * sv_ + mid_v * mid_v * s0
    hur, hui = hur - mid_u * hr, hui - mid_u * hi
    hvr, hvi = hvr - mid_v * hr, hvi - mid_v * hi
    ridge = 0.001 * s0 + 1.0
    duu, dvv = guu + ridge, gvv + ridge
    scale = 1.0 / (duu * dvv - guv * guv)
    base = 1.0 / (s0 + ridge)
    c1r, c1i = (dvv * hur - guv * hvr) * scale, (dvv * hui - guv * hvi) * scale
    c2r, c2i = (duu * hvr - guv * hur) * scale, (duu * hvi - guv * hui) * scale
    valid = lax.broadcasted_iota(jnp.int32, (1, LANES), 1) < SWEEP_TALLY
    rows_out = (hr * base - c1r * mid_u, hi * base - c1i * mid_u, c1r, c1i, c2r, c2i, mid_v)
    for m, value in enumerate(rows_out):
        fit[m : m + 1, :] = jnp.where(valid, value, 0.0)

    @pl.when(has_down)
    def _():
        for copy in downs:
            copy.wait_send()

    @pl.when(has_up)
    def _():
        for copy in ups:
            copy.wait_send()

    for copy, to, _ in corners:
        @pl.when(to)
        def _():
            copy.wait_send()

    for group in via:
        for give, copy in group[2:]:
            @pl.when(give)
            def _():
                copy.wait_send()

    @pl.when(has_right)
    def _():
        to_right.wait_send()

    @pl.when(has_left)
    def _():
        to_left.wait_send()

    for copy, to, _ in swaps:
        @pl.when(to)
        def _():
            copy.wait_send()


def back_kernel(n_rows, n_cols, block, gam, coh, memt, fit, ramped, coherence, out, across, lines, sem):
    height, width = coh.shape
    me_r, me_c = lax.axis_index("rows"), lax.axis_index("cols")
    coh_copy = pltpu.make_async_copy(coh, coherence, sem.at[0])
    coh_copy.start()
    for g in range(height // 8):
        row = lax.broadcasted_iota(jnp.int32, (8, LANES), 0) + (me_r * height + g * 8)
        dv = (row.astype(F32) + 0.5) * (2.0 / (height * n_rows)) - 1.0 - fit[6:7, :]
        one = memt[g * 8 : g * 8 + 8, :]
        for m, value in enumerate((fit[0:1, :] + fit[4:5, :] * dv, fit[1:2, :] + fit[5:6, :] * dv, fit[2:3, :], fit[3:4, :])):
            lines[g, m] = jnp.broadcast_to(row_sum(one * value), (8, LANES))
    lane_all = lax.broadcasted_iota(jnp.int32, (8, width), 1) + me_c * width
    across[...] = (lane_all.astype(F32) + 0.5) * (2.0 / (width * n_cols)) - 1.0

    copies = []
    for i in range(height // block):
        @pl.loop(0, block // 8)
        def _(b):
            g = i * (block // 8) + b
            rows = pl.ds(pl.multiple_of(g * 8, 8), 8)
            base_r, base_i, slope_r, slope_i = [lines[g, m] for m in range(4)]
            for t in range(width // LANES):
                lanes = slice(t * LANES, (t + 1) * LANES)
                real, imag, u = gam[0, rows, lanes], gam[1, rows, lanes], across[:, lanes]
                model_real = base_r + slope_r * u
                model_imag = base_i + slope_i * u
                out[0, rows, lanes] = real * model_real + imag * model_imag
                out[1, rows, lanes] = imag * model_real - real * model_imag

        rows = pl.ds(i * block, block)
        copy = pltpu.make_async_copy(out.at[:, rows, :], ramped.at[:, rows, :], sem.at[1 + i])
        copy.start()
        copies.append(copy)
    coh_copy.wait()
    for copy in copies:
        copy.wait()


def on_device(n_rows, n_cols, lead, trail, flags, sweep):
    height, width = flags.shape
    wide = width + 2 * LANES
    longest = 2 * height * n_rows // SWEEP_TALLY
    reach = max(1, min(n_rows - 1, (longest - 2) // height + 1))
    slots = (2 * reach + 1) * n_cols
    pieces = len(cuts(width // LANES))
    pair = 2 if width // LANES % 2 == 0 else 1
    hbm = pl.BlockSpec(memory_space=pltpu.HBM)
    vmem = pl.BlockSpec(memory_space=pltpu.VMEM)
    dma = pltpu.SemaphoreType.DMA
    gam, coh, memt, fit = pl.pallas_call(
        functools.partial(front_kernel, n_rows, n_cols, reach),
        out_shape=[
            pltpu.VMEM((2, height, width), F32),
            pltpu.VMEM((height, width), F32),
            pltpu.VMEM((height, LANES), F32),
            pltpu.VMEM((8, LANES), F32),
        ],
        in_specs=[hbm, hbm, hbm, hbm],
        out_specs=[vmem, vmem, vmem, vmem],
        scratch_shapes=[
            pltpu.VMEM((2, height, width), F32),
            pltpu.VMEM((2, height, width), F32),
            pltpu.VMEM((height, width), jnp.int32),
            pltpu.VMEM((1, height), jnp.int32),
            pltpu.VMEM((3, EDGE, width), F32),
            pltpu.VMEM((3, EDGE, width), F32),
            pltpu.VMEM((3, EDGE, width), F32),
            pltpu.VMEM((3, EDGE, width), F32),
            pltpu.VMEM((height, LANES), F32),
            pltpu.VMEM((height, LANES), F32),
            pltpu.VMEM((height, LANES), F32),
            pltpu.VMEM((height, LANES), F32),
            pltpu.VMEM((3, EDGE, width), F32),
            pltpu.VMEM((4, EDGE, LANES), F32),
            pltpu.VMEM((2, 4, height, wide), BF16),
            pltpu.VMEM((16 * EDGE, wide), BF16),
            pltpu.VMEM((4, height + 2 * EDGE, width), F32),
            pltpu.VMEM(((pair + 2) * LANES, pair * LANES), BF16),
            pltpu.VMEM((8, width), F32),
            pltpu.VMEM((height // 8, 4, 8, LANES), F32),
            pltpu.VMEM((height // 8, 3, 8, LANES), F32),
            pltpu.VMEM((8, LANES), F32),
            pltpu.VMEM((1, 2 * LANES), F32),
            pltpu.VMEM((slots, 1, 2 * LANES), F32),
            dma((4, 3)),
            dma((2, pieces)), dma((2, pieces)),
            dma((2,)), dma((2,)),
            dma((4,)), dma((4,)),
            dma((pieces,)), dma((pieces,)),
            dma((slots,)), dma((slots,)),
            pltpu.SemaphoreType.REGULAR,
        ],
        compiler_params=pltpu.CompilerParams(
            collective_id=0, has_side_effects=True, vmem_limit_bytes=60 * 1024 * 1024
        ),
        name="front",
    )(lead, trail, flags, sweep.reshape(1, height))
    block = 16 if height % 16 == 0 else 8
    return pl.pallas_call(
        functools.partial(back_kernel, n_rows, n_cols, block),
        out_shape=[
            jax.ShapeDtypeStruct((2, height, width), F32),
            jax.ShapeDtypeStruct((height, width), F32),
        ],
        in_specs=[vmem, vmem, vmem, vmem],
        out_specs=[hbm, hbm],
        scratch_shapes=[
            pltpu.VMEM((2, height, width), F32),
            pltpu.VMEM((8, width), F32),
            pltpu.VMEM((height // 8, 4, 8, LANES), F32),
            dma((1 + height // block,)),
        ],
        compiler_params=pltpu.CompilerParams(vmem_limit_bytes=16 * 1024 * 1024),
        name="back",
    )(gam, coh, memt, fit)


def solution(mesh):
    return jax.shard_map(
        functools.partial(on_device, mesh.shape["rows"], mesh.shape["cols"]),
        mesh=mesh,
        in_specs=(P(None, "rows", "cols"), P(None, "rows", "cols"), P("rows", "cols"), P("rows")),
        out_specs=(P(None, "rows", "cols"), P("rows", "cols")),
        check_vma=False,
    )
```

```python
import functools

import jax
import jax.numpy as jnp
from jax import lax
from jax.experimental import pallas as pl
from jax.experimental.pallas import tpu as pltpu
from jax.sharding import PartitionSpec as P

WIN_R = 32
WIN_C = 8
SWEEP_TALLY = 16

EDGE = WIN_R // 2
SIDE = WIN_C // 2
LANES = 128
SCALE = 2.0**56
FLOOR = 1e-36
F32 = jnp.float32
BF16 = jnp.bfloat16
MESH = pl.DeviceIdType.MESH


def masked(av, bv, wv, rows, lanes):
    w = wv[rows, lanes].astype(F32)
    return av[0, rows, lanes] * w, av[1, rows, lanes] * w, bv[0, rows, lanes] * w, bv[1, rows, lanes] * w


def encode(ar, ai, br, bi):
    sr, si = ar * SCALE, ai * SCALE
    power = sr * sr + si * si
    some = power > FLOOR
    inverse = lax.rsqrt(jnp.where(some, power, 1.0))
    return (
        jnp.where(some, power * inverse * (1.0 / SCALE), 0.0),
        jnp.where(some, (sr * br + si * bi) * inverse, br),
        jnp.where(some, (si * br - sr * bi) * inverse, bi),
    )


def decode(s, gr, gi):
    return s * gr, s * gi, s * s, gr * gr + gi * gi


def put_split(out, products, places):
    for plane, value in enumerate(products):
        high = value.astype(BF16)
        low = (value - high.astype(F32)).astype(BF16)
        for rows, lanes in places:
            out[0, plane, rows, lanes] = high
            out[1, plane, rows, lanes] = low


def edge_block(pack):
    lane = lax.broadcasted_iota(jnp.int32, pack.shape, 1)
    left, right = lane >= LANES - SIDE, lane < SIDE

    def pick(k):
        a = pack if k == 0 else pltpu.roll(pack, k * SIDE, 1)
        b = pack if k == 0 else pltpu.roll(pack, LANES - k * SIDE, 1)
        return jnp.where(left, a, jnp.where(right, b, 0.0))

    return pick(0), pick(1), pick(2)


def cuts(tiles):
    if tiles < EDGE:
        return ((0, tiles),), ((0, tiles),), ((1, 1),)
    down = [mark * tiles // 16 for mark in (0, 3, 7, 11, 14, 16)]
    up = [mark * tiles // 16 for mark in (0, 5, 9, 13)] + [tiles - 1]
    return tuple(zip(down[:-1], down[1:])), tuple(zip(up[:-1], up[1:])), ((2, 1), (3, 2), (4, 3), (5, 4))


def fold(x):
    total = x[:, 0:LANES]
    for t in range(1, x.shape[1] // LANES):
        total = total + x[:, t * LANES : (t + 1) * LANES]
    return total


def row_sum(x):
    return jnp.sum(x, 1, keepdims=True)


def front_kernel(
    n_rows, n_cols, reach,
    lead, trail, flags, sweep,
    gam, coh, memt, fit,
    av, bv, wv, sv, up_out, down_out, top_in, bot_in, left_out, right_out, left_in, right_in,
    relay_in, corner_in, split, halo_split, boxed, ribbon, across, own_part, row_parts, flag_parts, acc_h,
    tab_out, tab_in,
    load_sem, halo_send, halo_recv, side_send, side_recv, corner_send, corner_recv,
    relay_send, relay_recv, tab_send, tab_recv, token,
):
    me_r, me_c = lax.axis_index("rows"), lax.axis_index("cols")
    height, width = flags.shape
    tiles = width // LANES
    low = height - EDGE
    total_rows, total_cols = height * n_rows, width * n_cols
    chunk = 512 if width % 512 == 0 else LANES
    has_up, has_down = me_r > 0, me_r < n_rows - 1
    has_left, has_right = me_c > 0, me_c < n_cols - 1
    down_cuts, up_cuts, steps = cuts(tiles)
    pair = 2 if tiles % 2 == 0 else 1

    def load(part, rows, lanes=pl.ds(0, width)):
        group = [
            pltpu.make_async_copy(lead.at[:, rows, lanes], av.at[:, rows, lanes], load_sem.at[part, 0]),
            pltpu.make_async_copy(trail.at[:, rows, lanes], bv.at[:, rows, lanes], load_sem.at[part, 1]),
            pltpu.make_async_copy(flags.at[rows, lanes], wv.at[rows, lanes], load_sem.at[part, 2]),
        ]
        for copy in group:
            copy.start()
        return group

    top_rows, low_rows = pl.ds(0, EDGE), pl.ds(low, EDGE)
    tucked = up_cuts[-1][1] == tiles - 1
    first = max(up_cuts[:2][-1][1], down_cuts[:3][-1][1]) * LANES
    loads = [load(0, top_rows, pl.ds(0, first))]
    if first < width:
        if tucked:
            loads.append(load(1, top_rows, pl.ds(width - LANES, LANES)))
        loads.append(load(2, low_rows, pl.ds(0, first)))
    later_loads = []
    if first < width:
        rest = width - first - (LANES if tucked else 0)
        if rest:
            later_loads.append(load(3, top_rows, pl.ds(first, rest)))
        later_loads.append(load(4, low_rows, pl.ds(first, width - first)))
    else:
        later_loads.append(load(4, low_rows))
    sweep_load = pltpu.make_async_copy(sweep, sv, load_sem.at[6, 0])
    sweep_load.start()

    barrier = pltpu.get_barrier_semaphore()
    peers = []
    for dr in range(-reach, reach + 1):
        for dc in range(n_cols):
            if dr == 0 and dc == 0:
                continue
            to = jnp.logical_and(me_r + dr >= 0, me_r + dr < n_rows)
            of = jnp.logical_and(me_r - dr >= 0, me_r - dr < n_rows)
            peers.append(((dr + reach) * n_cols + dc, to, of, me_r + dr, lax.rem(me_c + dc, n_cols)))
    near = reach == 1
    n_greeted = 0
    for slot, to, _, row, col in peers:
        dr, dc = slot // n_cols - reach, slot % n_cols
        if near and dr != 0 and dc != 0:
            continue
        n_greeted = n_greeted + to.astype(jnp.int32)

        @pl.when(to)
        def _():
            pl.semaphore_signal(barrier, inc=1, device_id=(row, col), device_id_type=MESH)

    def remote(src, dst, send, recv, row, col):
        return pltpu.make_async_remote_copy(
            src_ref=src, dst_ref=dst, send_sem=send, recv_sem=recv, device_id=(row, col), device_id_type=MESH
        )

    def cut(ref, piece):
        return ref.at[:, :, pl.ds(piece[0] * LANES, (piece[1] - piece[0]) * LANES)]

    downs = [
        remote(cut(down_out, p), cut(top_in, p), halo_send.at[0, i], halo_recv.at[0, i], me_r + 1, me_c)
        for i, p in enumerate(down_cuts)
    ]
    ups = [
        remote(cut(up_out, p), cut(bot_in, p), halo_send.at[1, i], halo_recv.at[1, i], me_r - 1, me_c)
        for i, p in enumerate(up_cuts)
    ]
    to_right = remote(right_out, left_in, side_send.at[0], side_recv.at[0], me_r, me_c + 1)
    to_left = remote(left_out, right_in, side_send.at[1], side_recv.at[1], me_r, me_c - 1)
    corners = []
    for k, (src, rows, dr, dc, to, of) in enumerate((
        (right_out, low_rows, 1, 1, has_down & has_right, has_up & has_left),
        (left_out, low_rows, 1, -1, has_down & has_left, has_up & has_right),
        (right_out, top_rows, -1, 1, has_up & has_right, has_down & has_left),
        (left_out, top_rows, -1, -1, has_up & has_left, has_down & has_right),
    )):
        copy = remote(src.at[rows], corner_in.at[k], corner_send.at[k], corner_recv.at[k], me_r + dr, me_c + dc)
        corners.append((copy, to, of))

    relayed = 3 if n_rows % 2 == 0 and n_rows > 2 and len(up_cuts) > 3 else 0
    odd = lax.rem(me_r, 2) == 1
    even = jnp.logical_not(odd)
    place = lax.div(me_r, 2) * 4
    n_up = jnp.minimum(relayed, lax.div(place, n_rows // 2)) if relayed else 0
    n_down = jnp.minimum(relayed, 4 - lax.div(place + 4, n_rows // 2)) if relayed else 0
    via = []
    for i in range(relayed):
        p, q = up_cuts[i], down_cuts[i]
        ask_up, ask_down = even & (n_up > i), odd & (n_down > i)
        give_up, give_down = odd & (n_up > i), even & (n_down > i)
        via.append((
            (ask_up, remote(cut(up_out, p), cut(relay_in, p), halo_send.at[1, i], relay_recv.at[i], me_r + 1, me_c)),
            (ask_down, remote(cut(down_out, q), cut(relay_in, q), halo_send.at[0, i], relay_recv.at[i], me_r - 1, me_c)),
            (give_up, remote(cut(relay_in, p), cut(bot_in, p), relay_send.at[i], halo_recv.at[1, i], me_r - 2, me_c)),
            (give_down, remote(cut(relay_in, q), cut(top_in, q), relay_send.at[i], halo_recv.at[0, i], me_r + 2, me_c)),
        ))

    def forward(i):
        if i >= relayed:
            return
        for (_, arrival), (give, copy) in zip(via[i][:2], via[i][2:]):
            @pl.when(give)
            def _():
                arrival.wait_recv()
                copy.start()

    def encode_rows(first, out, piece):
        lanes = pl.ds(piece[0] * LANES, (piece[1] - piece[0]) * LANES)
        for k, value in enumerate(encode(*masked(av, bv, wv, pl.ds(first, EDGE), lanes))):
            out[k, :, lanes] = value

    def pack_sides(b):
        rows = pl.ds(b * 16, 16)
        lane = lax.broadcasted_iota(jnp.int32, (16, LANES), 1)
        s, gr, gi = encode(*masked(av, bv, wv, rows, pl.ds(width - LANES, LANES)))
        right_out[rows, :] = jnp.where(
            lane >= LANES - SIDE,
            s,
            jnp.where(
                lane >= LANES - 2 * SIDE,
                pltpu.roll(gr, LANES - SIDE, 1),
                jnp.where(lane >= LANES - 3 * SIDE, pltpu.roll(gi, LANES - 2 * SIDE, 1), 0.0),
            ),
        )
        s, gr, gi = encode(*masked(av, bv, wv, rows, pl.ds(0, LANES)))
        left_out[rows, :] = jnp.where(
            lane < SIDE,
            s,
            jnp.where(
                lane < 2 * SIDE,
                pltpu.roll(gr, SIDE, 1),
                jnp.where(lane < 3 * SIDE, pltpu.roll(gi, 2 * SIDE, 1), 0.0),
            ),
        )

    for group in loads:
        for copy in group:
            copy.wait()

    def tuck(piece):
        if tucked:
            for t in range(piece[0], min(piece[1], EDGE - 1)):
                for k in range(3):
                    up_out[k, EDGE - 1 : EDGE, t * LANES : (t + 1) * LANES] = up_out[k, t : t + 1, width - LANES : width]

    if first == width:
        for copy in later_loads[0]:
            copy.wait()
    if tucked:
        encode_rows(0, up_out, (tiles - 1, tiles))
    for piece in up_cuts[:2]:
        encode_rows(0, up_out, piece)
        tuck(piece)
    for piece in down_cuts[:3]:
        encode_rows(low, down_out, piece)

    pl.semaphore_wait(barrier, n_greeted)
    n_via = jnp.where(even, n_up, n_down)

    def send(point):
        for v in range(relayed + 1):
            later = [i for i in range(v, len(down_cuts)) if point == (i + 3 if v else i)]
            for parity, straight, other, asked in ((even, downs, ups, 0), (odd, ups, downs, 1)):
                ahead = 2 if v == asked == 0 else 1
                slots = range(ahead + 1) if point == 0 else (point + ahead,)

                @pl.when(parity & (n_via == v))
                def _():
                    far, near_by = (has_up, has_down) if asked == 0 else (has_down, has_up)
                    for k in slots:
                        if k < v:
                            via[k][asked][1].start()
                        elif k - v < len(straight):
                            @pl.when(near_by)
                            def _():
                                straight[k - v].start()
                    for i in (i for i in later if i < len(other)):
                        @pl.when(far)
                        def _():
                            other[i].start()

    send(0)
    if near:
        for dc in range(1, n_cols):
            pl.semaphore_signal(token, inc=1, device_id=(me_r, lax.rem(me_c + dc, n_cols)), device_id_type=MESH)

    if first < width:
        for group in later_loads:
            for copy in group:
                copy.wait()
        for piece in up_cuts[2:]:
            encode_rows(0, up_out, piece)
            tuck(piece)
        for piece in down_cuts[3:]:
            encode_rows(low, down_out, piece)
    bulk = load(5, pl.ds(EDGE, low - EDGE))
    for b in (0, height // 16 - 1):
        pack_sides(b)
    for copy in bulk:
        copy.wait()

    for b in range(1, height // 16 - 1):
        pack_sides(b)

    @pl.when(has_right)
    def _():
        to_right.start()

    @pl.when(has_left)
    def _():
        to_left.start()

    @pl.when(jnp.logical_not(has_left))
    def _():
        left_in[...] = jnp.zeros_like(left_in)

    @pl.when(jnp.logical_not(has_right))
    def _():
        right_in[...] = jnp.zeros_like(right_in)

    @pl.when(jnp.logical_not(has_up))
    def _():
        top_in[...] = jnp.zeros_like(top_in)

    @pl.when(jnp.logical_not(has_down))
    def _():
        bot_in[...] = jnp.zeros_like(bot_in)

    for k, (_, _, of) in enumerate(corners):
        @pl.when(jnp.logical_not(of))
        def _():
            corner_in[k] = jnp.zeros((EDGE, LANES), F32)

    for slot, _, of, _, _ in peers:
        @pl.when(jnp.logical_not(of))
        def _():
            tab_in[slot] = jnp.zeros((1, 2 * LANES), F32)

    if near:
        pl.semaphore_wait(token, n_cols - 1)
    for copy, to, _ in corners:
        @pl.when(to)
        def _():
            copy.start()

    lane_all = lax.broadcasted_iota(jnp.int32, (8, width), 1) + me_c * width
    across[...] = (lane_all.astype(F32) + 0.5) * (2.0 / total_cols) - 1.0

    @pl.loop(0, height // 16)
    def _(b):
        rows = pl.ds(pl.multiple_of(b * 16, 16), 16)

        @pl.loop(0, width // chunk)
        def _(c):
            lanes = pl.ds(pl.multiple_of(c * chunk, chunk), chunk)
            ar, ai, br, bi = masked(av, bv, wv, rows, lanes)
            put_split(
                split,
                (ar * br + ai * bi, ai * br - ar * bi, ar * ar + ai * ai, br * br + bi * bi),
                [(rows, pl.ds(pl.multiple_of(LANES + c * chunk, LANES), chunk))],
            )

    send(1)
    reach_in = (pair + 2) * LANES
    i = lax.broadcasted_iota(jnp.int32, (reach_in, pair * LANES), 0)
    j = lax.broadcasted_iota(jnp.int32, (reach_in, pair * LANES), 1) + LANES
    ribbon[...] = jnp.logical_and(i >= j - SIDE, i < j + SIDE).astype(F32).astype(BF16)

    def box_across(j):
        inner = pl.ds(pl.multiple_of(j * pair * LANES, pair * LANES), reach_in)
        outer = pl.ds(pl.multiple_of(j * pair * LANES, pair * LANES), pair * LANES)
        for plane in range(4):
            sums = jnp.dot(split[0, plane, :, inner], ribbon[...], preferred_element_type=F32)
            sums = sums + jnp.dot(split[1, plane, :, inner], ribbon[...], preferred_element_type=F32)
            boxed[plane, EDGE : EDGE + height, outer] = sums

    last = tiles // pair - 1
    middle = max(1, tiles // pair // 2)

    @pl.loop(1, middle)
    def _(j):
        box_across(j)

    send(2)

    @pl.loop(middle, max(middle, last))
    def _(j):
        box_across(j)

    @pl.when(has_left)
    def _():
        to_right.wait_recv()

    @pl.when(has_right)
    def _():
        to_left.wait_recv()

    sides = [pl.ds(0, LANES), pl.ds(LANES + width, LANES)]
    for b in range(height // 16):
        rows = pl.ds(b * 16, 16)
        lane = lax.broadcasted_iota(jnp.int32, (16, LANES), 1)
        pack = jnp.where(lane >= LANES // 2, left_in[rows, :], right_in[rows, :])
        put_split(split, decode(*edge_block(pack)), [(rows, lanes) for lanes in sides])

    send(3)
    forward(0)
    forward(1)
    for j in sorted({0, last}):
        box_across(j)

    sweep_load.wait()
    kind = lax.rem(lax.broadcasted_iota(jnp.int32, (LANES, height), 0), SWEEP_TALLY)
    memt[...] = (kind == sv[...]).astype(F32).T
    row_parts[...] = jnp.zeros_like(row_parts)

    group_lane = lax.broadcasted_iota(jnp.int32, (8, LANES), 1) // SWEEP_TALLY

    def row_v(group):
        row = lax.broadcasted_iota(jnp.int32, (8, LANES), 0) + (me_r * height + group * 8)
        return (row.astype(F32) + 0.5) * (2.0 / total_rows) - 1.0

    def arrange(group, values):
        table = values[0]
        for m, value in enumerate(values):
            table = value if m == 0 else jnp.where(group_lane >= m, value, table)
        return memt[group * 8 : group * 8 + 8, :] * jnp.where(group_lane < len(values), table, 0.0)

    @pl.loop(0, height // 8)
    def _(b):
        w = wv[pl.ds(pl.multiple_of(b * 8, 8), 8), :].astype(F32)
        u = across[...]
        wu = w * u
        for m, value in enumerate((w, wu, wu * u)):
            flag_parts[b, m] = fold(value)

    acc_g = None
    for b in range(height // 8):
        s0, su, suu = [row_sum(flag_parts[b, m]) for m in range(3)]
        v = row_v(b)
        part = arrange(b, (s0, su, v * s0, suu, v * su, v * v * s0))
        acc_g = part if acc_g is None else acc_g + part
    tab_out[:, 0:LANES] = jnp.sum(acc_g, 0, keepdims=True)

    send(4)
    sub = lax.broadcasted_iota(jnp.int32, (8, LANES), 0)

    edge_groups, groups = EDGE // 8, height // 8

    def shifted(x, following):
        n1, n2, n4 = following if following else (None, None, None)
        r1 = pltpu.roll(x, 7, 0)
        y1 = x + (r1 if n1 is None else jnp.where(sub < 7, r1, n1))
        r2 = pltpu.roll(y1, 6, 0)
        y2 = y1 + (r2 if n2 is None else jnp.where(sub < 6, r2, n2))
        r4 = pltpu.roll(y2, 4, 0)
        return y2 + (r4 if n4 is None else jnp.where(sub < 4, r4, n4)), (r1, r2, r4)

    def emit(g, lanes, window):
        rows = slice(g * 8, g * 8 + 8)
        inverse = lax.rsqrt((window[2] + 1.0) * (window[3] + 1.0))
        real, imag = window[0] * inverse, window[1] * inverse
        gam[0, rows, lanes] = real
        gam[1, rows, lanes] = imag
        coh[rows, lanes] = jnp.sqrt(real * real + imag * imag)
        w, u = wv[rows, lanes].astype(F32), across[:, lanes]
        wr, wi = w * real, w * imag
        for m, value in enumerate((wr, wi, wr * u, wi * u)):
            row_parts[g, m] += value

    def group_rows(g):
        return slice(g * 8, g * 8 + 8)

    def finish(t):
        lanes = pl.ds(pl.multiple_of(t * LANES, LANES), LANES)
        eights = [[None] * 4 for _ in range(groups + 2)]
        pairs = [[None] * 4 for _ in range(groups + 2)]
        following = [None] * 4
        for g in range(groups + 1, edge_groups - 1, -1):
            for plane in range(4):
                eights[g][plane], following[plane] = shifted(boxed[plane, group_rows(g), lanes], following[plane])
                if g <= groups - 1:
                    pairs[g][plane] = eights[g][plane] + eights[g + 1][plane]
            if g <= groups - 3:
                emit(g, lanes, [pairs[g][p] + pairs[g + 2][p] for p in range(4)])
        for p in range(4):
            kept = (
                pairs[edge_groups][p], eights[edge_groups][p] + pairs[edge_groups + 1][p], *following[p],
                eights[groups - 2][p] + pairs[groups - 1][p], pairs[groups - 1][p],
            )
            for k, value in enumerate(kept):
                own_part[p, k, :, lanes] = value

    def finish_edges(t):
        lanes = pl.ds(pl.multiple_of(t * LANES, LANES), LANES)
        outer, inner = [None] * 4, [None] * 4
        for p in range(4):
            near, following = shifted(boxed[p, group_rows(1), lanes], [own_part[p, k, :, lanes] for k in (2, 3, 4)])
            far, _ = shifted(boxed[p, group_rows(0), lanes], following)
            inner[p] = near + own_part[p, 1, :, lanes]
            outer[p] = far + near + own_part[p, 0, :, lanes]
        emit(0, lanes, outer)
        emit(1, lanes, inner)
        for p in range(4):
            _, following = shifted(boxed[p, group_rows(groups + 3), lanes], None)
            far, following = shifted(boxed[p, group_rows(groups + 2), lanes], following)
            near, _ = shifted(boxed[p, group_rows(groups + 1), lanes], following)
            inner[p] = near + own_part[p, 5, :, lanes]
            outer[p] = near + far + own_part[p, 6, :, lanes]
        emit(groups - 2, lanes, inner)
        emit(groups - 1, lanes, outer)

    def add_rows(groups):
        total = None
        for g in groups:
            hr, hi, hur, hui = [row_sum(row_parts[g, m]) for m in range(4)]
            v = row_v(g)
            part = arrange(g, (hr, hi, hur, hui, v * hr, v * hi))
            total = part if total is None else total + part
        return total

    @pl.loop(0, tiles // 2)
    def _(t):
        finish(t)

    send(5)
    forward(2)

    @pl.loop(tiles // 2, tiles)
    def _(t):
        finish(t)

    send(6)

    acc_h[...] = add_rows(range(edge_groups, groups - edge_groups))

    def put_halo(part, products, where):
        for plane, value in enumerate(products):
            first = (plane * 2 + part) * EDGE
            high = value.astype(BF16)
            low_part = (value - high.astype(F32)).astype(BF16)
            for lanes in where:
                halo_split[first : first + EDGE, lanes] = high
                halo_split[8 * EDGE + first : 9 * EDGE + first, lanes] = low_part

    def box_halo(j):
        inner = pl.ds(j * pair * LANES, reach_in)
        outer = pl.ds(j * pair * LANES, pair * LANES)
        sums = jnp.dot(halo_split[:, inner], ribbon[...], preferred_element_type=F32)
        for plane in range(4):
            for part, target in enumerate((0, EDGE + height)):
                first = (plane * 2 + part) * EDGE
                boxed[plane, target : target + EDGE, outer] = (
                    sums[first : first + EDGE] + sums[8 * EDGE + first : 9 * EDGE + first]
                )

    done = 0
    had_down, had_up = 0, 0
    for i, (need_down, need_up) in enumerate(steps):
        if i == 0:
            for copy, _, of in corners:
                @pl.when(of)
                def _():
                    copy.wait_recv()

            lane = lax.broadcasted_iota(jnp.int32, (EDGE, LANES), 1)
            packs = [jnp.where(lane >= LANES // 2, corner_in[k], corner_in[k + 1]) for k in (0, 2)]
            for part, pack in enumerate(packs):
                put_halo(part, decode(*edge_block(pack)), sides)

        @pl.when(has_up)
        def _():
            for copy in downs[had_down:need_down]:
                copy.wait_recv()

        @pl.when(has_down)
        def _():
            for copy in ups[had_up:need_up]:
                copy.wait_recv()

        end_up = up_cuts[need_up - 1][1]
        if tucked and i == len(steps) - 1:
            end_up = tiles
            for t in range(EDGE - 1):
                for k in range(3):
                    bot_in[k, t : t + 1, width - LANES : width] = bot_in[k, EDGE - 1 : EDGE, t * LANES : (t + 1) * LANES]
        ranges = ((down_cuts[had_down][0], down_cuts[need_down - 1][1]), (up_cuts[had_up][0], end_up))
        for part, (halo, (start, end)) in enumerate(zip((top_in, bot_in), ranges)):
            source = pl.ds(start * LANES, (end - start) * LANES)
            target = pl.ds((start + 1) * LANES, (end - start) * LANES)
            put_halo(part, decode(*[halo[m, :, source] for m in range(3)]), [target])
        had_down, had_up = need_down, need_up
        ready = tiles // pair if i == len(steps) - 1 else max(0, (min(ranges[0][1], ranges[1][1]) - 1) // pair)
        for j in range(done, ready):
            box_halo(j)
        if ready > done:
            @pl.loop(done, ready)
            def _(j):
                for t in range(pair):
                    finish_edges(j * pair + t)
        done = ready
        if i == 0:
            send(7)

    acc_last = acc_h[...] + add_rows(list(range(edge_groups)) + list(range(groups - edge_groups, groups)))
    tab_out[:, LANES:] = jnp.sum(acc_last, 0, keepdims=True)
    swaps = [
        (remote(tab_out, tab_in.at[slot], tab_send.at[slot], tab_recv.at[slot], row, col), to, of)
        for slot, to, of, row, col in peers
    ]
    for copy, to, _ in swaps:
        @pl.when(to)
        def _():
            copy.start()

    tab_in[reach * n_cols] = tab_out[...]
    @pl.when(has_down)
    def _():
        for copy in downs:
            copy.wait_send()

    @pl.when(has_up)
    def _():
        for copy in ups:
            copy.wait_send()

    for copy, to, _ in corners:
        @pl.when(to)
        def _():
            copy.wait_send()

    for group in via:
        for give, copy in group[2:]:
            @pl.when(give)
            def _():
                copy.wait_send()

    @pl.when(has_right)
    def _():
        to_right.wait_send()

    @pl.when(has_left)
    def _():
        to_left.wait_send()

    for copy, _, of in swaps:
        @pl.when(of)
        def _():
            copy.wait_recv()

    total = functools.reduce(jnp.add, [tab_in[slot] for slot in range(tab_in.shape[0])])

    def column(base, m):
        part = total[:, base : base + LANES]
        return part if m == 0 else pltpu.roll(part, LANES - m * SWEEP_TALLY, 1)

    s0, su, sv_, suu, suv, svv = [column(0, m) for m in range(6)]
    hr, hi, hur, hui, hvr, hvi = [column(LANES, m) for m in range(6)]
    floored = jnp.maximum(s0, 1.0)
    mid_u, mid_v = su / floored, sv_ / floored
    guu = suu - 2.0 * mid_u * su + mid_u * mid_u * s0
    guv = suv - mid_u * sv_ - mid_v * su + mid_u * mid_v * s0
    gvv = svv - 2.0 * mid_v * sv_ + mid_v * mid_v * s0
    hur, hui = hur - mid_u * hr, hui - mid_u * hi
    hvr, hvi = hvr - mid_v * hr, hvi - mid_v * hi
    ridge = 0.001 * s0 + 1.0
    duu, dvv = guu + ridge, gvv + ridge
    scale = 1.0 / (duu * dvv - guv * guv)
    base = 1.0 / (s0 + ridge)
    c1r, c1i = (dvv * hur - guv * hvr) * scale, (dvv * hui - guv * hvi) * scale
    c2r, c2i = (duu * hvr - guv * hur) * scale, (duu * hvi - guv * hui) * scale
    valid = lax.broadcasted_iota(jnp.int32, (1, LANES), 1) < SWEEP_TALLY
    rows_out = (hr * base - c1r * mid_u, hi * base - c1i * mid_u, c1r, c1i, c2r, c2i, mid_v)
    for m, value in enumerate(rows_out):
        fit[m : m + 1, :] = jnp.where(valid, value, 0.0)

    for copy, to, _ in swaps:
        @pl.when(to)
        def _():
            copy.wait_send()


def back_kernel(n_rows, n_cols, block, gam, coh, memt, fit, ramped, coherence, out, across, lines, sem):
    height, width = coh.shape
    me_r, me_c = lax.axis_index("rows"), lax.axis_index("cols")
    coh_copy = pltpu.make_async_copy(coh, coherence, sem.at[0])
    coh_copy.start()
    for g in range(height // 8):
        row = lax.broadcasted_iota(jnp.int32, (8, LANES), 0) + (me_r * height + g * 8)
        dv = (row.astype(F32) + 0.5) * (2.0 / (height * n_rows)) - 1.0 - fit[6:7, :]
        one = memt[g * 8 : g * 8 + 8, :]
        for m, value in enumerate((fit[0:1, :] + fit[4:5, :] * dv, fit[1:2, :] + fit[5:6, :] * dv, fit[2:3, :], fit[3:4, :])):
            lines[g, m] = jnp.broadcast_to(row_sum(one * value), (8, LANES))
    lane_all = lax.broadcasted_iota(jnp.int32, (8, width), 1) + me_c * width
    across[...] = (lane_all.astype(F32) + 0.5) * (2.0 / (width * n_cols)) - 1.0

    copies = []
    for i in range(height // block):
        @pl.loop(0, block // 8)
        def _(b):
            g = i * (block // 8) + b
            rows = pl.ds(pl.multiple_of(g * 8, 8), 8)
            base_r, base_i, slope_r, slope_i = [lines[g, m] for m in range(4)]
            for t in range(width // LANES):
                lanes = slice(t * LANES, (t + 1) * LANES)
                real, imag, u = gam[0, rows, lanes], gam[1, rows, lanes], across[:, lanes]
                model_real = base_r + slope_r * u
                model_imag = base_i + slope_i * u
                out[0, rows, lanes] = real * model_real + imag * model_imag
                out[1, rows, lanes] = imag * model_real - real * model_imag

        rows = pl.ds(i * block, block)
        copy = pltpu.make_async_copy(out.at[:, rows, :], ramped.at[:, rows, :], sem.at[1 + i])
        copy.start()
        copies.append(copy)
    coh_copy.wait()
    for copy in copies:
        copy.wait()


def on_device(n_rows, n_cols, lead, trail, flags, sweep):
    height, width = flags.shape
    wide = width + 2 * LANES
    longest = 2 * height * n_rows // SWEEP_TALLY
    reach = max(1, min(n_rows - 1, (longest - 2) // height + 1))
    slots = (2 * reach + 1) * n_cols
    pieces = len(cuts(width // LANES)[0])
    pair = 2 if width // LANES % 2 == 0 else 1
    hbm = pl.BlockSpec(memory_space=pltpu.HBM)
    vmem = pl.BlockSpec(memory_space=pltpu.VMEM)
    dma = pltpu.SemaphoreType.DMA
    gam, coh, memt, fit = pl.pallas_call(
        functools.partial(front_kernel, n_rows, n_cols, reach),
        out_shape=[
            pltpu.VMEM((2, height, width), F32),
            pltpu.VMEM((height, width), F32),
            pltpu.VMEM((height, LANES), F32),
            pltpu.VMEM((8, LANES), F32),
        ],
        in_specs=[hbm, hbm, hbm, hbm],
        out_specs=[vmem, vmem, vmem, vmem],
        scratch_shapes=[
            pltpu.VMEM((2, height, width), F32),
            pltpu.VMEM((2, height, width), F32),
            pltpu.VMEM((height, width), jnp.int32),
            pltpu.VMEM((1, height), jnp.int32),
            pltpu.VMEM((3, EDGE, width), F32),
            pltpu.VMEM((3, EDGE, width), F32),
            pltpu.VMEM((3, EDGE, width), F32),
            pltpu.VMEM((3, EDGE, width), F32),
            pltpu.VMEM((height, LANES), F32),
            pltpu.VMEM((height, LANES), F32),
            pltpu.VMEM((height, LANES), F32),
            pltpu.VMEM((height, LANES), F32),
            pltpu.VMEM((3, EDGE, width), F32),
            pltpu.VMEM((4, EDGE, LANES), F32),
            pltpu.VMEM((2, 4, height, wide), BF16),
            pltpu.VMEM((16 * EDGE, wide), BF16),
            pltpu.VMEM((4, height + 2 * EDGE, width), F32),
            pltpu.VMEM(((pair + 2) * LANES, pair * LANES), BF16),
            pltpu.VMEM((8, width), F32),
            pltpu.VMEM((4, 7, 8, width), F32),
            pltpu.VMEM((height // 8, 4, 8, LANES), F32),
            pltpu.VMEM((height // 8, 3, 8, LANES), F32),
            pltpu.VMEM((8, LANES), F32),
            pltpu.VMEM((1, 2 * LANES), F32),
            pltpu.VMEM((slots, 1, 2 * LANES), F32),
            dma((7, 3)),
            dma((2, pieces)), dma((2, pieces)),
            dma((2,)), dma((2,)),
            dma((4,)), dma((4,)),
            dma((pieces,)), dma((pieces,)),
            dma((slots,)), dma((slots,)),
            pltpu.SemaphoreType.REGULAR,
        ],
        compiler_params=pltpu.CompilerParams(
            collective_id=0, has_side_effects=True, vmem_limit_bytes=60 * 1024 * 1024
        ),
        name="front",
    )(lead, trail, flags, sweep.reshape(1, height))
    block = 16 if height % 16 == 0 else 8
    return pl.pallas_call(
        functools.partial(back_kernel, n_rows, n_cols, block),
        out_shape=[
            jax.ShapeDtypeStruct((2, height, width), F32),
            jax.ShapeDtypeStruct((height, width), F32),
        ],
        in_specs=[vmem, vmem, vmem, vmem],
        out_specs=[hbm, hbm],
        scratch_shapes=[
            pltpu.VMEM((2, height, width), F32),
            pltpu.VMEM((8, width), F32),
            pltpu.VMEM((height // 8, 4, 8, LANES), F32),
            dma((1 + height // block,)),
        ],
        compiler_params=pltpu.CompilerParams(vmem_limit_bytes=16 * 1024 * 1024),
        name="back",
    )(gam, coh, memt, fit)


def solution(mesh):
    return jax.shard_map(
        functools.partial(on_device, mesh.shape["rows"], mesh.shape["cols"]),
        mesh=mesh,
        in_specs=(P(None, "rows", "cols"), P(None, "rows", "cols"), P("rows", "cols"), P("rows")),
        out_specs=(P(None, "rows", "cols"), P("rows", "cols")),
        check_vma=False,
    )
```

```python
import functools

import jax
import jax.numpy as jnp
from jax import lax
from jax.experimental import pallas as pl
from jax.experimental.pallas import tpu as pltpu
from jax.sharding import PartitionSpec as P

WIN_R = 32
WIN_C = 8
SWEEP_TALLY = 16

EDGE = WIN_R // 2
SIDE = WIN_C // 2
LANES = 128
SCALE = 2.0**56
FLOOR = 1e-36
F32 = jnp.float32
BF16 = jnp.bfloat16
MESH = pl.DeviceIdType.MESH


def masked(av, bv, wv, rows, lanes):
    w = wv[rows, lanes].astype(F32)
    return av[0, rows, lanes] * w, av[1, rows, lanes] * w, bv[0, rows, lanes] * w, bv[1, rows, lanes] * w


def encode(ar, ai, br, bi):
    sr, si = ar * SCALE, ai * SCALE
    power = sr * sr + si * si
    some = power > FLOOR
    inverse = lax.rsqrt(jnp.where(some, power, 1.0))
    return (
        jnp.where(some, power * inverse * (1.0 / SCALE), 0.0),
        jnp.where(some, (sr * br + si * bi) * inverse, br),
        jnp.where(some, (si * br - sr * bi) * inverse, bi),
    )


def decode(s, gr, gi):
    return s * gr, s * gi, s * s, gr * gr + gi * gi


def put_split(out, products, places):
    for plane, value in enumerate(products):
        high = value.astype(BF16)
        low = (value - high.astype(F32)).astype(BF16)
        for rows, lanes in places:
            out[0, plane, rows, lanes] = high
            out[1, plane, rows, lanes] = low


def edge_block(pack):
    lane = lax.broadcasted_iota(jnp.int32, pack.shape, 1)
    left, right = lane >= LANES - SIDE, lane < SIDE

    def pick(k):
        a = pack if k == 0 else pltpu.roll(pack, k * SIDE, 1)
        b = pack if k == 0 else pltpu.roll(pack, LANES - k * SIDE, 1)
        return jnp.where(left, a, jnp.where(right, b, 0.0))

    return pick(0), pick(1), pick(2)


def cuts(tiles):
    if tiles < EDGE:
        return ((0, tiles),), ((0, tiles),), ((1, 1),)
    down = [mark * tiles // 16 for mark in (0, 3, 7, 11, 14, 16)]
    up = [mark * tiles // 16 for mark in (0, 5, 9, 13)] + [tiles - 1]
    return tuple(zip(down[:-1], down[1:])), tuple(zip(up[:-1], up[1:])), ((2, 1), (3, 2), (4, 3), (5, 4))


def fold(x):
    total = x[:, 0:LANES]
    for t in range(1, x.shape[1] // LANES):
        total = total + x[:, t * LANES : (t + 1) * LANES]
    return total


def row_sum(x):
    return jnp.sum(x, 1, keepdims=True)


def front_kernel(
    n_rows, n_cols, reach,
    lead, trail, flags, sweep,
    gam, coh, memt, fit,
    av, bv, wv, sv, up_out, down_out, top_in, bot_in, left_out, right_out, left_in, right_in,
    relay_in, corner_out, corner_in, split, halo_split, boxed, ribbon, across, own_part, row_parts, flag_parts, acc_h,
    tab_out, tab_in,
    load_sem, halo_send, halo_recv, side_send, side_recv, corner_send, corner_recv,
    relay_send, relay_recv, tab_send, tab_recv, token,
):
    me_r, me_c = lax.axis_index("rows"), lax.axis_index("cols")
    height, width = flags.shape
    tiles = width // LANES
    low = height - EDGE
    total_rows, total_cols = height * n_rows, width * n_cols
    chunk = 512 if width % 512 == 0 else LANES
    has_up, has_down = me_r > 0, me_r < n_rows - 1
    has_left, has_right = me_c > 0, me_c < n_cols - 1
    down_cuts, up_cuts, steps = cuts(tiles)
    pair = 2 if tiles % 2 == 0 else 1

    def load(part, rows, lanes=pl.ds(0, width)):
        group = [
            pltpu.make_async_copy(lead.at[:, rows, lanes], av.at[:, rows, lanes], load_sem.at[part, 0]),
            pltpu.make_async_copy(trail.at[:, rows, lanes], bv.at[:, rows, lanes], load_sem.at[part, 1]),
            pltpu.make_async_copy(flags.at[rows, lanes], wv.at[rows, lanes], load_sem.at[part, 2]),
        ]
        for copy in group:
            copy.start()
        return group

    top_rows, low_rows = pl.ds(0, EDGE), pl.ds(low, EDGE)
    tucked = up_cuts[-1][1] == tiles - 1
    first = max(up_cuts[:2][-1][1], down_cuts[:3][-1][1]) * LANES
    loads = [load(0, top_rows, pl.ds(0, first))]
    if first < width:
        if tucked:
            loads.append(load(1, top_rows, pl.ds(width - LANES, LANES)))
        loads.append(load(2, low_rows, pl.ds(0, first)))
    later_loads = []
    if first < width:
        rest = width - first - (LANES if tucked else 0)
        if rest:
            later_loads.append(load(3, top_rows, pl.ds(first, rest)))
        later_loads.append(load(4, low_rows, pl.ds(first, width - first)))
    else:
        later_loads.append(load(4, low_rows))
    sweep_load = pltpu.make_async_copy(sweep, sv, load_sem.at[6, 0])
    sweep_load.start()

    barrier = pltpu.get_barrier_semaphore()
    peers = []
    for dr in range(-reach, reach + 1):
        for dc in range(n_cols):
            if dr == 0 and dc == 0:
                continue
            to = jnp.logical_and(me_r + dr >= 0, me_r + dr < n_rows)
            of = jnp.logical_and(me_r - dr >= 0, me_r - dr < n_rows)
            peers.append(((dr + reach) * n_cols + dc, to, of, me_r + dr, lax.rem(me_c + dc, n_cols)))
    near = reach == 1
    n_greeted = 0
    for slot, to, _, row, col in peers:
        dr, dc = slot // n_cols - reach, slot % n_cols
        if near and dr != 0 and dc != 0:
            continue
        n_greeted = n_greeted + to.astype(jnp.int32)

        @pl.when(to)
        def _():
            pl.semaphore_signal(barrier, inc=1, device_id=(row, col), device_id_type=MESH)

    def remote(src, dst, send, recv, row, col):
        return pltpu.make_async_remote_copy(
            src_ref=src, dst_ref=dst, send_sem=send, recv_sem=recv, device_id=(row, col), device_id_type=MESH
        )

    def cut(ref, piece):
        return ref.at[:, :, pl.ds(piece[0] * LANES, (piece[1] - piece[0]) * LANES)]

    downs = [
        remote(cut(down_out, p), cut(top_in, p), halo_send.at[0, i], halo_recv.at[0, i], me_r + 1, me_c)
        for i, p in enumerate(down_cuts)
    ]
    ups = [
        remote(cut(up_out, p), cut(bot_in, p), halo_send.at[1, i], halo_recv.at[1, i], me_r - 1, me_c)
        for i, p in enumerate(up_cuts)
    ]
    to_right = remote(right_out, left_in, side_send.at[0], side_recv.at[0], me_r, me_c + 1)
    to_left = remote(left_out, right_in, side_send.at[1], side_recv.at[1], me_r, me_c - 1)
    corners = []
    for k, (dr, dc, to, of) in enumerate((
        (1, 1, has_down & has_right, has_up & has_left),
        (1, -1, has_down & has_left, has_up & has_right),
        (-1, 1, has_up & has_right, has_down & has_left),
        (-1, -1, has_up & has_left, has_down & has_right),
    )):
        copy = remote(corner_out.at[k], corner_in.at[k], corner_send.at[k], corner_recv.at[k], me_r + dr, me_c + dc)
        corners.append((copy, to, of))

    relayed = 3 if n_rows % 2 == 0 and n_rows > 2 and len(up_cuts) > 3 else 0
    odd = lax.rem(me_r, 2) == 1
    even = jnp.logical_not(odd)
    place = lax.div(me_r, 2) * 4
    n_up = jnp.minimum(relayed, lax.div(place, n_rows // 2)) if relayed else 0
    n_down = jnp.minimum(relayed, 4 - lax.div(place + 4, n_rows // 2)) if relayed else 0
    via = []
    for i in range(relayed):
        p, q = up_cuts[i], down_cuts[i]
        ask_up, ask_down = even & (n_up > i), odd & (n_down > i)
        give_up, give_down = odd & (n_up > i), even & (n_down > i)
        via.append((
            (ask_up, remote(cut(up_out, p), cut(relay_in, p), halo_send.at[1, i], relay_recv.at[i], me_r + 1, me_c)),
            (ask_down, remote(cut(down_out, q), cut(relay_in, q), halo_send.at[0, i], relay_recv.at[i], me_r - 1, me_c)),
            (give_up, remote(cut(relay_in, p), cut(bot_in, p), relay_send.at[i], halo_recv.at[1, i], me_r - 2, me_c)),
            (give_down, remote(cut(relay_in, q), cut(top_in, q), relay_send.at[i], halo_recv.at[0, i], me_r + 2, me_c)),
        ))

    def forward(i):
        if i >= relayed:
            return
        for (_, arrival), (give, copy) in zip(via[i][:2], via[i][2:]):
            @pl.when(give)
            def _():
                arrival.wait_recv()
                copy.start()

    def encode_rows(first, out, piece):
        lanes = pl.ds(piece[0] * LANES, (piece[1] - piece[0]) * LANES)
        for k, value in enumerate(encode(*masked(av, bv, wv, pl.ds(first, EDGE), lanes))):
            out[k, :, lanes] = value

    def pack_sides(b):
        rows = pl.ds(b * 16, 16)
        lane = lax.broadcasted_iota(jnp.int32, (16, LANES), 1)
        s, gr, gi = encode(*masked(av, bv, wv, rows, pl.ds(width - LANES, LANES)))
        right_out[rows, :] = jnp.where(
            lane >= LANES - SIDE,
            s,
            jnp.where(
                lane >= LANES - 2 * SIDE,
                pltpu.roll(gr, LANES - SIDE, 1),
                jnp.where(lane >= LANES - 3 * SIDE, pltpu.roll(gi, LANES - 2 * SIDE, 1), 0.0),
            ),
        )
        s, gr, gi = encode(*masked(av, bv, wv, rows, pl.ds(0, LANES)))
        left_out[rows, :] = jnp.where(
            lane < SIDE,
            s,
            jnp.where(
                lane < 2 * SIDE,
                pltpu.roll(gr, SIDE, 1),
                jnp.where(lane < 3 * SIDE, pltpu.roll(gi, 2 * SIDE, 1), 0.0),
            ),
        )

    for group in loads:
        for copy in group:
            copy.wait()

    def tuck(piece):
        if tucked:
            for t in range(piece[0], min(piece[1], EDGE - 1)):
                for k in range(3):
                    up_out[k, EDGE - 1 : EDGE, t * LANES : (t + 1) * LANES] = up_out[k, t : t + 1, width - LANES : width]

    if first == width:
        for copy in later_loads[0]:
            copy.wait()
    if tucked:
        encode_rows(0, up_out, (tiles - 1, tiles))
    for piece in up_cuts[:2]:
        encode_rows(0, up_out, piece)
        tuck(piece)
    for piece in down_cuts[:3]:
        encode_rows(low, down_out, piece)

    pl.semaphore_wait(barrier, n_greeted)
    n_via = jnp.where(even, n_up, n_down)

    def send(point):
        for v in range(relayed + 1):
            later = [i for i in range(v, len(down_cuts)) if point == (i + 3 if v else i)]
            for parity, straight, other, asked in ((even, downs, ups, 0), (odd, ups, downs, 1)):
                ahead = 2 if v == asked == 0 else 1
                slots = range(ahead + 1) if point == 0 else (point + ahead,)

                @pl.when(parity & (n_via == v))
                def _():
                    far, near_by = (has_up, has_down) if asked == 0 else (has_down, has_up)
                    for k in slots:
                        if k < v:
                            via[k][asked][1].start()
                        elif k - v < len(straight):
                            @pl.when(near_by)
                            def _():
                                straight[k - v].start()
                    for i in (i for i in later if i < len(other)):
                        @pl.when(far)
                        def _():
                            other[i].start()

    send(0)
    if near:
        for dc in range(1, n_cols):
            pl.semaphore_signal(token, inc=1, device_id=(me_r, lax.rem(me_c + dc, n_cols)), device_id_type=MESH)

    if first < width:
        for group in later_loads:
            for copy in group:
                copy.wait()
        for piece in up_cuts[2:]:
            encode_rows(0, up_out, piece)
            tuck(piece)
        for piece in down_cuts[3:]:
            encode_rows(low, down_out, piece)
    bulk = load(5, pl.ds(EDGE, low - EDGE))
    for b in (0, height // 16 - 1):
        pack_sides(b)
    sub = lax.broadcasted_iota(jnp.int32, (8, LANES), 0)
    for k, (src, start, sign) in enumerate(
        ((right_out, low, -1), (left_out, low, 1), (right_out, 0, -1), (left_out, 0, 1))
    ):
        for part in range(EDGE // 8):
            block = src[start + part * 8 : start + part * 8 + 8, :]
            line = jnp.where(sub == 0, block, 0.0)
            for m in range(1, 8):
                line = line + pltpu.roll(jnp.where(sub == m, block, 0.0), sign * 3 * SIDE * m % LANES, 1)
            corner_out[k, :, part * LANES : (part + 1) * LANES] = jnp.sum(line, 0, keepdims=True)
    for copy in bulk:
        copy.wait()

    for b in range(1, height // 16 - 1):
        pack_sides(b)

    @pl.when(has_right)
    def _():
        to_right.start()

    @pl.when(has_left)
    def _():
        to_left.start()

    @pl.when(jnp.logical_not(has_left))
    def _():
        left_in[...] = jnp.zeros_like(left_in)

    @pl.when(jnp.logical_not(has_right))
    def _():
        right_in[...] = jnp.zeros_like(right_in)

    @pl.when(jnp.logical_not(has_up))
    def _():
        top_in[...] = jnp.zeros_like(top_in)

    @pl.when(jnp.logical_not(has_down))
    def _():
        bot_in[...] = jnp.zeros_like(bot_in)

    for k, (_, _, of) in enumerate(corners):
        @pl.when(jnp.logical_not(of))
        def _():
            corner_in[k] = jnp.zeros((1, EDGE // 8 * LANES), F32)

    for slot, _, of, _, _ in peers:
        @pl.when(jnp.logical_not(of))
        def _():
            tab_in[slot] = jnp.zeros((1, 2 * LANES), F32)

    if near:
        pl.semaphore_wait(token, n_cols - 1)
    for copy, to, _ in corners:
        @pl.when(to)
        def _():
            copy.start()

    lane_all = lax.broadcasted_iota(jnp.int32, (8, width), 1) + me_c * width
    across[...] = (lane_all.astype(F32) + 0.5) * (2.0 / total_cols) - 1.0

    @pl.loop(0, height // 16)
    def _(b):
        rows = pl.ds(pl.multiple_of(b * 16, 16), 16)

        @pl.loop(0, width // chunk)
        def _(c):
            lanes = pl.ds(pl.multiple_of(c * chunk, chunk), chunk)
            ar, ai, br, bi = masked(av, bv, wv, rows, lanes)
            put_split(
                split,
                (ar * br + ai * bi, ai * br - ar * bi, ar * ar + ai * ai, br * br + bi * bi),
                [(rows, pl.ds(pl.multiple_of(LANES + c * chunk, LANES), chunk))],
            )

    send(1)
    reach_in = (pair + 2) * LANES
    i = lax.broadcasted_iota(jnp.int32, (reach_in, pair * LANES), 0)
    j = lax.broadcasted_iota(jnp.int32, (reach_in, pair * LANES), 1) + LANES
    ribbon[...] = jnp.logical_and(i >= j - SIDE, i < j + SIDE).astype(F32).astype(BF16)

    def box_across(j):
        inner = pl.ds(pl.multiple_of(j * pair * LANES, pair * LANES), reach_in)
        outer = pl.ds(pl.multiple_of(j * pair * LANES, pair * LANES), pair * LANES)
        for plane in range(4):
            sums = jnp.dot(split[0, plane, :, inner], ribbon[...], preferred_element_type=F32)
            sums = sums + jnp.dot(split[1, plane, :, inner], ribbon[...], preferred_element_type=F32)
            boxed[plane, EDGE : EDGE + height, outer] = sums

    last = tiles // pair - 1
    middle = max(1, tiles // pair // 2)

    @pl.loop(1, middle)
    def _(j):
        box_across(j)

    send(2)

    @pl.loop(middle, max(middle, last))
    def _(j):
        box_across(j)

    @pl.when(has_left)
    def _():
        to_right.wait_recv()

    @pl.when(has_right)
    def _():
        to_left.wait_recv()

    sides = [pl.ds(0, LANES), pl.ds(LANES + width, LANES)]
    for b in range(height // 16):
        rows = pl.ds(b * 16, 16)
        lane = lax.broadcasted_iota(jnp.int32, (16, LANES), 1)
        pack = jnp.where(lane >= LANES // 2, left_in[rows, :], right_in[rows, :])
        put_split(split, decode(*edge_block(pack)), [(rows, lanes) for lanes in sides])

    send(3)
    forward(0)
    forward(1)
    for j in sorted({0, last}):
        box_across(j)

    sweep_load.wait()
    kind = lax.rem(lax.broadcasted_iota(jnp.int32, (LANES, height), 0), SWEEP_TALLY)
    memt[...] = (kind == sv[...]).astype(F32).T
    row_parts[...] = jnp.zeros_like(row_parts)

    group_lane = lax.broadcasted_iota(jnp.int32, (8, LANES), 1) // SWEEP_TALLY

    def row_v(group):
        row = lax.broadcasted_iota(jnp.int32, (8, LANES), 0) + (me_r * height + group * 8)
        return (row.astype(F32) + 0.5) * (2.0 / total_rows) - 1.0

    def arrange(group, values):
        table = values[0]
        for m, value in enumerate(values):
            table = value if m == 0 else jnp.where(group_lane >= m, value, table)
        return memt[group * 8 : group * 8 + 8, :] * jnp.where(group_lane < len(values), table, 0.0)

    @pl.loop(0, height // 8)
    def _(b):
        w = wv[pl.ds(pl.multiple_of(b * 8, 8), 8), :].astype(F32)
        u = across[...]
        wu = w * u
        for m, value in enumerate((w, wu, wu * u)):
            flag_parts[b, m] = fold(value)

    acc_g = None
    for b in range(height // 8):
        s0, su, suu = [row_sum(flag_parts[b, m]) for m in range(3)]
        v = row_v(b)
        part = arrange(b, (s0, su, v * s0, suu, v * su, v * v * s0))
        acc_g = part if acc_g is None else acc_g + part
    tab_out[:, 0:LANES] = jnp.sum(acc_g, 0, keepdims=True)

    send(4)
    edge_groups, groups = EDGE // 8, height // 8

    def shifted(x, following):
        n1, n2, n4 = following if following else (None, None, None)
        r1 = pltpu.roll(x, 7, 0)
        y1 = x + (r1 if n1 is None else jnp.where(sub < 7, r1, n1))
        r2 = pltpu.roll(y1, 6, 0)
        y2 = y1 + (r2 if n2 is None else jnp.where(sub < 6, r2, n2))
        r4 = pltpu.roll(y2, 4, 0)
        return y2 + (r4 if n4 is None else jnp.where(sub < 4, r4, n4)), (r1, r2, r4)

    def emit(g, lanes, window):
        rows = slice(g * 8, g * 8 + 8)
        inverse = lax.rsqrt((window[2] + 1.0) * (window[3] + 1.0))
        real, imag = window[0] * inverse, window[1] * inverse
        gam[0, rows, lanes] = real
        gam[1, rows, lanes] = imag
        coh[rows, lanes] = jnp.sqrt(real * real + imag * imag)
        w, u = wv[rows, lanes].astype(F32), across[:, lanes]
        wr, wi = w * real, w * imag
        for m, value in enumerate((wr, wi, wr * u, wi * u)):
            row_parts[g, m] += value

    def group_rows(g):
        return slice(g * 8, g * 8 + 8)

    def finish(t):
        lanes = pl.ds(pl.multiple_of(t * LANES, LANES), LANES)
        eights = [[None] * 4 for _ in range(groups + 2)]
        pairs = [[None] * 4 for _ in range(groups + 2)]
        following = [None] * 4
        for g in range(groups + 1, edge_groups - 1, -1):
            for plane in range(4):
                eights[g][plane], following[plane] = shifted(boxed[plane, group_rows(g), lanes], following[plane])
                if g <= groups - 1:
                    pairs[g][plane] = eights[g][plane] + eights[g + 1][plane]
            if g <= groups - 3:
                emit(g, lanes, [pairs[g][p] + pairs[g + 2][p] for p in range(4)])
        for p in range(4):
            kept = (
                pairs[edge_groups][p], eights[edge_groups][p] + pairs[edge_groups + 1][p], *following[p],
                eights[groups - 2][p] + pairs[groups - 1][p], pairs[groups - 1][p],
            )
            for k, value in enumerate(kept):
                own_part[p, k, :, lanes] = value

    def finish_edges(t):
        lanes = pl.ds(pl.multiple_of(t * LANES, LANES), LANES)
        outer, inner = [None] * 4, [None] * 4
        for p in range(4):
            near, following = shifted(boxed[p, group_rows(1), lanes], [own_part[p, k, :, lanes] for k in (2, 3, 4)])
            far, _ = shifted(boxed[p, group_rows(0), lanes], following)
            inner[p] = near + own_part[p, 1, :, lanes]
            outer[p] = far + near + own_part[p, 0, :, lanes]
        emit(0, lanes, outer)
        emit(1, lanes, inner)
        for p in range(4):
            _, following = shifted(boxed[p, group_rows(groups + 3), lanes], None)
            far, following = shifted(boxed[p, group_rows(groups + 2), lanes], following)
            near, _ = shifted(boxed[p, group_rows(groups + 1), lanes], following)
            inner[p] = near + own_part[p, 5, :, lanes]
            outer[p] = near + far + own_part[p, 6, :, lanes]
        emit(groups - 2, lanes, inner)
        emit(groups - 1, lanes, outer)

    def add_rows(groups):
        total = None
        for g in groups:
            hr, hi, hur, hui = [row_sum(row_parts[g, m]) for m in range(4)]
            v = row_v(g)
            part = arrange(g, (hr, hi, hur, hui, v * hr, v * hi))
            total = part if total is None else total + part
        return total

    @pl.loop(0, tiles // 2)
    def _(t):
        finish(t)

    forward(2)
    send(5)

    @pl.loop(tiles // 2, tiles)
    def _(t):
        finish(t)

    send(6)

    acc_h[...] = add_rows(range(edge_groups, groups - edge_groups))

    def put_halo(part, products, where):
        for plane, value in enumerate(products):
            first = (plane * 2 + part) * EDGE
            high = value.astype(BF16)
            low_part = (value - high.astype(F32)).astype(BF16)
            for lanes in where:
                halo_split[first : first + EDGE, lanes] = high
                halo_split[8 * EDGE + first : 9 * EDGE + first, lanes] = low_part

    def box_halo(j):
        inner = pl.ds(j * pair * LANES, reach_in)
        outer = pl.ds(j * pair * LANES, pair * LANES)
        sums = jnp.dot(halo_split[:, inner], ribbon[...], preferred_element_type=F32)
        for plane in range(4):
            for part, target in enumerate((0, EDGE + height)):
                first = (plane * 2 + part) * EDGE
                boxed[plane, target : target + EDGE, outer] = (
                    sums[first : first + EDGE] + sums[8 * EDGE + first : 9 * EDGE + first]
                )

    done = 0
    had_down, had_up = 0, 0
    for i, (need_down, need_up) in enumerate(steps):
        if i == 0:
            for copy, _, of in corners:
                @pl.when(of)
                def _():
                    copy.wait_recv()

            def unpack(k, part):
                line = jnp.broadcast_to(corner_in[k, :, part * LANES : (part + 1) * LANES], (8, LANES))
                block = line
                for m in range(1, 8):
                    turned = pltpu.roll(line, (1, -1)[k % 2] * 3 * SIDE * m % LANES, 1)
                    block = jnp.where(sub == m, turned, block)
                return block

            lane = lax.broadcasted_iota(jnp.int32, (8, LANES), 1)
            packs = [
                jnp.concatenate(
                    [jnp.where(lane >= LANES // 2, unpack(k, part), unpack(k + 1, part)) for part in range(EDGE // 8)], 0
                )
                for k in (0, 2)
            ]
            for part, pack in enumerate(packs):
                put_halo(part, decode(*edge_block(pack)), sides)

        @pl.when(has_up)
        def _():
            for copy in downs[had_down:need_down]:
                copy.wait_recv()

        @pl.when(has_down)
        def _():
            for copy in ups[had_up:need_up]:
                copy.wait_recv()

        end_up = up_cuts[need_up - 1][1]
        if tucked and i == len(steps) - 1:
            end_up = tiles
            for t in range(EDGE - 1):
                for k in range(3):
                    bot_in[k, t : t + 1, width - LANES : width] = bot_in[k, EDGE - 1 : EDGE, t * LANES : (t + 1) * LANES]
        ranges = ((down_cuts[had_down][0], down_cuts[need_down - 1][1]), (up_cuts[had_up][0], end_up))
        for part, (halo, (start, end)) in enumerate(zip((top_in, bot_in), ranges)):
            source = pl.ds(start * LANES, (end - start) * LANES)
            target = pl.ds((start + 1) * LANES, (end - start) * LANES)
            put_halo(part, decode(*[halo[m, :, source] for m in range(3)]), [target])
        had_down, had_up = need_down, need_up
        ready = tiles // pair if i == len(steps) - 1 else max(0, (min(ranges[0][1], ranges[1][1]) - 1) // pair)
        for j in range(done, ready):
            box_halo(j)
        if ready > done:
            @pl.loop(done, ready)
            def _(j):
                for t in range(pair):
                    finish_edges(j * pair + t)
        done = ready
        if i == 0:
            send(7)

    acc_last = acc_h[...] + add_rows(list(range(edge_groups)) + list(range(groups - edge_groups, groups)))
    tab_out[:, LANES:] = jnp.sum(acc_last, 0, keepdims=True)
    swaps = [
        (remote(tab_out, tab_in.at[slot], tab_send.at[slot], tab_recv.at[slot], row, col), to, of)
        for slot, to, of, row, col in peers
    ]
    for copy, to, _ in swaps:
        @pl.when(to)
        def _():
            copy.start()

    tab_in[reach * n_cols] = tab_out[...]
    @pl.when(has_down)
    def _():
        for copy in downs:
            copy.wait_send()

    @pl.when(has_up)
    def _():
        for copy in ups:
            copy.wait_send()

    for copy, to, _ in corners:
        @pl.when(to)
        def _():
            copy.wait_send()

    for group in via:
        for give, copy in group[2:]:
            @pl.when(give)
            def _():
                copy.wait_send()

    @pl.when(has_right)
    def _():
        to_right.wait_send()

    @pl.when(has_left)
    def _():
        to_left.wait_send()

    for copy, _, of in swaps:
        @pl.when(of)
        def _():
            copy.wait_recv()

    total = functools.reduce(jnp.add, [tab_in[slot] for slot in range(tab_in.shape[0])])

    def column(base, m):
        part = total[:, base : base + LANES]
        return part if m == 0 else pltpu.roll(part, LANES - m * SWEEP_TALLY, 1)

    s0, su, sv_, suu, suv, svv = [column(0, m) for m in range(6)]
    hr, hi, hur, hui, hvr, hvi = [column(LANES, m) for m in range(6)]
    floored = jnp.maximum(s0, 1.0)
    mid_u, mid_v = su / floored, sv_ / floored
    guu = suu - 2.0 * mid_u * su + mid_u * mid_u * s0
    guv = suv - mid_u * sv_ - mid_v * su + mid_u * mid_v * s0
    gvv = svv - 2.0 * mid_v * sv_ + mid_v * mid_v * s0
    hur, hui = hur - mid_u * hr, hui - mid_u * hi
    hvr, hvi = hvr - mid_v * hr, hvi - mid_v * hi
    ridge = 0.001 * s0 + 1.0
    duu, dvv = guu + ridge, gvv + ridge
    scale = 1.0 / (duu * dvv - guv * guv)
    base = 1.0 / (s0 + ridge)
    c1r, c1i = (dvv * hur - guv * hvr) * scale, (dvv * hui - guv * hvi) * scale
    c2r, c2i = (duu * hvr - guv * hur) * scale, (duu * hvi - guv * hui) * scale
    valid = lax.broadcasted_iota(jnp.int32, (1, LANES), 1) < SWEEP_TALLY
    rows_out = (hr * base - c1r * mid_u, hi * base - c1i * mid_u, c1r, c1i, c2r, c2i, mid_v)
    for m, value in enumerate(rows_out):
        fit[m : m + 1, :] = jnp.where(valid, value, 0.0)

    for copy, to, _ in swaps:
        @pl.when(to)
        def _():
            copy.wait_send()


def back_kernel(n_rows, n_cols, block, gam, coh, memt, fit, ramped, coherence, out, across, lines, sem):
    height, width = coh.shape
    me_r, me_c = lax.axis_index("rows"), lax.axis_index("cols")
    coh_copy = pltpu.make_async_copy(coh, coherence, sem.at[0])
    coh_copy.start()
    for g in range(height // 8):
        row = lax.broadcasted_iota(jnp.int32, (8, LANES), 0) + (me_r * height + g * 8)
        dv = (row.astype(F32) + 0.5) * (2.0 / (height * n_rows)) - 1.0 - fit[6:7, :]
        one = memt[g * 8 : g * 8 + 8, :]
        for m, value in enumerate((fit[0:1, :] + fit[4:5, :] * dv, fit[1:2, :] + fit[5:6, :] * dv, fit[2:3, :], fit[3:4, :])):
            lines[g, m] = jnp.broadcast_to(row_sum(one * value), (8, LANES))
    lane_all = lax.broadcasted_iota(jnp.int32, (8, width), 1) + me_c * width
    across[...] = (lane_all.astype(F32) + 0.5) * (2.0 / (width * n_cols)) - 1.0

    copies = []
    for i in range(height // block):
        @pl.loop(0, block // 8)
        def _(b):
            g = i * (block // 8) + b
            rows = pl.ds(pl.multiple_of(g * 8, 8), 8)
            base_r, base_i, slope_r, slope_i = [lines[g, m] for m in range(4)]
            for t in range(width // LANES):
                lanes = slice(t * LANES, (t + 1) * LANES)
                real, imag, u = gam[0, rows, lanes], gam[1, rows, lanes], across[:, lanes]
                model_real = base_r + slope_r * u
                model_imag = base_i + slope_i * u
                out[0, rows, lanes] = real * model_real + imag * model_imag
                out[1, rows, lanes] = imag * model_real - real * model_imag

        rows = pl.ds(i * block, block)
        copy = pltpu.make_async_copy(out.at[:, rows, :], ramped.at[:, rows, :], sem.at[1 + i])
        copy.start()
        copies.append(copy)
    coh_copy.wait()
    for copy in copies:
        copy.wait()


def on_device(n_rows, n_cols, lead, trail, flags, sweep):
    height, width = flags.shape
    wide = width + 2 * LANES
    longest = 2 * height * n_rows // SWEEP_TALLY
    reach = max(1, min(n_rows - 1, (longest - 2) // height + 1))
    slots = (2 * reach + 1) * n_cols
    pieces = len(cuts(width // LANES)[0])
    pair = 2 if width // LANES % 2 == 0 else 1
    hbm = pl.BlockSpec(memory_space=pltpu.HBM)
    vmem = pl.BlockSpec(memory_space=pltpu.VMEM)
    dma = pltpu.SemaphoreType.DMA
    gam, coh, memt, fit = pl.pallas_call(
        functools.partial(front_kernel, n_rows, n_cols, reach),
        out_shape=[
            pltpu.VMEM((2, height, width), F32),
            pltpu.VMEM((height, width), F32),
            pltpu.VMEM((height, LANES), F32),
            pltpu.VMEM((8, LANES), F32),
        ],
        in_specs=[hbm, hbm, hbm, hbm],
        out_specs=[vmem, vmem, vmem, vmem],
        scratch_shapes=[
            pltpu.VMEM((2, height, width), F32),
            pltpu.VMEM((2, height, width), F32),
            pltpu.VMEM((height, width), jnp.int32),
            pltpu.VMEM((1, height), jnp.int32),
            pltpu.VMEM((3, EDGE, width), F32),
            pltpu.VMEM((3, EDGE, width), F32),
            pltpu.VMEM((3, EDGE, width), F32),
            pltpu.VMEM((3, EDGE, width), F32),
            pltpu.VMEM((height, LANES), F32),
            pltpu.VMEM((height, LANES), F32),
            pltpu.VMEM((height, LANES), F32),
            pltpu.VMEM((height, LANES), F32),
            pltpu.VMEM((3, EDGE, width), F32),
            pltpu.VMEM((4, 1, EDGE // 8 * LANES), F32),
            pltpu.VMEM((4, 1, EDGE // 8 * LANES), F32),
            pltpu.VMEM((2, 4, height, wide), BF16),
            pltpu.VMEM((16 * EDGE, wide), BF16),
            pltpu.VMEM((4, height + 2 * EDGE, width), F32),
            pltpu.VMEM(((pair + 2) * LANES, pair * LANES), BF16),
            pltpu.VMEM((8, width), F32),
            pltpu.VMEM((4, 7, 8, width), F32),
            pltpu.VMEM((height // 8, 4, 8, LANES), F32),
            pltpu.VMEM((height // 8, 3, 8, LANES), F32),
            pltpu.VMEM((8, LANES), F32),
            pltpu.VMEM((1, 2 * LANES), F32),
            pltpu.VMEM((slots, 1, 2 * LANES), F32),
            dma((7, 3)),
            dma((2, pieces)), dma((2, pieces)),
            dma((2,)), dma((2,)),
            dma((4,)), dma((4,)),
            dma((pieces,)), dma((pieces,)),
            dma((slots,)), dma((slots,)),
            pltpu.SemaphoreType.REGULAR,
        ],
        compiler_params=pltpu.CompilerParams(
            collective_id=0, has_side_effects=True, vmem_limit_bytes=60 * 1024 * 1024
        ),
        name="front",
    )(lead, trail, flags, sweep.reshape(1, height))
    block = 32 if height % 32 == 0 else 8
    return pl.pallas_call(
        functools.partial(back_kernel, n_rows, n_cols, block),
        out_shape=[
            jax.ShapeDtypeStruct((2, height, width), F32),
            jax.ShapeDtypeStruct((height, width), F32),
        ],
        in_specs=[vmem, vmem, vmem, vmem],
        out_specs=[hbm, hbm],
        scratch_shapes=[
            pltpu.VMEM((2, height, width), F32),
            pltpu.VMEM((8, width), F32),
            pltpu.VMEM((height // 8, 4, 8, LANES), F32),
            dma((1 + height // block,)),
        ],
        compiler_params=pltpu.CompilerParams(vmem_limit_bytes=16 * 1024 * 1024),
        name="back",
    )(gam, coh, memt, fit)


def solution(mesh):
    return jax.shard_map(
        functools.partial(on_device, mesh.shape["rows"], mesh.shape["cols"]),
        mesh=mesh,
        in_specs=(P(None, "rows", "cols"), P(None, "rows", "cols"), P("rows", "cols"), P("rows")),
        out_specs=(P(None, "rows", "cols"), P("rows", "cols")),
        check_vma=False,
    )
```

```python
import functools

import jax
import jax.numpy as jnp
from jax import lax
from jax.experimental import pallas as pl
from jax.experimental.pallas import tpu as pltpu
from jax.sharding import PartitionSpec as P

WIN_R = 32
WIN_C = 8
SWEEP_TALLY = 16

EDGE = WIN_R // 2
SIDE = WIN_C // 2
LANES = 128
SCALE = 2.0**56
FLOOR = 1e-36
F32 = jnp.float32
BF16 = jnp.bfloat16
MESH = pl.DeviceIdType.MESH


def masked(av, bv, wv, rows, lanes):
    w = wv[rows, lanes].astype(F32)
    return av[0, rows, lanes] * w, av[1, rows, lanes] * w, bv[0, rows, lanes] * w, bv[1, rows, lanes] * w


def encode(ar, ai, br, bi):
    sr, si = ar * SCALE, ai * SCALE
    power = sr * sr + si * si
    some = power > FLOOR
    inverse = lax.rsqrt(jnp.where(some, power, 1.0))
    return (
        jnp.where(some, power * inverse * (1.0 / SCALE), 0.0),
        jnp.where(some, (sr * br + si * bi) * inverse, br),
        jnp.where(some, (si * br - sr * bi) * inverse, bi),
    )


def decode(s, gr, gi):
    return s * gr, s * gi, s * s, gr * gr + gi * gi


def put_split(out, products, places):
    for plane, value in enumerate(products):
        high = value.astype(BF16)
        low = (value - high.astype(F32)).astype(BF16)
        for rows, lanes in places:
            out[0, plane, rows, lanes] = high
            out[1, plane, rows, lanes] = low


def edge_block(pack):
    lane = lax.broadcasted_iota(jnp.int32, pack.shape, 1)
    left, right = lane >= LANES - SIDE, lane < SIDE

    def pick(k):
        a = pack if k == 0 else pltpu.roll(pack, k * SIDE, 1)
        b = pack if k == 0 else pltpu.roll(pack, LANES - k * SIDE, 1)
        return jnp.where(left, a, jnp.where(right, b, 0.0))

    return pick(0), pick(1), pick(2)


def cuts(tiles):
    if tiles < EDGE:
        return ((0, tiles),), ((0, tiles),), ((1, 1),)
    down = [mark * tiles // 16 for mark in (0, 4, 8, 12, 14, 16)]
    up = [mark * tiles // 16 for mark in (0, 5, 9, 13)] + [tiles - 1]
    return tuple(zip(down[:-1], down[1:])), tuple(zip(up[:-1], up[1:])), ((2, 1), (3, 2), (4, 3), (5, 4))


def fold(x):
    total = x[:, 0:LANES]
    for t in range(1, x.shape[1] // LANES):
        total = total + x[:, t * LANES : (t + 1) * LANES]
    return total


def row_sum(x):
    return jnp.sum(x, 1, keepdims=True)


def front_kernel(
    n_rows, n_cols, reach,
    lead, trail, flags, sweep,
    gam, coh, memt, fit,
    av, bv, wv, sv, up_out, down_out, top_in, bot_in, left_out, right_out, left_in, right_in,
    relay_in, corner_out, corner_in, split, halo_split, boxed, ribbon, across, own_part, row_parts, flag_parts, acc_h,
    tab_out, tab_in,
    load_sem, halo_send, halo_recv, side_send, side_recv, corner_send, corner_recv,
    relay_send, relay_recv, tab_send, tab_recv, token,
):
    me_r, me_c = lax.axis_index("rows"), lax.axis_index("cols")
    height, width = flags.shape
    tiles = width // LANES
    low = height - EDGE
    total_rows, total_cols = height * n_rows, width * n_cols
    chunk = 512 if width % 512 == 0 else LANES
    has_up, has_down = me_r > 0, me_r < n_rows - 1
    has_left, has_right = me_c > 0, me_c < n_cols - 1
    down_cuts, up_cuts, steps = cuts(tiles)
    pair = 2 if tiles % 2 == 0 else 1

    def load(part, rows, lanes=pl.ds(0, width)):
        group = [
            pltpu.make_async_copy(lead.at[:, rows, lanes], av.at[:, rows, lanes], load_sem.at[part, 0]),
            pltpu.make_async_copy(trail.at[:, rows, lanes], bv.at[:, rows, lanes], load_sem.at[part, 1]),
            pltpu.make_async_copy(flags.at[rows, lanes], wv.at[rows, lanes], load_sem.at[part, 2]),
        ]
        for copy in group:
            copy.start()
        return group

    top_rows, low_rows = pl.ds(0, EDGE), pl.ds(low, EDGE)
    tucked = up_cuts[-1][1] == tiles - 1
    first = max(up_cuts[:2][-1][1], down_cuts[:3][-1][1]) * LANES
    loads = [load(0, top_rows, pl.ds(0, first))]
    if first < width:
        if tucked:
            loads.append(load(1, top_rows, pl.ds(width - LANES, LANES)))
        loads.append(load(2, low_rows, pl.ds(0, first)))
    later_loads = []
    if first < width:
        rest = width - first - (LANES if tucked else 0)
        if rest:
            later_loads.append(load(3, top_rows, pl.ds(first, rest)))
        later_loads.append(load(4, low_rows, pl.ds(first, width - first)))
    else:
        later_loads.append(load(4, low_rows))
    sweep_load = pltpu.make_async_copy(sweep, sv, load_sem.at[6, 0])
    sweep_load.start()

    barrier = pltpu.get_barrier_semaphore()
    peers = []
    for dr in range(-reach, reach + 1):
        for dc in range(n_cols):
            if dr == 0 and dc == 0:
                continue
            to = jnp.logical_and(me_r + dr >= 0, me_r + dr < n_rows)
            of = jnp.logical_and(me_r - dr >= 0, me_r - dr < n_rows)
            peers.append(((dr + reach) * n_cols + dc, to, of, me_r + dr, lax.rem(me_c + dc, n_cols)))
    near = reach == 1
    n_greeted = 0
    for slot, to, _, row, col in peers:
        dr, dc = slot // n_cols - reach, slot % n_cols
        if near and dr != 0 and dc != 0:
            continue
        n_greeted = n_greeted + to.astype(jnp.int32)

        @pl.when(to)
        def _():
            pl.semaphore_signal(barrier, inc=1, device_id=(row, col), device_id_type=MESH)

    def remote(src, dst, send, recv, row, col):
        return pltpu.make_async_remote_copy(
            src_ref=src, dst_ref=dst, send_sem=send, recv_sem=recv, device_id=(row, col), device_id_type=MESH
        )

    def cut(ref, piece):
        return ref.at[:, :, pl.ds(piece[0] * LANES, (piece[1] - piece[0]) * LANES)]

    downs = [
        remote(cut(down_out, p), cut(top_in, p), halo_send.at[0, i], halo_recv.at[0, i], me_r + 1, me_c)
        for i, p in enumerate(down_cuts)
    ]
    ups = [
        remote(cut(up_out, p), cut(bot_in, p), halo_send.at[1, i], halo_recv.at[1, i], me_r - 1, me_c)
        for i, p in enumerate(up_cuts)
    ]
    to_right = remote(right_out, left_in, side_send.at[0], side_recv.at[0], me_r, me_c + 1)
    to_left = remote(left_out, right_in, side_send.at[1], side_recv.at[1], me_r, me_c - 1)
    corners = []
    for k, (dr, dc, to, of) in enumerate((
        (1, 1, has_down & has_right, has_up & has_left),
        (1, -1, has_down & has_left, has_up & has_right),
        (-1, 1, has_up & has_right, has_down & has_left),
        (-1, -1, has_up & has_left, has_down & has_right),
    )):
        copy = remote(corner_out.at[k], corner_in.at[k], corner_send.at[k], corner_recv.at[k], me_r + dr, me_c + dc)
        corners.append((copy, to, of))

    relayed = 3 if n_rows % 2 == 0 and n_rows > 2 and len(up_cuts) > 3 else 0
    odd = lax.rem(me_r, 2) == 1
    even = jnp.logical_not(odd)
    place = lax.div(me_r, 2) * 4
    n_up = jnp.minimum(relayed, lax.div(place, n_rows // 2)) if relayed else 0
    n_down = jnp.minimum(relayed, 4 - lax.div(place + 4, n_rows // 2)) if relayed else 0
    via = []
    for i in range(relayed):
        p, q = up_cuts[i], down_cuts[i]
        ask_up, ask_down = even & (n_up > i), odd & (n_down > i)
        give_up, give_down = odd & (n_up > i), even & (n_down > i)
        via.append((
            (ask_up, remote(cut(up_out, p), cut(relay_in, p), halo_send.at[1, i], relay_recv.at[i], me_r + 1, me_c)),
            (ask_down, remote(cut(down_out, q), cut(relay_in, q), halo_send.at[0, i], relay_recv.at[i], me_r - 1, me_c)),
            (give_up, remote(cut(relay_in, p), cut(bot_in, p), relay_send.at[i], halo_recv.at[1, i], me_r - 2, me_c)),
            (give_down, remote(cut(relay_in, q), cut(top_in, q), relay_send.at[i], halo_recv.at[0, i], me_r + 2, me_c)),
        ))

    def forward(i):
        if i >= relayed:
            return
        for (_, arrival), (give, copy) in zip(via[i][:2], via[i][2:]):
            @pl.when(give)
            def _():
                arrival.wait_recv()
                copy.start()

    def encode_rows(first, out, piece):
        lanes = pl.ds(piece[0] * LANES, (piece[1] - piece[0]) * LANES)
        for k, value in enumerate(encode(*masked(av, bv, wv, pl.ds(first, EDGE), lanes))):
            out[k, :, lanes] = value

    def pack_sides(b):
        rows = pl.ds(b * 16, 16)
        lane = lax.broadcasted_iota(jnp.int32, (16, LANES), 1)
        s, gr, gi = encode(*masked(av, bv, wv, rows, pl.ds(width - LANES, LANES)))
        right_out[rows, :] = jnp.where(
            lane >= LANES - SIDE,
            s,
            jnp.where(
                lane >= LANES - 2 * SIDE,
                pltpu.roll(gr, LANES - SIDE, 1),
                jnp.where(lane >= LANES - 3 * SIDE, pltpu.roll(gi, LANES - 2 * SIDE, 1), 0.0),
            ),
        )
        s, gr, gi = encode(*masked(av, bv, wv, rows, pl.ds(0, LANES)))
        left_out[rows, :] = jnp.where(
            lane < SIDE,
            s,
            jnp.where(
                lane < 2 * SIDE,
                pltpu.roll(gr, SIDE, 1),
                jnp.where(lane < 3 * SIDE, pltpu.roll(gi, 2 * SIDE, 1), 0.0),
            ),
        )

    for group in loads:
        for copy in group:
            copy.wait()

    def tuck(piece):
        if tucked:
            for t in range(piece[0], min(piece[1], EDGE - 1)):
                for k in range(3):
                    up_out[k, EDGE - 1 : EDGE, t * LANES : (t + 1) * LANES] = up_out[k, t : t + 1, width - LANES : width]

    if first == width:
        for copy in later_loads[0]:
            copy.wait()
    if tucked:
        encode_rows(0, up_out, (tiles - 1, tiles))
    for piece in up_cuts[:2]:
        encode_rows(0, up_out, piece)
        tuck(piece)
    for piece in down_cuts[:3]:
        encode_rows(low, down_out, piece)

    pl.semaphore_wait(barrier, n_greeted)
    n_via = jnp.where(even, n_up, n_down)

    def send(point):
        for v in range(relayed + 1):
            later = [i for i in range(v, len(down_cuts)) if point == (i + (2 if i < 3 else 3) if v else i)]
            for parity, straight, other, asked in ((even, downs, ups, 0), (odd, ups, downs, 1)):
                ahead = 2 if v == asked == 0 else 1
                slots = range(ahead + 1) if point == 0 else (point + ahead,)

                @pl.when(parity & (n_via == v))
                def _():
                    far, near_by = (has_up, has_down) if asked == 0 else (has_down, has_up)
                    for k in slots:
                        if k < v:
                            via[k][asked][1].start()
                        elif k - v < len(straight):
                            @pl.when(near_by)
                            def _():
                                straight[k - v].start()
                    for i in (i for i in later if i < len(other)):
                        @pl.when(far)
                        def _():
                            other[i].start()

    send(0)
    if near:
        for dc in range(1, n_cols):
            pl.semaphore_signal(token, inc=1, device_id=(me_r, lax.rem(me_c + dc, n_cols)), device_id_type=MESH)

    if first < width:
        for group in later_loads:
            for copy in group:
                copy.wait()
        for piece in up_cuts[2:]:
            encode_rows(0, up_out, piece)
            tuck(piece)
        for piece in down_cuts[3:]:
            encode_rows(low, down_out, piece)
    bulk = load(5, pl.ds(EDGE, low - EDGE))
    for b in (0, height // 16 - 1):
        pack_sides(b)
    sub = lax.broadcasted_iota(jnp.int32, (8, LANES), 0)
    for k, (src, start, sign) in enumerate(
        ((right_out, low, -1), (left_out, low, 1), (right_out, 0, -1), (left_out, 0, 1))
    ):
        for part in range(EDGE // 8):
            block = src[start + part * 8 : start + part * 8 + 8, :]
            line = jnp.where(sub == 0, block, 0.0)
            for m in range(1, 8):
                line = line + pltpu.roll(jnp.where(sub == m, block, 0.0), sign * 3 * SIDE * m % LANES, 1)
            corner_out[k, :, part * LANES : (part + 1) * LANES] = jnp.sum(line, 0, keepdims=True)
    for copy in bulk:
        copy.wait()

    for b in range(1, height // 16 - 1):
        pack_sides(b)

    @pl.when(has_right)
    def _():
        to_right.start()

    @pl.when(has_left)
    def _():
        to_left.start()

    @pl.when(jnp.logical_not(has_left))
    def _():
        left_in[...] = jnp.zeros_like(left_in)

    @pl.when(jnp.logical_not(has_right))
    def _():
        right_in[...] = jnp.zeros_like(right_in)

    @pl.when(jnp.logical_not(has_up))
    def _():
        top_in[...] = jnp.zeros_like(top_in)

    @pl.when(jnp.logical_not(has_down))
    def _():
        bot_in[...] = jnp.zeros_like(bot_in)

    for k, (_, _, of) in enumerate(corners):
        @pl.when(jnp.logical_not(of))
        def _():
            corner_in[k] = jnp.zeros((1, EDGE // 8 * LANES), F32)

    for slot, _, of, _, _ in peers:
        @pl.when(jnp.logical_not(of))
        def _():
            tab_in[slot] = jnp.zeros((1, 2 * LANES), F32)

    if near:
        pl.semaphore_wait(token, n_cols - 1)
    for copy, to, _ in corners:
        @pl.when(to)
        def _():
            copy.start()

    lane_all = lax.broadcasted_iota(jnp.int32, (8, width), 1) + me_c * width
    across[...] = (lane_all.astype(F32) + 0.5) * (2.0 / total_cols) - 1.0

    @pl.loop(0, height // 16)
    def _(b):
        rows = pl.ds(pl.multiple_of(b * 16, 16), 16)

        @pl.loop(0, width // chunk)
        def _(c):
            lanes = pl.ds(pl.multiple_of(c * chunk, chunk), chunk)
            ar, ai, br, bi = masked(av, bv, wv, rows, lanes)
            put_split(
                split,
                (ar * br + ai * bi, ai * br - ar * bi, ar * ar + ai * ai, br * br + bi * bi),
                [(rows, pl.ds(pl.multiple_of(LANES + c * chunk, LANES), chunk))],
            )

    send(1)
    reach_in = (pair + 2) * LANES
    i = lax.broadcasted_iota(jnp.int32, (reach_in, pair * LANES), 0)
    j = lax.broadcasted_iota(jnp.int32, (reach_in, pair * LANES), 1) + LANES
    ribbon[...] = jnp.logical_and(i >= j - SIDE, i < j + SIDE).astype(F32).astype(BF16)

    def box_across(j):
        inner = pl.ds(pl.multiple_of(j * pair * LANES, pair * LANES), reach_in)
        outer = pl.ds(pl.multiple_of(j * pair * LANES, pair * LANES), pair * LANES)
        for plane in range(4):
            sums = jnp.dot(split[0, plane, :, inner], ribbon[...], preferred_element_type=F32)
            sums = sums + jnp.dot(split[1, plane, :, inner], ribbon[...], preferred_element_type=F32)
            boxed[plane, EDGE : EDGE + height, outer] = sums

    last = tiles // pair - 1
    middle = max(1, tiles // pair // 2)

    @pl.loop(1, middle)
    def _(j):
        box_across(j)

    send(2)

    @pl.loop(middle, max(middle, last))
    def _(j):
        box_across(j)

    @pl.when(has_left)
    def _():
        to_right.wait_recv()

    @pl.when(has_right)
    def _():
        to_left.wait_recv()

    sides = [pl.ds(0, LANES), pl.ds(LANES + width, LANES)]
    for b in range(height // 16):
        rows = pl.ds(b * 16, 16)
        lane = lax.broadcasted_iota(jnp.int32, (16, LANES), 1)
        pack = jnp.where(lane >= LANES // 2, left_in[rows, :], right_in[rows, :])
        put_split(split, decode(*edge_block(pack)), [(rows, lanes) for lanes in sides])

    send(3)
    forward(0)
    forward(1)
    for j in sorted({0, last}):
        box_across(j)

    sweep_load.wait()
    kind = lax.rem(lax.broadcasted_iota(jnp.int32, (LANES, height), 0), SWEEP_TALLY)
    memt[...] = (kind == sv[...]).astype(F32).T
    row_parts[...] = jnp.zeros_like(row_parts)

    group_lane = lax.broadcasted_iota(jnp.int32, (8, LANES), 1) // SWEEP_TALLY

    def row_v(group):
        row = lax.broadcasted_iota(jnp.int32, (8, LANES), 0) + (me_r * height + group * 8)
        return (row.astype(F32) + 0.5) * (2.0 / total_rows) - 1.0

    def arrange(group, values):
        table = values[0]
        for m, value in enumerate(values):
            table = value if m == 0 else jnp.where(group_lane >= m, value, table)
        return memt[group * 8 : group * 8 + 8, :] * jnp.where(group_lane < len(values), table, 0.0)

    @pl.loop(0, height // 8)
    def _(b):
        w = wv[pl.ds(pl.multiple_of(b * 8, 8), 8), :].astype(F32)
        u = across[...]
        wu = w * u
        for m, value in enumerate((w, wu, wu * u)):
            flag_parts[b, m] = fold(value)

    acc_g = None
    for b in range(height // 8):
        s0, su, suu = [row_sum(flag_parts[b, m]) for m in range(3)]
        v = row_v(b)
        part = arrange(b, (s0, su, v * s0, suu, v * su, v * v * s0))
        acc_g = part if acc_g is None else acc_g + part
    tab_out[:, 0:LANES] = jnp.sum(acc_g, 0, keepdims=True)

    send(4)
    edge_groups, groups = EDGE // 8, height // 8

    def shifted(x, following):
        n1, n2, n4 = following if following else (None, None, None)
        r1 = pltpu.roll(x, 7, 0)
        y1 = x + (r1 if n1 is None else jnp.where(sub < 7, r1, n1))
        r2 = pltpu.roll(y1, 6, 0)
        y2 = y1 + (r2 if n2 is None else jnp.where(sub < 6, r2, n2))
        r4 = pltpu.roll(y2, 4, 0)
        return y2 + (r4 if n4 is None else jnp.where(sub < 4, r4, n4)), (r1, r2, r4)

    def emit(g, lanes, window):
        rows = slice(g * 8, g * 8 + 8)
        inverse = lax.rsqrt((window[2] + 1.0) * (window[3] + 1.0))
        real, imag = window[0] * inverse, window[1] * inverse
        gam[0, rows, lanes] = real
        gam[1, rows, lanes] = imag
        coh[rows, lanes] = jnp.sqrt(real * real + imag * imag)
        w, u = wv[rows, lanes].astype(F32), across[:, lanes]
        wr, wi = w * real, w * imag
        for m, value in enumerate((wr, wi, wr * u, wi * u)):
            row_parts[g, m] += value

    def group_rows(g):
        return slice(g * 8, g * 8 + 8)

    def finish(t):
        lanes = pl.ds(pl.multiple_of(t * LANES, LANES), LANES)
        eights = [[None] * 4 for _ in range(groups + 2)]
        pairs = [[None] * 4 for _ in range(groups + 2)]
        following = [None] * 4
        for g in range(groups + 1, edge_groups - 1, -1):
            for plane in range(4):
                eights[g][plane], following[plane] = shifted(boxed[plane, group_rows(g), lanes], following[plane])
                if g <= groups - 1:
                    pairs[g][plane] = eights[g][plane] + eights[g + 1][plane]
            if g <= groups - 3:
                emit(g, lanes, [pairs[g][p] + pairs[g + 2][p] for p in range(4)])
        for p in range(4):
            kept = (
                pairs[edge_groups][p], eights[edge_groups][p] + pairs[edge_groups + 1][p], *following[p],
                eights[groups - 2][p] + pairs[groups - 1][p], pairs[groups - 1][p],
            )
            for k, value in enumerate(kept):
                own_part[p, k, :, lanes] = value

    def finish_edges(t):
        lanes = pl.ds(pl.multiple_of(t * LANES, LANES), LANES)
        outer, inner = [None] * 4, [None] * 4
        for p in range(4):
            near, following = shifted(boxed[p, group_rows(1), lanes], [own_part[p, k, :, lanes] for k in (2, 3, 4)])
            far, _ = shifted(boxed[p, group_rows(0), lanes], following)
            inner[p] = near + own_part[p, 1, :, lanes]
            outer[p] = far + near + own_part[p, 0, :, lanes]
        emit(0, lanes, outer)
        emit(1, lanes, inner)
        for p in range(4):
            _, following = shifted(boxed[p, group_rows(groups + 3), lanes], None)
            far, following = shifted(boxed[p, group_rows(groups + 2), lanes], following)
            near, _ = shifted(boxed[p, group_rows(groups + 1), lanes], following)
            inner[p] = near + own_part[p, 5, :, lanes]
            outer[p] = near + far + own_part[p, 6, :, lanes]
        emit(groups - 2, lanes, inner)
        emit(groups - 1, lanes, outer)

    def add_rows(groups):
        total = None
        for g in groups:
            hr, hi, hur, hui = [row_sum(row_parts[g, m]) for m in range(4)]
            v = row_v(g)
            part = arrange(g, (hr, hi, hur, hui, v * hr, v * hi))
            total = part if total is None else total + part
        return total

    @pl.loop(0, tiles // 2)
    def _(t):
        finish(t)

    forward(2)
    send(5)

    @pl.loop(tiles // 2, tiles)
    def _(t):
        finish(t)

    send(6)

    acc_h[...] = add_rows(range(edge_groups, groups - edge_groups))

    def put_halo(part, products, where):
        for plane, value in enumerate(products):
            first = (plane * 2 + part) * EDGE
            high = value.astype(BF16)
            low_part = (value - high.astype(F32)).astype(BF16)
            for lanes in where:
                halo_split[first : first + EDGE, lanes] = high
                halo_split[8 * EDGE + first : 9 * EDGE + first, lanes] = low_part

    def box_halo(j):
        inner = pl.ds(j * pair * LANES, reach_in)
        outer = pl.ds(j * pair * LANES, pair * LANES)
        sums = jnp.dot(halo_split[:, inner], ribbon[...], preferred_element_type=F32)
        for plane in range(4):
            for part, target in enumerate((0, EDGE + height)):
                first = (plane * 2 + part) * EDGE
                boxed[plane, target : target + EDGE, outer] = (
                    sums[first : first + EDGE] + sums[8 * EDGE + first : 9 * EDGE + first]
                )

    done = 0
    had_down, had_up = 0, 0
    for i, (need_down, need_up) in enumerate(steps):
        if i == 0:
            for copy, _, of in corners:
                @pl.when(of)
                def _():
                    copy.wait_recv()

            def unpack(k, part):
                line = jnp.broadcast_to(corner_in[k, :, part * LANES : (part + 1) * LANES], (8, LANES))
                block = line
                for m in range(1, 8):
                    turned = pltpu.roll(line, (1, -1)[k % 2] * 3 * SIDE * m % LANES, 1)
                    block = jnp.where(sub == m, turned, block)
                return block

            lane = lax.broadcasted_iota(jnp.int32, (8, LANES), 1)
            packs = [
                jnp.concatenate(
                    [jnp.where(lane >= LANES // 2, unpack(k, part), unpack(k + 1, part)) for part in range(EDGE // 8)], 0
                )
                for k in (0, 2)
            ]
            for part, pack in enumerate(packs):
                put_halo(part, decode(*edge_block(pack)), sides)

        @pl.when(has_up)
        def _():
            for copy in downs[had_down:need_down]:
                copy.wait_recv()

        @pl.when(has_down)
        def _():
            for copy in ups[had_up:need_up]:
                copy.wait_recv()

        end_up = up_cuts[need_up - 1][1]
        if tucked and i == len(steps) - 1:
            end_up = tiles
            for t in range(EDGE - 1):
                for k in range(3):
                    bot_in[k, t : t + 1, width - LANES : width] = bot_in[k, EDGE - 1 : EDGE, t * LANES : (t + 1) * LANES]
        ranges = ((down_cuts[had_down][0], down_cuts[need_down - 1][1]), (up_cuts[had_up][0], end_up))
        for part, (halo, (start, end)) in enumerate(zip((top_in, bot_in), ranges)):
            source = pl.ds(start * LANES, (end - start) * LANES)
            target = pl.ds((start + 1) * LANES, (end - start) * LANES)
            put_halo(part, decode(*[halo[m, :, source] for m in range(3)]), [target])
        had_down, had_up = need_down, need_up
        ready = tiles // pair if i == len(steps) - 1 else max(0, (min(ranges[0][1], ranges[1][1]) - 1) // pair)
        for j in range(done, ready):
            box_halo(j)
        if ready > done:
            @pl.loop(done, ready)
            def _(j):
                for t in range(pair):
                    finish_edges(j * pair + t)
        done = ready
        if i == 0:
            send(7)

    acc_last = acc_h[...] + add_rows(list(range(edge_groups)) + list(range(groups - edge_groups, groups)))
    tab_out[:, LANES:] = jnp.sum(acc_last, 0, keepdims=True)
    swaps = [
        (remote(tab_out, tab_in.at[slot], tab_send.at[slot], tab_recv.at[slot], row, col), to, of)
        for slot, to, of, row, col in peers
    ]
    for copy, to, _ in swaps:
        @pl.when(to)
        def _():
            copy.start()

    tab_in[reach * n_cols] = tab_out[...]
    @pl.when(has_down)
    def _():
        for copy in downs:
            copy.wait_send()

    @pl.when(has_up)
    def _():
        for copy in ups:
            copy.wait_send()

    for copy, to, _ in corners:
        @pl.when(to)
        def _():
            copy.wait_send()

    for group in via:
        for give, copy in group[2:]:
            @pl.when(give)
            def _():
                copy.wait_send()

    @pl.when(has_right)
    def _():
        to_right.wait_send()

    @pl.when(has_left)
    def _():
        to_left.wait_send()

    for copy, _, of in swaps:
        @pl.when(of)
        def _():
            copy.wait_recv()

    total = functools.reduce(jnp.add, [tab_in[slot] for slot in range(tab_in.shape[0])])

    def column(base, m):
        part = total[:, base : base + LANES]
        return part if m == 0 else pltpu.roll(part, LANES - m * SWEEP_TALLY, 1)

    s0, su, sv_, suu, suv, svv = [column(0, m) for m in range(6)]
    hr, hi, hur, hui, hvr, hvi = [column(LANES, m) for m in range(6)]
    floored = jnp.maximum(s0, 1.0)
    mid_u, mid_v = su / floored, sv_ / floored
    guu = suu - 2.0 * mid_u * su + mid_u * mid_u * s0
    guv = suv - mid_u * sv_ - mid_v * su + mid_u * mid_v * s0
    gvv = svv - 2.0 * mid_v * sv_ + mid_v * mid_v * s0
    hur, hui = hur - mid_u * hr, hui - mid_u * hi
    hvr, hvi = hvr - mid_v * hr, hvi - mid_v * hi
    ridge = 0.001 * s0 + 1.0
    duu, dvv = guu + ridge, gvv + ridge
    scale = 1.0 / (duu * dvv - guv * guv)
    base = 1.0 / (s0 + ridge)
    c1r, c1i = (dvv * hur - guv * hvr) * scale, (dvv * hui - guv * hvi) * scale
    c2r, c2i = (duu * hvr - guv * hur) * scale, (duu * hvi - guv * hui) * scale
    valid = lax.broadcasted_iota(jnp.int32, (1, LANES), 1) < SWEEP_TALLY
    rows_out = (hr * base - c1r * mid_u, hi * base - c1i * mid_u, c1r, c1i, c2r, c2i, mid_v)
    for m, value in enumerate(rows_out):
        fit[m : m + 1, :] = jnp.where(valid, value, 0.0)

    for copy, to, _ in swaps:
        @pl.when(to)
        def _():
            copy.wait_send()


def back_kernel(n_rows, n_cols, block, gam, coh, memt, fit, ramped, coherence, out, across, lines, sem):
    height, width = coh.shape
    me_r, me_c = lax.axis_index("rows"), lax.axis_index("cols")
    coh_copy = pltpu.make_async_copy(coh, coherence, sem.at[0])
    coh_copy.start()
    for g in range(height // 8):
        row = lax.broadcasted_iota(jnp.int32, (8, LANES), 0) + (me_r * height + g * 8)
        dv = (row.astype(F32) + 0.5) * (2.0 / (height * n_rows)) - 1.0 - fit[6:7, :]
        one = memt[g * 8 : g * 8 + 8, :]
        for m, value in enumerate((fit[0:1, :] + fit[4:5, :] * dv, fit[1:2, :] + fit[5:6, :] * dv, fit[2:3, :], fit[3:4, :])):
            lines[g, m] = jnp.broadcast_to(row_sum(one * value), (8, LANES))
    lane_all = lax.broadcasted_iota(jnp.int32, (8, width), 1) + me_c * width
    across[...] = (lane_all.astype(F32) + 0.5) * (2.0 / (width * n_cols)) - 1.0

    copies = []
    for i in range(height // block):
        @pl.loop(0, block // 8)
        def _(b):
            g = i * (block // 8) + b
            rows = pl.ds(pl.multiple_of(g * 8, 8), 8)
            base_r, base_i, slope_r, slope_i = [lines[g, m] for m in range(4)]
            for t in range(width // LANES):
                lanes = slice(t * LANES, (t + 1) * LANES)
                real, imag, u = gam[0, rows, lanes], gam[1, rows, lanes], across[:, lanes]
                model_real = base_r + slope_r * u
                model_imag = base_i + slope_i * u
                out[0, rows, lanes] = real * model_real + imag * model_imag
                out[1, rows, lanes] = imag * model_real - real * model_imag

        rows = pl.ds(i * block, block)
        copy = pltpu.make_async_copy(out.at[:, rows, :], ramped.at[:, rows, :], sem.at[1 + i])
        copy.start()
        copies.append(copy)
    coh_copy.wait()
    for copy in copies:
        copy.wait()


def on_device(n_rows, n_cols, lead, trail, flags, sweep):
    height, width = flags.shape
    wide = width + 2 * LANES
    longest = 2 * height * n_rows // SWEEP_TALLY
    reach = max(1, min(n_rows - 1, (longest - 2) // height + 1))
    slots = (2 * reach + 1) * n_cols
    pieces = len(cuts(width // LANES)[0])
    pair = 2 if width // LANES % 2 == 0 else 1
    hbm = pl.BlockSpec(memory_space=pltpu.HBM)
    vmem = pl.BlockSpec(memory_space=pltpu.VMEM)
    dma = pltpu.SemaphoreType.DMA
    gam, coh, memt, fit = pl.pallas_call(
        functools.partial(front_kernel, n_rows, n_cols, reach),
        out_shape=[
            pltpu.VMEM((2, height, width), F32),
            pltpu.VMEM((height, width), F32),
            pltpu.VMEM((height, LANES), F32),
            pltpu.VMEM((8, LANES), F32),
        ],
        in_specs=[hbm, hbm, hbm, hbm],
        out_specs=[vmem, vmem, vmem, vmem],
        scratch_shapes=[
            pltpu.VMEM((2, height, width), F32),
            pltpu.VMEM((2, height, width), F32),
            pltpu.VMEM((height, width), jnp.int32),
            pltpu.VMEM((1, height), jnp.int32),
            pltpu.VMEM((3, EDGE, width), F32),
            pltpu.VMEM((3, EDGE, width), F32),
            pltpu.VMEM((3, EDGE, width), F32),
            pltpu.VMEM((3, EDGE, width), F32),
            pltpu.VMEM((height, LANES), F32),
            pltpu.VMEM((height, LANES), F32),
            pltpu.VMEM((height, LANES), F32),
            pltpu.VMEM((height, LANES), F32),
            pltpu.VMEM((3, EDGE, width), F32),
            pltpu.VMEM((4, 1, EDGE // 8 * LANES), F32),
            pltpu.VMEM((4, 1, EDGE // 8 * LANES), F32),
            pltpu.VMEM((2, 4, height, wide), BF16),
            pltpu.VMEM((16 * EDGE, wide), BF16),
            pltpu.VMEM((4, height + 2 * EDGE, width), F32),
            pltpu.VMEM(((pair + 2) * LANES, pair * LANES), BF16),
            pltpu.VMEM((8, width), F32),
            pltpu.VMEM((4, 7, 8, width), F32),
            pltpu.VMEM((height // 8, 4, 8, LANES), F32),
            pltpu.VMEM((height // 8, 3, 8, LANES), F32),
            pltpu.VMEM((8, LANES), F32),
            pltpu.VMEM((1, 2 * LANES), F32),
            pltpu.VMEM((slots, 1, 2 * LANES), F32),
            dma((7, 3)),
            dma((2, pieces)), dma((2, pieces)),
            dma((2,)), dma((2,)),
            dma((4,)), dma((4,)),
            dma((pieces,)), dma((pieces,)),
            dma((slots,)), dma((slots,)),
            pltpu.SemaphoreType.REGULAR,
        ],
        compiler_params=pltpu.CompilerParams(
            collective_id=0, has_side_effects=True, vmem_limit_bytes=60 * 1024 * 1024
        ),
        name="front",
    )(lead, trail, flags, sweep.reshape(1, height))
    block = 32 if height % 32 == 0 else 8
    return pl.pallas_call(
        functools.partial(back_kernel, n_rows, n_cols, block),
        out_shape=[
            jax.ShapeDtypeStruct((2, height, width), F32),
            jax.ShapeDtypeStruct((height, width), F32),
        ],
        in_specs=[vmem, vmem, vmem, vmem],
        out_specs=[hbm, hbm],
        scratch_shapes=[
            pltpu.VMEM((2, height, width), F32),
            pltpu.VMEM((8, width), F32),
            pltpu.VMEM((height // 8, 4, 8, LANES), F32),
            dma((1 + height // block,)),
        ],
        compiler_params=pltpu.CompilerParams(vmem_limit_bytes=16 * 1024 * 1024),
        name="back",
    )(gam, coh, memt, fit)


def solution(mesh):
    return jax.shard_map(
        functools.partial(on_device, mesh.shape["rows"], mesh.shape["cols"]),
        mesh=mesh,
        in_specs=(P(None, "rows", "cols"), P(None, "rows", "cols"), P("rows", "cols"), P("rows")),
        out_specs=(P(None, "rows", "cols"), P("rows", "cols")),
        check_vma=False,
    )
```

```python
import functools

import jax
import jax.numpy as jnp
from jax import lax
from jax.experimental import pallas as pl
from jax.experimental.pallas import tpu as pltpu
from jax.sharding import PartitionSpec as P

WIN_R = 32
WIN_C = 8
SWEEP_TALLY = 16

EDGE = WIN_R // 2
SIDE = WIN_C // 2
LANES = 128
SCALE = 2.0**56
FLOOR = 1e-36
F32 = jnp.float32
BF16 = jnp.bfloat16
MESH = pl.DeviceIdType.MESH


def masked(av, bv, wv, rows, lanes):
    w = wv[rows, lanes].astype(F32)
    return av[0, rows, lanes] * w, av[1, rows, lanes] * w, bv[0, rows, lanes] * w, bv[1, rows, lanes] * w


def encode(ar, ai, br, bi):
    sr, si = ar * SCALE, ai * SCALE
    power = sr * sr + si * si
    some = power > FLOOR
    inverse = lax.rsqrt(jnp.where(some, power, 1.0))
    return (
        jnp.where(some, power * inverse * (1.0 / SCALE), 0.0),
        jnp.where(some, (sr * br + si * bi) * inverse, br),
        jnp.where(some, (si * br - sr * bi) * inverse, bi),
    )


def decode(s, gr, gi):
    return s * gr, s * gi, s * s, gr * gr + gi * gi


def put_split(out, products, places):
    for plane, value in enumerate(products):
        high = value.astype(BF16)
        low = (value - high.astype(F32)).astype(BF16)
        for rows, lanes in places:
            out[0, plane, rows, lanes] = high
            out[1, plane, rows, lanes] = low


def edge_block(pack):
    lane = lax.broadcasted_iota(jnp.int32, pack.shape, 1)
    left, right = lane >= LANES - SIDE, lane < SIDE

    def pick(k):
        a = pack if k == 0 else pltpu.roll(pack, k * SIDE, 1)
        b = pack if k == 0 else pltpu.roll(pack, LANES - k * SIDE, 1)
        return jnp.where(left, a, jnp.where(right, b, 0.0))

    return pick(0), pick(1), pick(2)


def cuts(tiles):
    if tiles < EDGE:
        return ((0, tiles),), ((0, tiles),), ((1, 1),)
    down = [mark * tiles // 16 for mark in (0, 4, 8, 12, 14, 16)]
    up = [mark * tiles // 16 for mark in (0, 5, 9, 13)] + [tiles - 1]
    return tuple(zip(down[:-1], down[1:])), tuple(zip(up[:-1], up[1:])), ((2, 1), (3, 2), (4, 3), (5, 4))


def fold(x):
    total = x[:, 0:LANES]
    for t in range(1, x.shape[1] // LANES):
        total = total + x[:, t * LANES : (t + 1) * LANES]
    return total


def row_sum(x):
    return jnp.sum(x, 1, keepdims=True)


def front_kernel(
    n_rows, n_cols, reach,
    lead, trail, flags, sweep,
    gam, coh, memt, fit,
    av, bv, wv, sv, up_out, down_out, top_in, bot_in, left_out, right_out, left_in, right_in,
    relay_in, corner_out, corner_in, split, halo_split, boxed, ribbon, across, own_part, row_parts, flag_parts, acc_h,
    tab_out, tab_in,
    load_sem, halo_send, halo_recv, side_send, side_recv, corner_send, corner_recv,
    relay_send, relay_recv, tab_send, tab_recv, token,
):
    me_r, me_c = lax.axis_index("rows"), lax.axis_index("cols")
    height, width = flags.shape
    tiles = width // LANES
    low = height - EDGE
    total_rows, total_cols = height * n_rows, width * n_cols
    chunk = 512 if width % 512 == 0 else LANES
    has_up, has_down = me_r > 0, me_r < n_rows - 1
    has_left, has_right = me_c > 0, me_c < n_cols - 1
    down_cuts, up_cuts, steps = cuts(tiles)
    pair = 2 if tiles % 2 == 0 else 1

    def load(part, rows, lanes=pl.ds(0, width)):
        group = [
            pltpu.make_async_copy(lead.at[:, rows, lanes], av.at[:, rows, lanes], load_sem.at[part, 0]),
            pltpu.make_async_copy(trail.at[:, rows, lanes], bv.at[:, rows, lanes], load_sem.at[part, 1]),
            pltpu.make_async_copy(flags.at[rows, lanes], wv.at[rows, lanes], load_sem.at[part, 2]),
        ]
        for copy in group:
            copy.start()
        return group

    top_rows, low_rows = pl.ds(0, EDGE), pl.ds(low, EDGE)
    tucked = up_cuts[-1][1] == tiles - 1
    first = max(up_cuts[:2][-1][1], down_cuts[:3][-1][1]) * LANES
    loads = [load(0, top_rows, pl.ds(0, first))]
    if first < width:
        if tucked:
            loads.append(load(1, top_rows, pl.ds(width - LANES, LANES)))
        loads.append(load(2, low_rows, pl.ds(0, first)))
    later_loads = []
    if first < width:
        rest = width - first - (LANES if tucked else 0)
        if rest:
            later_loads.append(load(3, top_rows, pl.ds(first, rest)))
        later_loads.append(load(4, low_rows, pl.ds(first, width - first)))
    else:
        later_loads.append(load(4, low_rows))
    sweep_load = pltpu.make_async_copy(sweep, sv, load_sem.at[6, 0])
    sweep_load.start()

    barrier = pltpu.get_barrier_semaphore()
    peers = []
    for dr in range(-reach, reach + 1):
        for dc in range(n_cols):
            if dr == 0 and dc == 0:
                continue
            to = jnp.logical_and(me_r + dr >= 0, me_r + dr < n_rows)
            of = jnp.logical_and(me_r - dr >= 0, me_r - dr < n_rows)
            peers.append(((dr + reach) * n_cols + dc, to, of, me_r + dr, lax.rem(me_c + dc, n_cols)))
    near = reach == 1
    n_greeted = 0
    for slot, to, _, row, col in peers:
        dr, dc = slot // n_cols - reach, slot % n_cols
        if near and dr != 0 and dc != 0:
            continue
        n_greeted = n_greeted + to.astype(jnp.int32)

        @pl.when(to)
        def _():
            pl.semaphore_signal(barrier, inc=1, device_id=(row, col), device_id_type=MESH)

    def remote(src, dst, send, recv, row, col):
        return pltpu.make_async_remote_copy(
            src_ref=src, dst_ref=dst, send_sem=send, recv_sem=recv, device_id=(row, col), device_id_type=MESH
        )

    def cut(ref, piece):
        return ref.at[:, :, pl.ds(piece[0] * LANES, (piece[1] - piece[0]) * LANES)]

    downs = [
        remote(cut(down_out, p), cut(top_in, p), halo_send.at[0, i], halo_recv.at[0, i], me_r + 1, me_c)
        for i, p in enumerate(down_cuts)
    ]
    ups = [
        remote(cut(up_out, p), cut(bot_in, p), halo_send.at[1, i], halo_recv.at[1, i], me_r - 1, me_c)
        for i, p in enumerate(up_cuts)
    ]
    to_right = remote(right_out, left_in, side_send.at[0], side_recv.at[0], me_r, me_c + 1)
    to_left = remote(left_out, right_in, side_send.at[1], side_recv.at[1], me_r, me_c - 1)
    corners = []
    for k, (dr, dc, to, of) in enumerate((
        (1, 1, has_down & has_right, has_up & has_left),
        (1, -1, has_down & has_left, has_up & has_right),
        (-1, 1, has_up & has_right, has_down & has_left),
        (-1, -1, has_up & has_left, has_down & has_right),
    )):
        copy = remote(corner_out.at[k], corner_in.at[k], corner_send.at[k], corner_recv.at[k], me_r + dr, me_c + dc)
        corners.append((copy, to, of))

    relayed = 3 if n_rows % 2 == 0 and n_rows > 2 and len(up_cuts) > 3 else 0
    odd = lax.rem(me_r, 2) == 1
    even = jnp.logical_not(odd)
    place = lax.div(me_r, 2) * 4
    n_up = jnp.minimum(relayed, lax.div(place, n_rows // 2)) if relayed else 0
    n_down = jnp.minimum(relayed, 4 - lax.div(place + 4, n_rows // 2)) if relayed else 0
    via = []
    for i in range(relayed):
        p, q = up_cuts[i], down_cuts[i]
        ask_up, ask_down = even & (n_up > i), odd & (n_down > i)
        give_up, give_down = odd & (n_up > i), even & (n_down > i)
        via.append((
            (ask_up, remote(cut(up_out, p), cut(relay_in, p), halo_send.at[1, i], relay_recv.at[i], me_r + 1, me_c)),
            (ask_down, remote(cut(down_out, q), cut(relay_in, q), halo_send.at[0, i], relay_recv.at[i], me_r - 1, me_c)),
            (give_up, remote(cut(relay_in, p), cut(bot_in, p), relay_send.at[i], halo_recv.at[1, i], me_r - 2, me_c)),
            (give_down, remote(cut(relay_in, q), cut(top_in, q), relay_send.at[i], halo_recv.at[0, i], me_r + 2, me_c)),
        ))

    def forward(i):
        if i >= relayed:
            return
        for (_, arrival), (give, copy) in zip(via[i][:2], via[i][2:]):
            @pl.when(give)
            def _():
                arrival.wait_recv()
                copy.start()

    def encode_rows(first, out, piece):
        lanes = pl.ds(piece[0] * LANES, (piece[1] - piece[0]) * LANES)
        for k, value in enumerate(encode(*masked(av, bv, wv, pl.ds(first, EDGE), lanes))):
            out[k, :, lanes] = value

    def pack_sides(b):
        rows = pl.ds(b * 16, 16)
        lane = lax.broadcasted_iota(jnp.int32, (16, LANES), 1)
        s, gr, gi = encode(*masked(av, bv, wv, rows, pl.ds(width - LANES, LANES)))
        right_out[rows, :] = jnp.where(
            lane >= LANES - SIDE,
            s,
            jnp.where(
                lane >= LANES - 2 * SIDE,
                pltpu.roll(gr, LANES - SIDE, 1),
                jnp.where(lane >= LANES - 3 * SIDE, pltpu.roll(gi, LANES - 2 * SIDE, 1), 0.0),
            ),
        )
        s, gr, gi = encode(*masked(av, bv, wv, rows, pl.ds(0, LANES)))
        left_out[rows, :] = jnp.where(
            lane < SIDE,
            s,
            jnp.where(
                lane < 2 * SIDE,
                pltpu.roll(gr, SIDE, 1),
                jnp.where(lane < 3 * SIDE, pltpu.roll(gi, 2 * SIDE, 1), 0.0),
            ),
        )

    for group in loads:
        for copy in group:
            copy.wait()

    def tuck(piece):
        if tucked:
            for t in range(piece[0], min(piece[1], EDGE - 1)):
                for k in range(3):
                    up_out[k, EDGE - 1 : EDGE, t * LANES : (t + 1) * LANES] = up_out[k, t : t + 1, width - LANES : width]

    if first == width:
        for copy in later_loads[0]:
            copy.wait()
    if tucked:
        encode_rows(0, up_out, (tiles - 1, tiles))
    for piece in up_cuts[:2]:
        encode_rows(0, up_out, piece)
        tuck(piece)
    for piece in down_cuts[:3]:
        encode_rows(low, down_out, piece)

    pl.semaphore_wait(barrier, n_greeted)
    n_via = jnp.where(even, n_up, n_down)

    def send(point):
        for v in range(relayed + 1):
            later = [i for i in range(v, len(down_cuts)) if point == (i + (2 if i < 3 else 3) if v else i)]
            for parity, straight, other, asked in ((even, downs, ups, 0), (odd, ups, downs, 1)):
                ahead = 2 if v == asked == 0 else 1
                slots = range(ahead + 1) if point == 0 else (point + ahead,)

                @pl.when(parity & (n_via == v))
                def _():
                    far, near_by = (has_up, has_down) if asked == 0 else (has_down, has_up)
                    for k in slots:
                        if k < v:
                            via[k][asked][1].start()
                        elif k - v < len(straight):
                            @pl.when(near_by)
                            def _():
                                straight[k - v].start()
                    for i in (i for i in later if i < len(other)):
                        @pl.when(far)
                        def _():
                            other[i].start()

    send(0)
    if near:
        for dc in range(1, n_cols):
            pl.semaphore_signal(token, inc=1, device_id=(me_r, lax.rem(me_c + dc, n_cols)), device_id_type=MESH)

    if first < width:
        for group in later_loads:
            for copy in group:
                copy.wait()
        for piece in up_cuts[2:]:
            encode_rows(0, up_out, piece)
            tuck(piece)
        for piece in down_cuts[3:]:
            encode_rows(low, down_out, piece)
    bulk = load(5, pl.ds(EDGE, low - EDGE))
    for b in (0, height // 16 - 1):
        pack_sides(b)
    sub = lax.broadcasted_iota(jnp.int32, (8, LANES), 0)
    for k, (src, start, sign) in enumerate(
        ((right_out, low, -1), (left_out, low, 1), (right_out, 0, -1), (left_out, 0, 1))
    ):
        for part in range(EDGE // 8):
            block = src[start + part * 8 : start + part * 8 + 8, :]
            line = jnp.where(sub == 0, block, 0.0)
            for m in range(1, 8):
                line = line + pltpu.roll(jnp.where(sub == m, block, 0.0), sign * 3 * SIDE * m % LANES, 1)
            corner_out[k, :, part * LANES : (part + 1) * LANES] = jnp.sum(line, 0, keepdims=True)
    for copy in bulk:
        copy.wait()

    for b in range(1, height // 16 - 1):
        pack_sides(b)

    @pl.when(has_right)
    def _():
        to_right.start()

    @pl.when(has_left)
    def _():
        to_left.start()

    @pl.when(jnp.logical_not(has_left))
    def _():
        left_in[...] = jnp.zeros_like(left_in)

    @pl.when(jnp.logical_not(has_right))
    def _():
        right_in[...] = jnp.zeros_like(right_in)

    @pl.when(jnp.logical_not(has_up))
    def _():
        top_in[...] = jnp.zeros_like(top_in)

    @pl.when(jnp.logical_not(has_down))
    def _():
        bot_in[...] = jnp.zeros_like(bot_in)

    for k, (_, _, of) in enumerate(corners):
        @pl.when(jnp.logical_not(of))
        def _():
            corner_in[k] = jnp.zeros((1, EDGE // 8 * LANES), F32)

    for slot, _, of, _, _ in peers:
        @pl.when(jnp.logical_not(of))
        def _():
            tab_in[slot] = jnp.zeros((1, 2 * LANES), F32)

    if near:
        pl.semaphore_wait(token, n_cols - 1)
    for copy, to, _ in corners:
        @pl.when(to)
        def _():
            copy.start()

    lane_all = lax.broadcasted_iota(jnp.int32, (8, width), 1) + me_c * width
    across[...] = (lane_all.astype(F32) + 0.5) * (2.0 / total_cols) - 1.0

    @pl.loop(0, height // 16)
    def _(b):
        rows = pl.ds(pl.multiple_of(b * 16, 16), 16)

        @pl.loop(0, width // chunk)
        def _(c):
            lanes = pl.ds(pl.multiple_of(c * chunk, chunk), chunk)
            ar, ai, br, bi = masked(av, bv, wv, rows, lanes)
            put_split(
                split,
                (ar * br + ai * bi, ai * br - ar * bi, ar * ar + ai * ai, br * br + bi * bi),
                [(rows, pl.ds(pl.multiple_of(LANES + c * chunk, LANES), chunk))],
            )

    send(1)
    reach_in = (pair + 2) * LANES
    i = lax.broadcasted_iota(jnp.int32, (reach_in, pair * LANES), 0)
    j = lax.broadcasted_iota(jnp.int32, (reach_in, pair * LANES), 1) + LANES
    ribbon[...] = jnp.logical_and(i >= j - SIDE, i < j + SIDE).astype(F32).astype(BF16)

    def box_across(j):
        inner = pl.ds(pl.multiple_of(j * pair * LANES, pair * LANES), reach_in)
        outer = pl.ds(pl.multiple_of(j * pair * LANES, pair * LANES), pair * LANES)
        for plane in range(4):
            sums = jnp.dot(split[0, plane, :, inner], ribbon[...], preferred_element_type=F32)
            sums = sums + jnp.dot(split[1, plane, :, inner], ribbon[...], preferred_element_type=F32)
            boxed[plane, EDGE : EDGE + height, outer] = sums

    last = tiles // pair - 1
    middle = max(1, tiles // pair // 2)

    @pl.loop(1, middle)
    def _(j):
        box_across(j)

    send(2)

    @pl.loop(middle, max(middle, last))
    def _(j):
        box_across(j)

    @pl.when(has_left)
    def _():
        to_right.wait_recv()

    @pl.when(has_right)
    def _():
        to_left.wait_recv()

    sides = [pl.ds(0, LANES), pl.ds(LANES + width, LANES)]
    for b in range(height // 16):
        rows = pl.ds(b * 16, 16)
        lane = lax.broadcasted_iota(jnp.int32, (16, LANES), 1)
        pack = jnp.where(lane >= LANES // 2, left_in[rows, :], right_in[rows, :])
        put_split(split, decode(*edge_block(pack)), [(rows, lanes) for lanes in sides])

    send(3)
    forward(0)
    forward(1)
    for j in sorted({0, last}):
        box_across(j)

    sweep_load.wait()
    kind = lax.rem(lax.broadcasted_iota(jnp.int32, (LANES, height), 0), SWEEP_TALLY)
    memt[...] = (kind == sv[...]).astype(F32).T
    row_parts[...] = jnp.zeros_like(row_parts)

    group_lane = lax.broadcasted_iota(jnp.int32, (8, LANES), 1) // SWEEP_TALLY

    def row_v(group):
        row = lax.broadcasted_iota(jnp.int32, (8, LANES), 0) + (me_r * height + group * 8)
        return (row.astype(F32) + 0.5) * (2.0 / total_rows) - 1.0

    def arrange(group, values):
        table = values[0]
        for m, value in enumerate(values):
            table = value if m == 0 else jnp.where(group_lane >= m, value, table)
        return memt[group * 8 : group * 8 + 8, :] * jnp.where(group_lane < len(values), table, 0.0)

    @pl.loop(0, height // 8)
    def _(b):
        w = wv[pl.ds(pl.multiple_of(b * 8, 8), 8), :].astype(F32)
        u = across[...]
        wu = w * u
        for m, value in enumerate((w, wu, wu * u)):
            flag_parts[b, m] = fold(value)

    acc_g = None
    for b in range(height // 8):
        s0, su, suu = [row_sum(flag_parts[b, m]) for m in range(3)]
        v = row_v(b)
        part = arrange(b, (s0, su, v * s0, suu, v * su, v * v * s0))
        acc_g = part if acc_g is None else acc_g + part
    tab_out[:, 0:LANES] = jnp.sum(acc_g, 0, keepdims=True)

    send(4)
    edge_groups, groups = EDGE // 8, height // 8

    def shifted(x, following):
        n1, n2, n4 = following if following else (None, None, None)
        r1 = pltpu.roll(x, 7, 0)
        y1 = x + (r1 if n1 is None else jnp.where(sub < 7, r1, n1))
        r2 = pltpu.roll(y1, 6, 0)
        y2 = y1 + (r2 if n2 is None else jnp.where(sub < 6, r2, n2))
        r4 = pltpu.roll(y2, 4, 0)
        return y2 + (r4 if n4 is None else jnp.where(sub < 4, r4, n4)), (r1, r2, r4)

    def emit(g, lanes, window):
        rows = slice(g * 8, g * 8 + 8)
        inverse = lax.rsqrt((window[2] + 1.0) * (window[3] + 1.0))
        real, imag = window[0] * inverse, window[1] * inverse
        gam[0, rows, lanes] = real
        gam[1, rows, lanes] = imag
        coh[rows, lanes] = jnp.sqrt(real * real + imag * imag)
        w, u = wv[rows, lanes].astype(F32), across[:, lanes]
        wr, wi = w * real, w * imag
        for m, value in enumerate((wr, wi, wr * u, wi * u)):
            row_parts[g, m] += value

    def group_rows(g):
        return slice(g * 8, g * 8 + 8)

    def finish(t):
        lanes = pl.ds(pl.multiple_of(t * LANES, LANES), LANES)
        eights = [[None] * 4 for _ in range(groups + 2)]
        pairs = [[None] * 4 for _ in range(groups + 2)]
        following = [None] * 4
        for g in range(groups + 1, edge_groups - 1, -1):
            for plane in range(4):
                eights[g][plane], following[plane] = shifted(boxed[plane, group_rows(g), lanes], following[plane])
                if g <= groups - 1:
                    pairs[g][plane] = eights[g][plane] + eights[g + 1][plane]
            if g <= groups - 3:
                emit(g, lanes, [pairs[g][p] + pairs[g + 2][p] for p in range(4)])
        for p in range(4):
            kept = (
                pairs[edge_groups][p], eights[edge_groups][p] + pairs[edge_groups + 1][p], *following[p],
                eights[groups - 2][p] + pairs[groups - 1][p], pairs[groups - 1][p],
            )
            for k, value in enumerate(kept):
                own_part[p, k, :, lanes] = value

    def finish_edges(t):
        lanes = pl.ds(pl.multiple_of(t * LANES, LANES), LANES)
        outer, inner = [None] * 4, [None] * 4
        for p in range(4):
            near, following = shifted(boxed[p, group_rows(1), lanes], [own_part[p, k, :, lanes] for k in (2, 3, 4)])
            far, _ = shifted(boxed[p, group_rows(0), lanes], following)
            inner[p] = near + own_part[p, 1, :, lanes]
            outer[p] = far + near + own_part[p, 0, :, lanes]
        emit(0, lanes, outer)
        emit(1, lanes, inner)
        for p in range(4):
            _, following = shifted(boxed[p, group_rows(groups + 3), lanes], None)
            far, following = shifted(boxed[p, group_rows(groups + 2), lanes], following)
            near, _ = shifted(boxed[p, group_rows(groups + 1), lanes], following)
            inner[p] = near + own_part[p, 5, :, lanes]
            outer[p] = near + far + own_part[p, 6, :, lanes]
        emit(groups - 2, lanes, inner)
        emit(groups - 1, lanes, outer)

    def add_rows(groups):
        total = None
        for g in groups:
            hr, hi, hur, hui = [row_sum(row_parts[g, m]) for m in range(4)]
            v = row_v(g)
            part = arrange(g, (hr, hi, hur, hui, v * hr, v * hi))
            total = part if total is None else total + part
        return total

    @pl.loop(0, tiles // 2)
    def _(t):
        finish(t)

    forward(2)
    send(5)

    @pl.loop(tiles // 2, tiles)
    def _(t):
        finish(t)

    send(6)

    acc_h[...] = add_rows(range(edge_groups, groups - edge_groups))

    def put_halo(part, products, where):
        for plane, value in enumerate(products):
            first = (plane * 2 + part) * EDGE
            high = value.astype(BF16)
            low_part = (value - high.astype(F32)).astype(BF16)
            for lanes in where:
                halo_split[first : first + EDGE, lanes] = high
                halo_split[8 * EDGE + first : 9 * EDGE + first, lanes] = low_part

    def box_halo(j):
        inner = pl.ds(j * pair * LANES, reach_in)
        outer = pl.ds(j * pair * LANES, pair * LANES)
        sums = jnp.dot(halo_split[:, inner], ribbon[...], preferred_element_type=F32)
        for plane in range(4):
            for part, target in enumerate((0, EDGE + height)):
                first = (plane * 2 + part) * EDGE
                boxed[plane, target : target + EDGE, outer] = (
                    sums[first : first + EDGE] + sums[8 * EDGE + first : 9 * EDGE + first]
                )

    done = 0
    had_down, had_up = 0, 0
    for i, (need_down, need_up) in enumerate(steps):
        if i == 0:
            for copy, _, of in corners:
                @pl.when(of)
                def _():
                    copy.wait_recv()

            def unpack(k, part):
                line = jnp.broadcast_to(corner_in[k, :, part * LANES : (part + 1) * LANES], (8, LANES))
                block = line
                for m in range(1, 8):
                    turned = pltpu.roll(line, (1, -1)[k % 2] * 3 * SIDE * m % LANES, 1)
                    block = jnp.where(sub == m, turned, block)
                return block

            lane = lax.broadcasted_iota(jnp.int32, (8, LANES), 1)
            packs = [
                jnp.concatenate(
                    [jnp.where(lane >= LANES // 2, unpack(k, part), unpack(k + 1, part)) for part in range(EDGE // 8)], 0
                )
                for k in (0, 2)
            ]
            for part, pack in enumerate(packs):
                put_halo(part, decode(*edge_block(pack)), sides)

        @pl.when(has_up)
        def _():
            for copy in downs[had_down:need_down]:
                copy.wait_recv()

        @pl.when(has_down)
        def _():
            for copy in ups[had_up:need_up]:
                copy.wait_recv()

        end_up = up_cuts[need_up - 1][1]
        if tucked and i == len(steps) - 1:
            end_up = tiles
            for t in range(EDGE - 1):
                for k in range(3):
                    bot_in[k, t : t + 1, width - LANES : width] = bot_in[k, EDGE - 1 : EDGE, t * LANES : (t + 1) * LANES]
        ranges = ((down_cuts[had_down][0], down_cuts[need_down - 1][1]), (up_cuts[had_up][0], end_up))
        for part, (halo, (start, end)) in enumerate(zip((top_in, bot_in), ranges)):
            source = pl.ds(start * LANES, (end - start) * LANES)
            target = pl.ds((start + 1) * LANES, (end - start) * LANES)
            put_halo(part, decode(*[halo[m, :, source] for m in range(3)]), [target])
        had_down, had_up = need_down, need_up
        ready = tiles // pair if i == len(steps) - 1 else max(0, (min(ranges[0][1], ranges[1][1]) - 1) // pair)
        for j in range(done, ready):
            box_halo(j)
        if ready > done:
            @pl.loop(done, ready)
            def _(j):
                for t in range(pair):
                    finish_edges(j * pair + t)
        done = ready
        if i == 0:
            send(7)

    acc_last = acc_h[...] + add_rows(list(range(edge_groups)) + list(range(groups - edge_groups, groups)))
    tab_out[:, LANES:] = jnp.sum(acc_last, 0, keepdims=True)
    swaps = [
        (remote(tab_out, tab_in.at[slot], tab_send.at[slot], tab_recv.at[slot], row, col), to, of)
        for slot, to, of, row, col in sorted(peers, key=lambda p: (p[0] // n_cols == reach, p[0] % n_cols == 0))
    ]
    for copy, to, _ in swaps:
        @pl.when(to)
        def _():
            copy.start()

    tab_in[reach * n_cols] = tab_out[...]
    @pl.when(has_down)
    def _():
        for copy in downs:
            copy.wait_send()

    @pl.when(has_up)
    def _():
        for copy in ups:
            copy.wait_send()

    for copy, to, _ in corners:
        @pl.when(to)
        def _():
            copy.wait_send()

    for group in via:
        for give, copy in group[2:]:
            @pl.when(give)
            def _():
                copy.wait_send()

    @pl.when(has_right)
    def _():
        to_right.wait_send()

    @pl.when(has_left)
    def _():
        to_left.wait_send()

    for copy, _, of in swaps:
        @pl.when(of)
        def _():
            copy.wait_recv()

    total = functools.reduce(jnp.add, [tab_in[slot] for slot in range(tab_in.shape[0])])

    def column(base, m):
        part = total[:, base : base + LANES]
        return part if m == 0 else pltpu.roll(part, LANES - m * SWEEP_TALLY, 1)

    s0, su, sv_, suu, suv, svv = [column(0, m) for m in range(6)]
    hr, hi, hur, hui, hvr, hvi = [column(LANES, m) for m in range(6)]
    floored = jnp.maximum(s0, 1.0)
    mid_u, mid_v = su / floored, sv_ / floored
    guu = suu - 2.0 * mid_u * su + mid_u * mid_u * s0
    guv = suv - mid_u * sv_ - mid_v * su + mid_u * mid_v * s0
    gvv = svv - 2.0 * mid_v * sv_ + mid_v * mid_v * s0
    hur, hui = hur - mid_u * hr, hui - mid_u * hi
    hvr, hvi = hvr - mid_v * hr, hvi - mid_v * hi
    ridge = 0.001 * s0 + 1.0
    duu, dvv = guu + ridge, gvv + ridge
    scale = 1.0 / (duu * dvv - guv * guv)
    base = 1.0 / (s0 + ridge)
    c1r, c1i = (dvv * hur - guv * hvr) * scale, (dvv * hui - guv * hvi) * scale
    c2r, c2i = (duu * hvr - guv * hur) * scale, (duu * hvi - guv * hui) * scale
    valid = lax.broadcasted_iota(jnp.int32, (1, LANES), 1) < SWEEP_TALLY
    rows_out = (hr * base - c1r * mid_u, hi * base - c1i * mid_u, c1r, c1i, c2r, c2i, mid_v)
    for m, value in enumerate(rows_out):
        fit[m : m + 1, :] = jnp.where(valid, value, 0.0)

    for copy, to, _ in swaps:
        @pl.when(to)
        def _():
            copy.wait_send()


def back_kernel(n_rows, n_cols, block, gam, coh, memt, fit, ramped, coherence, out, across, lines, sem):
    height, width = coh.shape
    me_r, me_c = lax.axis_index("rows"), lax.axis_index("cols")
    coh_copy = pltpu.make_async_copy(coh, coherence, sem.at[0])
    coh_copy.start()
    for g in range(height // 8):
        row = lax.broadcasted_iota(jnp.int32, (8, LANES), 0) + (me_r * height + g * 8)
        dv = (row.astype(F32) + 0.5) * (2.0 / (height * n_rows)) - 1.0 - fit[6:7, :]
        one = memt[g * 8 : g * 8 + 8, :]
        for m, value in enumerate((fit[0:1, :] + fit[4:5, :] * dv, fit[1:2, :] + fit[5:6, :] * dv, fit[2:3, :], fit[3:4, :])):
            lines[g, m] = jnp.broadcast_to(row_sum(one * value), (8, LANES))
    lane_all = lax.broadcasted_iota(jnp.int32, (8, width), 1) + me_c * width
    across[...] = (lane_all.astype(F32) + 0.5) * (2.0 / (width * n_cols)) - 1.0

    copies = []
    for i in range(height // block):
        @pl.loop(0, block // 8)
        def _(b):
            g = i * (block // 8) + b
            rows = pl.ds(pl.multiple_of(g * 8, 8), 8)
            base_r, base_i, slope_r, slope_i = [lines[g, m] for m in range(4)]
            for t in range(width // LANES):
                lanes = slice(t * LANES, (t + 1) * LANES)
                real, imag, u = gam[0, rows, lanes], gam[1, rows, lanes], across[:, lanes]
                model_real = base_r + slope_r * u
                model_imag = base_i + slope_i * u
                out[0, rows, lanes] = real * model_real + imag * model_imag
                out[1, rows, lanes] = imag * model_real - real * model_imag

        rows = pl.ds(i * block, block)
        copy = pltpu.make_async_copy(out.at[:, rows, :], ramped.at[:, rows, :], sem.at[1 + i])
        copy.start()
        copies.append(copy)
    coh_copy.wait()
    for copy in copies:
        copy.wait()


def on_device(n_rows, n_cols, lead, trail, flags, sweep):
    height, width = flags.shape
    wide = width + 2 * LANES
    longest = 2 * height * n_rows // SWEEP_TALLY
    reach = max(1, min(n_rows - 1, (longest - 2) // height + 1))
    slots = (2 * reach + 1) * n_cols
    pieces = len(cuts(width // LANES)[0])
    pair = 2 if width // LANES % 2 == 0 else 1
    hbm = pl.BlockSpec(memory_space=pltpu.HBM)
    vmem = pl.BlockSpec(memory_space=pltpu.VMEM)
    dma = pltpu.SemaphoreType.DMA
    gam, coh, memt, fit = pl.pallas_call(
        functools.partial(front_kernel, n_rows, n_cols, reach),
        out_shape=[
            pltpu.VMEM((2, height, width), F32),
            pltpu.VMEM((height, width), F32),
            pltpu.VMEM((height, LANES), F32),
            pltpu.VMEM((8, LANES), F32),
        ],
        in_specs=[hbm, hbm, hbm, hbm],
        out_specs=[vmem, vmem, vmem, vmem],
        scratch_shapes=[
            pltpu.VMEM((2, height, width), F32),
            pltpu.VMEM((2, height, width), F32),
            pltpu.VMEM((height, width), jnp.int32),
            pltpu.VMEM((1, height), jnp.int32),
            pltpu.VMEM((3, EDGE, width), F32),
            pltpu.VMEM((3, EDGE, width), F32),
            pltpu.VMEM((3, EDGE, width), F32),
            pltpu.VMEM((3, EDGE, width), F32),
            pltpu.VMEM((height, LANES), F32),
            pltpu.VMEM((height, LANES), F32),
            pltpu.VMEM((height, LANES), F32),
            pltpu.VMEM((height, LANES), F32),
            pltpu.VMEM((3, EDGE, width), F32),
            pltpu.VMEM((4, 1, EDGE // 8 * LANES), F32),
            pltpu.VMEM((4, 1, EDGE // 8 * LANES), F32),
            pltpu.VMEM((2, 4, height, wide), BF16),
            pltpu.VMEM((16 * EDGE, wide), BF16),
            pltpu.VMEM((4, height + 2 * EDGE, width), F32),
            pltpu.VMEM(((pair + 2) * LANES, pair * LANES), BF16),
            pltpu.VMEM((8, width), F32),
            pltpu.VMEM((4, 7, 8, width), F32),
            pltpu.VMEM((height // 8, 4, 8, LANES), F32),
            pltpu.VMEM((height // 8, 3, 8, LANES), F32),
            pltpu.VMEM((8, LANES), F32),
            pltpu.VMEM((1, 2 * LANES), F32),
            pltpu.VMEM((slots, 1, 2 * LANES), F32),
            dma((7, 3)),
            dma((2, pieces)), dma((2, pieces)),
            dma((2,)), dma((2,)),
            dma((4,)), dma((4,)),
            dma((pieces,)), dma((pieces,)),
            dma((slots,)), dma((slots,)),
            pltpu.SemaphoreType.REGULAR,
        ],
        compiler_params=pltpu.CompilerParams(
            collective_id=0, has_side_effects=True, vmem_limit_bytes=60 * 1024 * 1024
        ),
        name="front",
    )(lead, trail, flags, sweep.reshape(1, height))
    block = 32 if height % 32 == 0 else 8
    return pl.pallas_call(
        functools.partial(back_kernel, n_rows, n_cols, block),
        out_shape=[
            jax.ShapeDtypeStruct((2, height, width), F32),
            jax.ShapeDtypeStruct((height, width), F32),
        ],
        in_specs=[vmem, vmem, vmem, vmem],
        out_specs=[hbm, hbm],
        scratch_shapes=[
            pltpu.VMEM((2, height, width), F32),
            pltpu.VMEM((8, width), F32),
            pltpu.VMEM((height // 8, 4, 8, LANES), F32),
            dma((1 + height // block,)),
        ],
        compiler_params=pltpu.CompilerParams(vmem_limit_bytes=16 * 1024 * 1024),
        name="back",
    )(gam, coh, memt, fit)


def solution(mesh):
    return jax.shard_map(
        functools.partial(on_device, mesh.shape["rows"], mesh.shape["cols"]),
        mesh=mesh,
        in_specs=(P(None, "rows", "cols"), P(None, "rows", "cols"), P("rows", "cols"), P("rows")),
        out_specs=(P(None, "rows", "cols"), P("rows", "cols")),
        check_vma=False,
    )
```
